128 devices in a mesh: row: 16 (over z_hi, y, core), col: 8 (over x, z_lo).
Axes of the slice: x: 4, y: 4, z: 4 (z_hi: 2, z_lo: 2; z = z_hi * 2 + z_lo), core: 2. Of those that a mesh axis runs over, the one named last changes fastest.
Arguments:
- tokens: bfloat16 [16384, 2048], P(('row', 'col')), may hold values from -30 to 30
- ln1_gain: float32 [2048], replicated, may hold values from 0.25 to 1.75
- qkv_weight: bfloat16 [2048, 16, 3, 128], P('row', 'col'), may hold values from -4 to 4
- out_weight: bfloat16 [2048, 2048], P('col', 'row'), may hold values from -0.125 to 0.125
- ln2_gain: float32 [2048], replicated, may hold values from 0.25 to 1.75
- ffn_in: bfloat16 [2048, 8192], P('row', 'col'), may hold values from -0.125 to 0.125
- ffn_out: bfloat16 [8192, 2048], P('col', 'row'), may hold values from -0.0625 to 0.0625
- expert_ids: int32 [16384, 1], P(('row', 'col')), may hold values from 0 to 63; in each aligned block of 128 rows (0 to 127, 128 to 255, ...) at most 4 rows name the same one
- expert_in: bfloat16 [128, 2048, 2048], P(('row', 'col')), may hold values from -0.125 to 0.125
- expert_out: bfloat16 [128, 2048, 2048], P(('row', 'col')), may hold values from -0.09375 to 0.09375
Outputs:
- block_out: bfloat16 [16384, 2048], P(('row', 'col'))
The draws below stay inside these ranges and needn't reach their ends.
Inputs may be any that keep to these rules, and one draw needn't show every extreme that they name: `expert_ids`: among the tokens of one device no expert is named more than 4 times, and in every draw some expert is named exactly 4 times by the tokens of some device.
All inputs are finite; a program needn't handle non-finite values.
Results may differ from the reference program's by a relative error of at most 0.013.
Values may be sent and summed in bfloat16 or wider, within the bound.
A program may use at most 128 MiB of HBM per device.

```python
import math
import jax
import jax.numpy as jnp
import numpy as np
from jax import lax

D = 2048
HEADS = 16
DH = 128
FF = 8192
FFE = 4096
TOK_DEV = 128
SEQ = 1024
TOKENS = 16384
EXPERTS = 64
CAP = 4
FF_BLOCK = 1024
HALF = 2048
N_ROW = 16
N_COL = 8


def draw_tokens(key, part):
    first_key = jax.random.fold_in(jax.random.fold_in(key, 11), 0)
    base_values = jax.random.normal(first_key, (TOKENS, D), jnp.float32)
    return jnp.clip(base_values, -30.0, 30.0).astype(jnp.bfloat16)


def draw_qkv_weight(key, part):
    first_key = jax.random.fold_in(jax.random.fold_in(key, 23), 0)
    base_values = jax.random.normal(first_key, (D, HEADS, 3, DH), jnp.float32) * D ** (-0.5)
    factors = jnp.array([2.0, 1.0, 1.0], jnp.float32)[None, None, :, None]
    base_values = base_values * factors
    return jnp.clip(base_values, -4.0, 4.0).astype(jnp.bfloat16)


def block_scale(key, dims, shards, low, high):
    gain, own = 1.0, jax.random.fold_in(key, 6)
    for dim, blocks in shards:
        draws = jnp.exp(jax.random.uniform(jax.random.fold_in(own, dim), (blocks,), jnp.float32, low / len(shards), high / len(shards)))
        gain = gain * jnp.repeat(draws, dims[dim] // blocks).reshape([-1 if axis == dim else 1 for axis in range(len(dims))])
    return gain


def assign_block(key, own, number, rows, count, top, reach, slope):
    ranking = jax.random.permutation(key, count)
    crowded, common = portions_of(count, rows * top, reach, slope, True), portions_of(count, rows * top, reach, slope, False)
    places = jnp.arange(count)

    def named(lengths, offset_by):
        used = int((lengths > 0).sum())
        fixed = max(1, used // 4)
        passed = fixed + (places - fixed + offset_by * (used - fixed)) % max(1, count - fixed)
        return jnp.zeros((count,), jnp.int32).at[ranking[jnp.where(places < fixed, places, passed)]].set(jnp.asarray(lengths, jnp.int32))

    lengths = jnp.where(number % 4 == 0, named(crowded, number // 4), named(common, number - number // 4 - 1))
    mixed = jax.random.permutation(jax.random.fold_in(own, 3), count)
    giver, receiver = mixed[0:count // 2 * 2:2], mixed[1:count // 2 * 2:2]
    margin = jnp.minimum(lengths[giver] - 1, reach - lengths[receiver]) // 2
    margin = jnp.where((giver == ranking[0]) | (receiver == ranking[0]) | (lengths[receiver] == 0), 0, jnp.maximum(margin, 0))
    passed = jax.random.randint(jax.random.fold_in(own, 4), (count // 2,), 0, 1 << 20) % (margin + 1)
    lengths = lengths.at[giver].add(-passed).at[receiver].add(passed)
    members = jnp.searchsorted(jnp.cumsum(lengths), jnp.arange(rows * top), side="right").astype(jnp.int32)
    grid = members.reshape(top, rows).T
    grid = grid[jax.random.permutation(jax.random.fold_in(own, 1), rows)]
    offset_by = jax.random.randint(jax.random.fold_in(own, 2), (rows, 1), 0, top)
    return jnp.take_along_axis(grid, (jnp.arange(top)[None, :] + offset_by) % top, axis=1)


def portions_of(count, total, limit, skew, full):
    weights = [(1 << 20) // math.isqrt(rank ** skew) + 1 for rank in range(1, count + 1)]
    largest = limit if full else min(limit, max(-(-total // count), total * weights[0] // sum(weights)))
    least = 1 if total - largest >= count - 1 else 0
    holding, rest = [largest] + [least] * (count - 1), total - largest - least * (count - 1)
    while rest > 0:
        candidates = [i for i in range(1, count) if holding[i] < largest] or [i for i in range(1, count) if holding[i] < limit]
        whole, remaining = sum([weights[i] for i in candidates]), rest
        for i in candidates:
            extra = min(limit - holding[i], max(1, remaining * weights[i] // whole), rest)
            holding[i] = holding[i] + extra
            rest = rest - extra
    return np.array(holding)


def normal_values(own_key, dims, width, bound, pieces=(), held_as=jnp.bfloat16):
    factor_of = block_scale(own_key, dims, pieces, -0.22, 0.18) if pieces else 1.0
    values = jax.random.normal(own_key, dims, jnp.float32) * width * factor_of
    return jnp.minimum(jnp.maximum(values, -bound), bound).astype(held_as)


def setup_inputs(seed: int = 0) -> dict:
    key_list = jax.random.split(jax.random.key(seed), 11)
    tokens = draw_tokens(jax.random.fold_in(key_list[10], 71), 0)
    ln1_gain = jnp.clip(1.0 + 0.15 * jax.random.normal(key_list[1], (D,), jnp.float32), 0.25, 1.75)
    qkv_weight = draw_qkv_weight(jax.random.fold_in(key_list[10], 71), 0)
    out_weight = normal_values(key_list[3], (HEADS * DH, D), (HEADS * DH) ** -0.5, 0.125, ((0, 8), (1, 16)))
    ln2_gain = jnp.clip(1.0 + 0.15 * jax.random.normal(key_list[4], (D,), jnp.float32), 0.25, 1.75)
    ffn_in = normal_values(key_list[5], (D, FF), D ** -0.5, 0.125, ((0, 16), (1, 8)))
    ffn_out = normal_values(key_list[6], (FF, D), FF ** -0.5, 0.0625, ((0, 8), (1, 16)))
    expert_ids_keys = jax.random.split(jax.random.fold_in(key_list[7], 1), TOKENS // TOK_DEV)
    expert_ids_turns = jax.random.permutation(jax.random.fold_in(key_list[7], 3), TOKENS // TOK_DEV)
    expert_ids = jax.vmap(lambda own, number: assign_block(jax.random.fold_in(key_list[7], 2), own, number, TOK_DEV, EXPERTS, 1, CAP, 2))(expert_ids_keys, expert_ids_turns).reshape((TOKENS, 1))
    expert_in = normal_values(key_list[8], (EXPERTS * 2, D, HALF), D ** -0.5, 0.125, ((0, 128),))
    expert_out = normal_values(key_list[9], (EXPERTS * 2, HALF, D), FFE ** -0.5, 0.09375, ((0, 128),))
    return {"tokens": tokens, "ln1_gain": ln1_gain, "qkv_weight": qkv_weight, "out_weight": out_weight, "ln2_gain": ln2_gain, "ffn_in": ffn_in, "ffn_out": ffn_out, "expert_ids": expert_ids, "expert_in": expert_in, "expert_out": expert_out}


def layer_norm(row_data, gain_vector):
    row_data = row_data.astype(jnp.float32)
    centered = row_data - lax.optimization_barrier(jnp.mean(row_data, axis=-1, keepdims=True))
    spread = lax.optimization_barrier(jnp.mean(centered * centered, axis=-1, keepdims=True))
    return centered * lax.rsqrt(spread + 1e-06) * gain_vector

def attend_head(queries, key_rows, value_rows):
    scores = jnp.dot(queries, key_rows.T, preferred_element_type=jnp.float32) * DH ** (-0.5)
    row_max = lax.optimization_barrier(jnp.max(scores, axis=-1, keepdims=True))
    weights = jnp.exp(scores - row_max)
    probabilities = (weights / lax.optimization_barrier(jnp.sum(weights, axis=-1, keepdims=True))).astype(jnp.bfloat16)
    return jnp.dot(probabilities, value_rows, preferred_element_type=jnp.float32).astype(jnp.bfloat16)

def image_block(image_rows, ln1_gain, qkv_weight, out_weight, ln2_gain, ffn_in, ffn_out):
    normed = layer_norm(image_rows, ln1_gain).astype(jnp.bfloat16)
    projected = jnp.dot(normed, qkv_weight.reshape(D, HEADS * 3 * DH), preferred_element_type=jnp.float32)
    projected = projected.astype(jnp.bfloat16).reshape(SEQ, HEADS, 3, DH)
    by_head = jnp.transpose(projected, (1, 2, 0, 3))
    attended = lax.map(lambda head_item: attend_head(head_item[0], head_item[1], head_item[2]), by_head)
    attended = jnp.transpose(attended, (1, 0, 2)).reshape(SEQ, HEADS * DH)
    mixed_heads = jnp.dot(attended, out_weight, preferred_element_type=jnp.float32)
    hidden_state = (image_rows.astype(jnp.float32) + mixed_heads).astype(jnp.bfloat16)
    normed_two = layer_norm(hidden_state, ln2_gain).astype(jnp.bfloat16)
    inner_sum = jnp.dot(normed_two, ffn_in, preferred_element_type=jnp.float32)
    hidden_units = jax.nn.gelu(inner_sum, approximate=False).astype(jnp.bfloat16)
    dense_sum = jnp.zeros((SEQ, D), jnp.float32)
    for column_block in range(N_COL):
        lower_edge = column_block * FF_BLOCK
        part_sum = jnp.dot(hidden_units[:, lower_edge:lower_edge + FF_BLOCK], ffn_out[lower_edge:lower_edge + FF_BLOCK], preferred_element_type=jnp.float32)
        rounded = lax.optimization_barrier(part_sum.astype(jnp.bfloat16))
        dense_sum = dense_sum + rounded.astype(jnp.float32)
    return (hidden_state, normed_two, dense_sum)

def reference(tokens, ln1_gain, qkv_weight, out_weight, ln2_gain, ffn_in, ffn_out, expert_ids, expert_in, expert_out):
    device_count = N_ROW * N_COL
    images = tokens.reshape(TOKENS // SEQ, SEQ, D)

    def one_image(image_rows):
        return image_block(image_rows, ln1_gain, qkv_weight, out_weight, ln2_gain, ffn_in, ffn_out)
    hidden_state, normed_two, dense_sum = lax.map(one_image, images)
    hidden_state = hidden_state.reshape(TOKENS, D)
    normed_two = normed_two.reshape(TOKENS, D)
    dense_sum = dense_sum.reshape(TOKENS, D)
    chosen = expert_ids[:, 0].astype(jnp.int32)
    by_device = chosen.reshape(device_count, TOK_DEV)
    one_hot = (by_device[:, :, None] == jnp.arange(EXPERTS, dtype=jnp.int32)[None, None, :]).astype(jnp.int32)
    earlier = jnp.cumsum(one_hot, axis=1) - one_hot
    local_slot = lax.optimization_barrier(jnp.sum(earlier * one_hot, axis=2))
    global_slot = (local_slot + CAP * jnp.arange(device_count, dtype=jnp.int32)[:, None]).reshape(TOKENS).astype(jnp.int32)
    buffers = jnp.zeros((EXPERTS, device_count * CAP, D), normed_two.dtype).at[chosen, global_slot].set(normed_two)
    paired_in = expert_in.reshape(EXPERTS, 2, D, HALF)
    paired_out = expert_out.reshape(EXPERTS, 2, HALF, D)

    def run_expert(operands):
        buffer_rows, weights_in, weights_out = operands
        whole_in = jnp.concatenate((weights_in[0], weights_in[1]), axis=1)
        whole_out = jnp.concatenate((weights_out[0], weights_out[1]), axis=0)
        inner_units = jax.nn.gelu(jnp.dot(buffer_rows, whole_in, preferred_element_type=jnp.float32), approximate=False).astype(jnp.bfloat16)
        return jnp.dot(inner_units, whole_out, preferred_element_type=jnp.float32).astype(jnp.bfloat16)
    results = lax.map(run_expert, (buffers, paired_in, paired_out))
    expert_rows = results[chosen, global_slot]
    block_out = hidden_state.astype(jnp.float32) + dense_sum + expert_rows.astype(jnp.float32)
    return block_out.astype(jnp.bfloat16)
```

```python
import heapq

import jax
import jax.numpy as jnp
from jax import lax
from jax.experimental import pallas as pl
from jax.experimental.pallas import tpu as pltpu
from jax.sharding import Mesh
from jax.sharding import PartitionSpec as P

ROW = ("zh", "y", "core")
COL = ("x", "zl")
ROW_COL = ("zh", "y", "core", "x", "zl")
BF16 = jnp.bfloat16
F32 = jnp.float32


class Spot:
    def __init__(self):
        self.x = lax.axis_index("x")
        self.y = lax.axis_index("y")
        self.zh = lax.axis_index("zh")
        self.zl = lax.axis_index("zl")
        self.core = lax.axis_index("core")
        self.row = (self.zh * 4 + self.y) * 2 + self.core
        z = self.zh * 2 + self.zl
        zp, zm = lax.rem(z + 1, 4), lax.rem(z + 3, 4)
        self.zhp, self.zhm = lax.div(zp, 2), lax.div(zm, 2)
        self.yp, self.ym = lax.rem(self.y + 1, 4), lax.rem(self.y + 3, 4)
        self.up = {
            "x": {"x": lax.rem(self.x + 1, 4)},
            "y": {"y": self.yp},
            "z": {"zh": self.zhp, "zl": lax.rem(zp, 2)},
        }
        self.down = {
            "x": {"x": lax.rem(self.x + 3, 4)},
            "y": {"y": self.ym},
            "z": {"zh": self.zhm, "zl": lax.rem(zm, 2)},
        }
        self.sibling = {"core": 1 - self.core}
        self.pair = {"zl": 1 - self.zl}


class Wire:
    def __init__(self, send_sems, recv_sems):
        self.send_sems, self.recv_sems = send_sems, recv_sems
        self.sent = []

    def send(self, src, dst, where):
        k = len(self.sent)
        copy = pltpu.make_async_remote_copy(
            src_ref=src,
            dst_ref=dst,
            send_sem=self.send_sems.at[k],
            recv_sem=self.recv_sems.at[k],
            device_id=where,
            device_id_type=pl.DeviceIdType.MESH,
        )
        copy.start()
        self.sent.append(copy)
        return copy


def greet(places):
    barrier = pltpu.get_barrier_semaphore()
    for place in places:
        pl.semaphore_signal(
            barrier, inc=1, device_id=place, device_id_type=pl.DeviceIdType.MESH
        )
    pl.semaphore_wait(barrier, len(places))


def run_streams(streams):
    queue = []
    for n, stream in enumerate(streams):
        step = next(stream, None)
        if step is not None:
            heapq.heappush(queue, (step[0], n, step[1], stream))
    while queue:
        _, n, copy, stream = heapq.heappop(queue)
        copy.wait_recv()
        step = next(stream, None)
        if step is not None:
            heapq.heappush(queue, (step[0], n, step[1], stream))


def gather_weight(wire, at, own, local, whole, half, first, start, block):
    c, zh, y = at.core, at.zh, at.y
    rows = own.shape[0] // 2
    low, high = pl.ds(0, rows), pl.ds(rows, rows)
    if first == "y":
        a = wire.send(own, whole.at[0, zh, y, c, half], at.up["y"])
        b = wire.send(own, whole.at[0, zh, y, c, half], at.down["y"])
        yield start + 2 * block, a
        slot = whole.at[0, zh, at.ym, c, half, low]
        e = wire.send(slot, slot, at.up["y"])
        yield start + 2 * block, b
        slot = whole.at[0, zh, at.yp, c, half, high]
        f = wire.send(slot, slot, at.down["y"])
        yield start + 3 * block, e
        yield start + 3 * block, f
        local.wait()
        group = whole.at[0, zh, :, c, half]
        far = whole.at[1, zh, :, c, half]
        g = wire.send(group, far, at.up["z"])
        h = wire.send(group, far, at.down["z"])
        s = [wire.send(group, group, at.sibling)]
        yield start + 11 * block, g
        lower = pl.ds(0, 2)
        i = wire.send(
            whole.at[1, at.zhm, lower, c, half], whole.at[0, at.zhm, lower, c, half], at.up["z"]
        )
        s.append(wire.send(whole.at[1, at.zhm, :, c, half], whole.at[1, at.zhm, :, c, half], at.sibling))
        yield start + 11 * block, h
        upper = pl.ds(2, 2)
        j = wire.send(
            whole.at[1, at.zhp, upper, c, half], whole.at[0, at.zhp, upper, c, half], at.down["z"]
        )
        s.append(wire.send(whole.at[1, at.zhp, :, c, half], whole.at[1, at.zhp, :, c, half], at.sibling))
        yield start + 15 * block, i
        slot = whole.at[0, 1 - zh, lower, c, half]
        s.append(wire.send(slot, slot, at.sibling))
        yield start + 15 * block, j
        slot = whole.at[0, 1 - zh, upper, c, half]
        s.append(wire.send(slot, slot, at.sibling))
    else:
        a = wire.send(own, whole.at[1, zh, y, c, half], at.up["z"])
        b = wire.send(own, whole.at[1, zh, y, c, half], at.down["z"])
        yield start + 2 * block, a
        e = wire.send(
            whole.at[1, at.zhm, y, c, half, low], whole.at[0, at.zhm, y, c, half, low], at.up["z"]
        )
        yield start + 2 * block, b
        f = wire.send(
            whole.at[1, at.zhp, y, c, half, high], whole.at[0, at.zhp, y, c, half, high], at.down["z"]
        )
        yield start + 3 * block, e
        yield start + 3 * block, f
        local.wait()
        group = whole.at[:, :, y, c, half]
        g = wire.send(group, group, at.up["y"])
        h = wire.send(group, group, at.down["y"])
        s = [wire.send(group, group, at.sibling)]
        yield start + 11 * block, g
        slot = whole.at[0, :, at.ym, c, half]
        i = wire.send(slot, slot, at.up["y"])
        slot = whole.at[:, :, at.ym, c, half]
        s.append(wire.send(slot, slot, at.sibling))
        yield start + 11 * block, h
        slot = whole.at[1, :, at.yp, c, half]
        j = wire.send(slot, slot, at.down["y"])
        slot = whole.at[:, :, at.yp, c, half]
        s.append(wire.send(slot, slot, at.sibling))
        across = lax.rem(y + 2, 4)
        yield start + 15 * block, i
        slot = whole.at[0, :, across, c, half]
        s.append(wire.send(slot, slot, at.sibling))
        yield start + 15 * block, j
        slot = whole.at[1, :, across, c, half]
        s.append(wire.send(slot, slot, at.sibling))
    for n, copy in enumerate(s):
        yield start + 15 * block + 2 + n / 8, copy


def gather_x(wire, at, own, tiles, parts, start, block):
    half = own.shape[0] // 2 if parts == 2 else own.shape[0]
    low, high = pl.ds(0, half), pl.ds(half, half)
    if parts == 2:
        a1 = wire.send(own.at[low], tiles.at[3, low], at.up["x"])
        b1 = wire.send(own.at[high], tiles.at[1, high], at.down["x"])
        a2 = wire.send(own.at[high], tiles.at[3, high], at.up["x"])
        b2 = wire.send(own.at[low], tiles.at[1, low], at.down["x"])
        yield start + block, a1
        e = wire.send(tiles.at[3, low], tiles.at[2, low], at.up["x"])
        yield start + block, b1
        f = wire.send(tiles.at[1, high], tiles.at[2, high], at.down["x"])
        yield start + 2 * block, a2
        yield start + 2 * block, b2
        yield start + 3 * block, e
        yield start + 3 * block, f
    else:
        a = wire.send(own, tiles.at[3], at.up["x"])
        b = wire.send(own, tiles.at[1], at.down["x"])
        yield start + block, a
        e = wire.send(tiles.at[3], tiles.at[2], at.up["x"])
        yield start + block, b
        yield start + 2 * block, e


def scatter_x(wire, at, terms, got, passing, start, block):
    half = terms.shape[1] // 2
    low, high = pl.ds(0, half), pl.ds(half, half)
    c1 = wire.send(terms.at[2, low], passing.at[0], at.up["x"])
    c2 = wire.send(terms.at[2, high], passing.at[1], at.down["x"])
    a = wire.send(terms.at[1], got.at[0], at.up["x"])
    b = wire.send(terms.at[3], got.at[1], at.down["x"])
    yield start + block, c1
    d1 = wire.send(passing.at[0], got.at[2, low], at.up["x"])
    yield start + block, c2
    d2 = wire.send(passing.at[1], got.at[2, high], at.down["x"])
    yield start + 3 * block, a
    yield start + 3 * block, b
    yield start + 4 * block, d1
    yield start + 4 * block, d2


def comm_call(body, inputs, outs, scratch, copies, locals_, number, sent_bytes, name):
    return pl.pallas_call(
        body,
        out_shape=outs,
        in_specs=[pl.BlockSpec(memory_space=pl.ANY)] * len(inputs),
        out_specs=[pl.BlockSpec(memory_space=pl.ANY)] * len(outs),
        scratch_shapes=[
            *scratch,
            pltpu.SemaphoreType.DMA((copies,)),
            pltpu.SemaphoreType.DMA((copies,)),
            pltpu.SemaphoreType.DMA((max(1, locals_),)),
        ],
        compiler_params=pltpu.CompilerParams(
            collective_id=number, has_side_effects=True, vmem_limit_bytes=8 << 20
        ),
        name=name,
    )(*inputs)


def like(shape, dtype=BF16):
    return jax.ShapeDtypeStruct(shape, dtype)


GATHER_COPIES = 13


def first_gather(tokens, pos, qkv, out):
    def body(tok, pos_in, qkv_in, out_in, tiles, spots, qkv_all, out_all,
             tok_v, pos_v, qkv_v, out_v, ss, rs, ls):
        at = Spot()
        loads = [
            pltpu.make_async_copy(tok, tok_v, ls.at[0]),
            pltpu.make_async_copy(pos_in, pos_v, ls.at[1]),
            pltpu.make_async_copy(qkv_in, qkv_v, ls.at[2]),
            pltpu.make_async_copy(out_in, out_v, ls.at[3]),
        ]
        for load in loads:
            load.start()
        greet([at.up["x"], at.down["x"], at.up["y"], at.down["y"], at.up["z"], at.down["z"], at.sibling])
        for load in loads:
            load.wait()
        stores = [
            pltpu.make_async_copy(tok_v, tiles.at[0], ls.at[4]),
            pltpu.make_async_copy(pos_v, spots.at[0], ls.at[5]),
            *[
                pltpu.make_async_copy(src.at[h], dst.at[0, at.zh, at.y, at.core, h], ls.at[6 + 2 * n + h])
                for n, (src, dst) in enumerate(((qkv_v, qkv_all), (out_v, out_all)))
                for h in range(2)
            ],
        ]
        for store in stores:
            store.start()
        wire = Wire(ss, rs)
        run_streams([
            gather_x(wire, at, pos_v, spots, 1, 0, 2),
            gather_x(wire, at, tok_v, tiles, 2, 0, 5.7),
            gather_weight(wire, at, qkv_v.at[0], stores[2], qkv_all, 0, "y", 0, 1.1),
            gather_weight(wire, at, qkv_v.at[1], stores[3], qkv_all, 1, "z", 0, 1.1),
            gather_weight(wire, at, out_v.at[0], stores[4], out_all, 0, "y", 1, 1.4),
            gather_weight(wire, at, out_v.at[1], stores[5], out_all, 1, "z", 1, 1.4),
        ])
        for store in stores[:2]:
            store.wait()
        for copy in wire.sent:
            copy.wait_send()

    outs = [
        like((4, *tokens.shape)),
        like((4, *pos.shape), jnp.int32),
        like((2, 2, 4, 2, *qkv.shape)),
        like((2, 2, 4, 2, *out.shape)),
    ]
    scratch = [
        pltpu.VMEM(tokens.shape, BF16),
        pltpu.VMEM(pos.shape, jnp.int32),
        pltpu.VMEM(qkv.shape, BF16),
        pltpu.VMEM(out.shape, BF16),
    ]
    return comm_call(body, [tokens, pos, qkv, out], outs, scratch,
                     9 + 4 * GATHER_COPIES, 10, 1, 0, "gather_first")


def pair_swap(mine, number, name):
    def body(src, dst, ss, rs, ls):
        at = Spot()
        greet([at.pair])
        wire = Wire(ss, rs)
        copy = wire.send(src.at[1], dst, at.pair)
        copy.wait()

    return comm_call(body, [mine], [like(mine.shape[1:])], [], 1, 0, number, 0, name)[0]


def scatter_and_weight(terms, weight, number, name):
    def body(src, w_in, got, passing, w_all, w_v, ss, rs, ls):
        at = Spot()
        load = pltpu.make_async_copy(w_in, w_v, ls.at[0])
        load.start()
        greet([at.up["x"], at.down["x"], at.up["y"], at.down["y"], at.up["z"], at.down["z"], at.sibling])
        load.wait()
        stores = [
            pltpu.make_async_copy(w_v.at[h], w_all.at[0, at.zh, at.y, at.core, h], ls.at[1 + h])
            for h in range(2)
        ]
        for store in stores:
            store.start()
        wire = Wire(ss, rs)
        run_streams([
            scatter_x(wire, at, src, got, passing, 0, 5.7),
            gather_weight(wire, at, w_v.at[0], stores[0], w_all, 0, "y", 0, 1.4),
            gather_weight(wire, at, w_v.at[1], stores[1], w_all, 1, "z", 0, 1.4),
        ])
        for copy in wire.sent:
            copy.wait_send()

    rows, width = terms.shape[1:]
    outs = [
        like((3, rows, width)),
        like((2, rows // 2, width)),
        like((2, 2, 4, 2, *weight.shape)),
    ]
    got, _, whole = comm_call(body, [terms, weight], outs, [pltpu.VMEM(weight.shape, BF16)],
                              6 + 2 * GATHER_COPIES, 3, number, 0, name)
    return got, whole


def gather_and_weight(block, weight, number, name):
    def body(src, w_in, tiles, w_all, src_v, w_v, ss, rs, ls):
        at = Spot()
        loads = [
            pltpu.make_async_copy(src, src_v, ls.at[0]),
            pltpu.make_async_copy(w_in, w_v, ls.at[1]),
        ]
        for load in loads:
            load.start()
        greet([at.up["x"], at.down["x"], at.up["y"], at.down["y"], at.up["z"], at.down["z"], at.sibling])
        for load in loads:
            load.wait()
        stores = [pltpu.make_async_copy(src_v, tiles.at[0], ls.at[2])] + [
            pltpu.make_async_copy(w_v.at[h], w_all.at[0, at.zh, at.y, at.core, h], ls.at[3 + h])
            for h in range(2)
        ]
        for store in stores:
            store.start()
        wire = Wire(ss, rs)
        run_streams([
            gather_x(wire, at, src_v, tiles, 2, 0, 5.7),
            gather_weight(wire, at, w_v.at[0], stores[1], w_all, 0, "y", 0, 1.4),
            gather_weight(wire, at, w_v.at[1], stores[2], w_all, 1, "z", 0, 1.4),
        ])
        stores[0].wait()
        for copy in wire.sent:
            copy.wait_send()

    outs = [like((4, *block.shape)), like((2, 2, 4, 2, *weight.shape))]
    scratch = [pltpu.VMEM(block.shape, BF16), pltpu.VMEM(weight.shape, BF16)]
    return comm_call(body, [block, weight], outs, scratch,
                     6 + 2 * GATHER_COPIES, 5, number, 0, name)


def scatter_only(terms, number, name):
    def body(src, got, passing, ss, rs, ls):
        at = Spot()
        greet([at.up["x"], at.down["x"]])
        wire = Wire(ss, rs)
        run_streams([scatter_x(wire, at, src, got, passing, 0, 5.7)])
        for copy in wire.sent:
            copy.wait_send()

    rows, width = terms.shape[1:]
    outs = [like((3, rows, width)), like((2, rows // 2, width))]
    return comm_call(body, [terms], outs, [], 6, 0, number, 0, name)[0]


def exchange(table, number, name):
    both = table.ndim == 3
    rows, width = table.shape[-2:]

    def body(src, dst, own_v, ss, rs, ls):
        at = Spot()
        own = src.at[at.row] if both else src.at[at.zl, at.row]
        load = pltpu.make_async_copy(own, own_v, ls.at[0])
        load.start()
        places = []
        for dzh in range(2):
            for dzl in range(2):
                for dy in range(4):
                    for dc in range(2):
                        if dzh or dzl or dy or dc:
                            zh = 1 - at.zh if dzh else at.zh
                            zl = 1 - at.zl if dzl else at.zl
                            core = 1 - at.core if dc else at.core
                            y = lax.rem(at.y + dy, 4)
                            places.append((zh, zl, y, core))
        ids = [{"zh": zh, "zl": zl, "y": y, "core": core} for zh, zl, y, core in places]
        greet(ids)
        wire = Wire(ss, rs)
        for (zh, zl, y, core), where in zip(places, ids):
            row = (zh * 4 + y) * 2 + core
            block = src.at[row] if both else src.at[zl, row]
            wire.send(block, dst.at[at.zl, at.row], where)
        load.wait()
        store = pltpu.make_async_copy(own_v, dst.at[at.zl, at.row], ls.at[1])
        store.start()
        store.wait()
        for copy in wire.sent:
            copy.wait()

    return comm_call(body, [table], [like((2, 16, rows, width))], [pltpu.VMEM((rows, width), BF16)],
                     31, 2, number, 0, name)[0]


def layer_norm(row_data, gain_vector):
    row_data = row_data.astype(F32)
    centered = row_data - jnp.mean(row_data, axis=-1, keepdims=True)
    spread = jnp.mean(centered * centered, axis=-1, keepdims=True)
    return centered * lax.rsqrt(spread + 1e-06) * gain_vector


def dot(a, b):
    return jnp.dot(a, b, preferred_element_type=F32)


def dot_nt(a, b):
    return lax.dot_general(a, b, (((1,), (1,)), ((), ())), preferred_element_type=F32)


def shards(
    tokens, ln1_gain, qkv_weight, out_weight, ln2_gain, ffn_in, ffn_out,
    expert_ids, expert_in, expert_out,
):
    count, width = tokens.shape
    experts, slots = 64, 4
    chosen = expert_ids[:, 0]
    one_hot = (chosen[:, None] == jnp.arange(experts, dtype=jnp.int32)[None, :]).astype(BF16)
    order = jnp.arange(count, dtype=jnp.int32)
    before = (order[None, :] < order[:, None]).astype(BF16)
    earlier = jnp.sum(dot(before, one_hot) * one_hot.astype(F32), axis=1)
    pos = (chosen * slots + earlier.astype(jnp.int32))[None, :]

    heads, head_dim = qkv_weight.shape[1], qkv_weight.shape[3]
    qkv_width = heads * 3 * head_dim
    tiles, spots, qkv_all, out_all = first_gather(
        tokens, pos, qkv_weight.reshape(2, -1, qkv_width), out_weight.T.reshape(2, -1, out_weight.shape[0])
    )
    normed = layer_norm(tiles.reshape(4 * count, width), ln1_gain).astype(BF16)
    qkv_all = qkv_all.reshape(2, width, qkv_width)
    projected = jnp.stack([dot(normed, qkv_all[n]).astype(BF16) for n in range(2)])
    other = pair_swap(projected, 2, "swap_heads")
    image = jnp.concatenate([projected[0], other]).reshape(-1, heads, 3, head_dim)
    scores = jnp.einsum(
        "qhd,khd->hqk", image[:, :, 0], image[:, :, 1], preferred_element_type=F32
    ) * head_dim ** (-0.5)
    weights = jnp.exp(scores - jnp.max(scores, axis=-1, keepdims=True))
    probabilities = (weights / jnp.sum(weights, axis=-1, keepdims=True)).astype(BF16)
    attended = jnp.einsum("hqk,khd->qhd", probabilities, image[:, :, 2], preferred_element_type=F32)
    attended = attended.astype(BF16).reshape(2, 4 * count, heads * head_dim)
    other = pair_swap(attended, 3, "swap_attended")
    out_all = out_all.reshape(2, width, -1)
    mixed = dot_nt(attended[0], out_all[0]) + dot_nt(other, out_all[1])
    mixed = mixed.astype(BF16).reshape(4, count, width)
    got, in_all = scatter_and_weight(mixed, ffn_in.reshape(2, -1, ffn_in.shape[1]), 4, "scatter_heads")
    hidden = (
        tokens.astype(F32) + mixed[0].astype(F32) + got[0].astype(F32) + got[1].astype(F32) + got[2].astype(F32)
    ).astype(BF16)
    normed_mine = layer_norm(hidden, ln2_gain).astype(BF16)
    down = ffn_out.T
    tiles, down_all = gather_and_weight(normed_mine, down.reshape(2, -1, down.shape[1]), 5, "gather_normed")
    normed = tiles.reshape(4 * count, width)

    slot = jnp.arange(256, dtype=jnp.int32)[:, None, None]
    source = jnp.arange(4, dtype=jnp.int32)[None, :, None]
    wanted = ((slot // 16) * 4 + lax.axis_index("x")) * slots + slot % 4
    placing = ((spots.reshape(1, 4, count) == wanted) & ((slot // 4) % 4 == source)).astype(BF16)
    placing = placing.reshape(256, 4 * count)
    table = dot(placing, normed).astype(BF16).reshape(16, 16, width)
    arrived = exchange(table, 6, "dispatch").reshape(-1, width)
    inner = jax.nn.gelu(dot(arrived, expert_in[0]), approximate=False).astype(BF16)
    partial = dot(inner, expert_out[0]).astype(BF16).reshape(2, 16, 16, width)
    returned = exchange(partial, 7, "return").reshape(-1, width)

    in_all = in_all.reshape(2, width, -1)
    down_all = down_all.reshape(2, width, -1)
    total = 0
    for n in range(2):
        hidden_units = jax.nn.gelu(dot(normed, in_all[n]), approximate=False).astype(BF16)
        total = total + dot_nt(hidden_units, down_all[n])
    for n in range(2):
        total = total + lax.dot_general(
            placing, returned[n * 256 : (n + 1) * 256], (((0,), (0,)), ((), ())), preferred_element_type=F32
        )
    total = total.astype(BF16).reshape(4, count, width)
    got = scatter_only(total, 8, "scatter_dense")
    block_out = (
        hidden.astype(F32) + total[0].astype(F32) + got[0].astype(F32) + got[1].astype(F32) + got[2].astype(F32)
    )
    return block_out.astype(BF16)


def solution(mesh):
    split = Mesh(mesh.devices.reshape(2, 4, 2, 4, 2), ROW_COL)
    in_specs = (
        P(ROW_COL, None),
        P(),
        P(ROW, COL, None, None),
        P(COL, ROW),
        P(),
        P(ROW, COL),
        P(COL, ROW),
        P(ROW_COL, None),
        P(ROW_COL, None, None),
        P(ROW_COL, None, None),
    )
    out_specs = P(ROW_COL, None)
    return jax.shard_map(shards, mesh=split, in_specs=in_specs, out_specs=out_specs, check_vma=False)
```

```python
import heapq

import jax
import jax.numpy as jnp
from jax import lax
from jax.experimental import pallas as pl
from jax.experimental.pallas import tpu as pltpu
from jax.sharding import Mesh
from jax.sharding import PartitionSpec as P

ROW = ("zh", "y", "core")
COL = ("x", "zl")
ROW_COL = ("zh", "y", "core", "x", "zl")
BF16 = jnp.bfloat16
F32 = jnp.float32


class Spot:
    def __init__(self):
        self.x = lax.axis_index("x")
        self.y = lax.axis_index("y")
        self.zh = lax.axis_index("zh")
        self.zl = lax.axis_index("zl")
        self.core = lax.axis_index("core")
        self.row = (self.zh * 4 + self.y) * 2 + self.core
        z = self.zh * 2 + self.zl
        zp, zm = lax.rem(z + 1, 4), lax.rem(z + 3, 4)
        self.zhp, self.zhm = lax.div(zp, 2), lax.div(zm, 2)
        self.yp, self.ym = lax.rem(self.y + 1, 4), lax.rem(self.y + 3, 4)
        self.up = {
            "x": {"x": lax.rem(self.x + 1, 4)},
            "y": {"y": self.yp},
            "z": {"zh": self.zhp, "zl": lax.rem(zp, 2)},
        }
        self.down = {
            "x": {"x": lax.rem(self.x + 3, 4)},
            "y": {"y": self.ym},
            "z": {"zh": self.zhm, "zl": lax.rem(zm, 2)},
        }
        self.sibling = {"core": 1 - self.core}
        self.pair = {"zl": 1 - self.zl}


class Wire:
    def __init__(self, send_sems, recv_sems):
        self.send_sems, self.recv_sems = send_sems, recv_sems
        self.sent = []

    def send(self, src, dst, where):
        k = len(self.sent)
        copy = pltpu.make_async_remote_copy(
            src_ref=src,
            dst_ref=dst,
            send_sem=self.send_sems.at[k],
            recv_sem=self.recv_sems.at[k],
            device_id=where,
            device_id_type=pl.DeviceIdType.MESH,
        )
        copy.start()
        self.sent.append(copy)
        return copy


def greet(places):
    barrier = pltpu.get_barrier_semaphore()
    for place in places:
        pl.semaphore_signal(
            barrier, inc=1, device_id=place, device_id_type=pl.DeviceIdType.MESH
        )
    pl.semaphore_wait(barrier, len(places))


def run_streams(streams, late=()):
    queue, count = [], 0
    for stream in streams:
        step = next(stream, None)
        if step is not None:
            heapq.heappush(queue, (step[0], count, step[1], stream))
        count += 1
    while queue:
        _, n, copy, stream = heapq.heappop(queue)
        if copy is not None:
            copy.wait_recv()
        step = next(stream, None)
        if step is not None:
            heapq.heappush(queue, (step[0], n, step[1], stream))
        while late:
            step, stream = late.pop()
            heapq.heappush(queue, (step[0], count, step[1], stream))
            count += 1


def gather_weight(wire, at, own, local, whole, half, first, start, block):
    c, zh, y = at.core, at.zh, at.y
    rows = own.shape[0] // 2
    low, high = pl.ds(0, rows), pl.ds(rows, rows)
    if first == "y":
        a = wire.send(own, whole.at[0, zh, y, c, half], at.up["y"])
        b = wire.send(own, whole.at[0, zh, y, c, half], at.down["y"])
        yield start + 2 * block, a
        slot = whole.at[0, zh, at.ym, c, half, low]
        e = wire.send(slot, slot, at.up["y"])
        yield start + 2 * block, b
        slot = whole.at[0, zh, at.yp, c, half, high]
        f = wire.send(slot, slot, at.down["y"])
        yield start + 3 * block, e
        yield start + 3 * block, f
        local.wait()
        group = whole.at[0, zh, :, c, half]
        far = whole.at[1, zh, :, c, half]
        g = wire.send(group, far, at.up["z"])
        h = wire.send(group, far, at.down["z"])
        s = [wire.send(group, group, at.sibling)]
        yield start + 11 * block, g
        lower = pl.ds(0, 2)
        i = wire.send(
            whole.at[1, at.zhm, lower, c, half], whole.at[0, at.zhm, lower, c, half], at.up["z"]
        )
        s.append(wire.send(whole.at[1, at.zhm, :, c, half], whole.at[1, at.zhm, :, c, half], at.sibling))
        yield start + 11 * block, h
        upper = pl.ds(2, 2)
        j = wire.send(
            whole.at[1, at.zhp, upper, c, half], whole.at[0, at.zhp, upper, c, half], at.down["z"]
        )
        s.append(wire.send(whole.at[1, at.zhp, :, c, half], whole.at[1, at.zhp, :, c, half], at.sibling))
        yield start + 15 * block, i
        slot = whole.at[0, 1 - zh, lower, c, half]
        s.append(wire.send(slot, slot, at.sibling))
        yield start + 15 * block, j
        slot = whole.at[0, 1 - zh, upper, c, half]
        s.append(wire.send(slot, slot, at.sibling))
    else:
        a = wire.send(own, whole.at[1, zh, y, c, half], at.up["z"])
        b = wire.send(own, whole.at[1, zh, y, c, half], at.down["z"])
        yield start + 2 * block, a
        e = wire.send(
            whole.at[1, at.zhm, y, c, half, low], whole.at[0, at.zhm, y, c, half, low], at.up["z"]
        )
        yield start + 2 * block, b
        f = wire.send(
            whole.at[1, at.zhp, y, c, half, high], whole.at[0, at.zhp, y, c, half, high], at.down["z"]
        )
        yield start + 3 * block, e
        yield start + 3 * block, f
        local.wait()
        group = whole.at[:, :, y, c, half]
        g = wire.send(group, group, at.up["y"])
        h = wire.send(group, group, at.down["y"])
        s = [wire.send(group, group, at.sibling)]
        yield start + 11 * block, g
        slot = whole.at[0, :, at.ym, c, half]
        i = wire.send(slot, slot, at.up["y"])
        slot = whole.at[:, :, at.ym, c, half]
        s.append(wire.send(slot, slot, at.sibling))
        yield start + 11 * block, h
        slot = whole.at[1, :, at.yp, c, half]
        j = wire.send(slot, slot, at.down["y"])
        slot = whole.at[:, :, at.yp, c, half]
        s.append(wire.send(slot, slot, at.sibling))
        across = lax.rem(y + 2, 4)
        yield start + 15 * block, i
        slot = whole.at[0, :, across, c, half]
        s.append(wire.send(slot, slot, at.sibling))
        yield start + 15 * block, j
        slot = whole.at[1, :, across, c, half]
        s.append(wire.send(slot, slot, at.sibling))
    for n, copy in enumerate(s):
        yield start + 15 * block + 2 + n / 8, copy


def gather_x(wire, at, own, tiles, parts, start, block):
    half = own.shape[0] // 2 if parts == 2 else own.shape[0]
    low, high = pl.ds(0, half), pl.ds(half, half)
    if parts == 2:
        a1 = wire.send(own.at[low], tiles.at[3, low], at.up["x"])
        b1 = wire.send(own.at[high], tiles.at[1, high], at.down["x"])
        a2 = wire.send(own.at[high], tiles.at[3, high], at.up["x"])
        b2 = wire.send(own.at[low], tiles.at[1, low], at.down["x"])
        yield start + block, a1
        e = wire.send(tiles.at[3, low], tiles.at[2, low], at.up["x"])
        yield start + block, b1
        f = wire.send(tiles.at[1, high], tiles.at[2, high], at.down["x"])
        yield start + 2 * block, a2
        yield start + 2 * block, b2
        yield start + 3 * block, e
        yield start + 3 * block, f
    else:
        a = wire.send(own, tiles.at[3], at.up["x"])
        b = wire.send(own, tiles.at[1], at.down["x"])
        yield start + block, a
        e = wire.send(tiles.at[3], tiles.at[2], at.up["x"])
        yield start + block, b
        yield start + 2 * block, e


def scatter_x(wire, at, terms, got, passing, start, block):
    half = terms.shape[1] // 2
    low, high = pl.ds(0, half), pl.ds(half, half)
    c1 = wire.send(terms.at[2, low], passing.at[0], at.up["x"])
    c2 = wire.send(terms.at[2, high], passing.at[1], at.down["x"])
    a = wire.send(terms.at[1], got.at[0], at.up["x"])
    b = wire.send(terms.at[3], got.at[1], at.down["x"])
    yield start + block, c1
    d1 = wire.send(passing.at[0], got.at[2, low], at.up["x"])
    yield start + block, c2
    d2 = wire.send(passing.at[1], got.at[2, high], at.down["x"])
    yield start + 3 * block, a
    yield start + 3 * block, b
    yield start + 4 * block, d1
    yield start + 4 * block, d2


def comm_call(body, inputs, outs, scratch, copies, locals_, number, sent_bytes, name):
    return pl.pallas_call(
        body,
        out_shape=outs,
        in_specs=[pl.BlockSpec(memory_space=pl.ANY)] * len(inputs),
        out_specs=[pl.BlockSpec(memory_space=pl.ANY)] * len(outs),
        scratch_shapes=[
            *scratch,
            pltpu.SemaphoreType.DMA((copies,)),
            pltpu.SemaphoreType.DMA((copies,)),
            pltpu.SemaphoreType.DMA((max(1, locals_),)),
        ],
        compiler_params=pltpu.CompilerParams(
            collective_id=number, has_side_effects=True, vmem_limit_bytes=8 << 20
        ),
        name=name,
    )(*inputs)


def like(shape, dtype=BF16):
    return jax.ShapeDtypeStruct(shape, dtype)


GATHER_COPIES = 13


def first_gather(tokens, pos, qkv, out):
    def body(tok, pos_in, qkv_in, out_in, tiles, spots, qkv_all, out_all,
             tok_v, pos_v, qkv_v, out_v, ss, rs, ls):
        at = Spot()
        loads = [
            pltpu.make_async_copy(tok, tok_v, ls.at[0]),
            pltpu.make_async_copy(pos_in, pos_v, ls.at[1]),
            pltpu.make_async_copy(qkv_in, qkv_v, ls.at[2]),
            pltpu.make_async_copy(out_in, out_v, ls.at[3]),
        ]
        for load in loads:
            load.start()
        greet([at.up["x"], at.down["x"], at.up["y"], at.down["y"], at.up["z"], at.down["z"], at.sibling])
        for load in loads:
            load.wait()
        stores = [
            pltpu.make_async_copy(tok_v, tiles.at[0], ls.at[4]),
            pltpu.make_async_copy(pos_v, spots.at[0], ls.at[5]),
            *[
                pltpu.make_async_copy(src.at[h], dst.at[0, at.zh, at.y, at.core, h], ls.at[6 + 2 * n + h])
                for n, (src, dst) in enumerate(((qkv_v, qkv_all), (out_v, out_all)))
                for h in range(2)
            ],
        ]
        for store in stores:
            store.start()
        wire = Wire(ss, rs)
        run_streams([
            gather_x(wire, at, pos_v, spots, 1, 0, 2),
            gather_x(wire, at, tok_v, tiles, 2, 0, 5.7),
            gather_weight(wire, at, qkv_v.at[0], stores[2], qkv_all, 0, "y", 0, 1.1),
            gather_weight(wire, at, qkv_v.at[1], stores[3], qkv_all, 1, "z", 0, 1.1),
            gather_weight(wire, at, out_v.at[0], stores[4], out_all, 0, "y", 1, 1.4),
            gather_weight(wire, at, out_v.at[1], stores[5], out_all, 1, "z", 1, 1.4),
        ])
        for store in stores[:2]:
            store.wait()
        for copy in wire.sent:
            copy.wait_send()

    outs = [
        like((4, *tokens.shape)),
        like((4, *pos.shape), jnp.int32),
        like((2, 2, 4, 2, *qkv.shape)),
        like((2, 2, 4, 2, *out.shape)),
    ]
    scratch = [
        pltpu.VMEM(tokens.shape, BF16),
        pltpu.VMEM(pos.shape, jnp.int32),
        pltpu.VMEM(qkv.shape, BF16),
        pltpu.VMEM(out.shape, BF16),
    ]
    return comm_call(body, [tokens, pos, qkv, out], outs, scratch,
                     9 + 4 * GATHER_COPIES, 10, 1, 0, "gather_first")


def pair_swap(mine, number, name):
    def body(src, dst, ss, rs, ls):
        at = Spot()
        greet([at.pair])
        wire = Wire(ss, rs)
        copy = wire.send(src.at[1], dst, at.pair)
        copy.wait()

    return comm_call(body, [mine], [like(mine.shape[1:])], [], 1, 0, number, 0, name)[0]


def scatter_and_weight(terms, weight, number, name):
    def body(src, w_in, got, passing, w_all, w_v, ss, rs, ls):
        at = Spot()
        load = pltpu.make_async_copy(w_in, w_v, ls.at[0])
        load.start()
        greet([at.up["x"], at.down["x"], at.up["y"], at.down["y"], at.up["z"], at.down["z"], at.sibling])
        load.wait()
        stores = [
            pltpu.make_async_copy(w_v.at[h], w_all.at[0, at.zh, at.y, at.core, h], ls.at[1 + h])
            for h in range(2)
        ]
        for store in stores:
            store.start()
        wire = Wire(ss, rs)
        run_streams([
            scatter_x(wire, at, src, got, passing, 0, 5.7),
            gather_weight(wire, at, w_v.at[0], stores[0], w_all, 0, "y", 0, 1.4),
            gather_weight(wire, at, w_v.at[1], stores[1], w_all, 1, "z", 0, 1.4),
        ])
        for copy in wire.sent:
            copy.wait_send()

    rows, width = terms.shape[1:]
    outs = [
        like((3, rows, width)),
        like((2, rows // 2, width)),
        like((2, 2, 4, 2, *weight.shape)),
    ]
    got, _, whole = comm_call(body, [terms, weight], outs, [pltpu.VMEM(weight.shape, BF16)],
                              6 + 2 * GATHER_COPIES, 3, number, 0, name)
    return got, whole


def gather_and_weight(block, weight, number, name):
    def body(src, w_in, tiles, w_all, src_v, w_v, ss, rs, ls):
        at = Spot()
        loads = [
            pltpu.make_async_copy(src, src_v, ls.at[0]),
            pltpu.make_async_copy(w_in, w_v, ls.at[1]),
        ]
        for load in loads:
            load.start()
        greet([at.up["x"], at.down["x"], at.up["y"], at.down["y"], at.up["z"], at.down["z"], at.sibling])
        for load in loads:
            load.wait()
        stores = [pltpu.make_async_copy(src_v, tiles.at[0], ls.at[2])] + [
            pltpu.make_async_copy(w_v.at[h], w_all.at[0, at.zh, at.y, at.core, h], ls.at[3 + h])
            for h in range(2)
        ]
        for store in stores:
            store.start()
        wire = Wire(ss, rs)
        run_streams([
            gather_x(wire, at, src_v, tiles, 2, 0, 5.7),
            gather_weight(wire, at, w_v.at[0], stores[1], w_all, 0, "y", 0, 1.4),
            gather_weight(wire, at, w_v.at[1], stores[2], w_all, 1, "z", 0, 1.4),
        ])
        stores[0].wait()
        for copy in wire.sent:
            copy.wait_send()

    outs = [like((4, *block.shape)), like((2, 2, 4, 2, *weight.shape))]
    scratch = [pltpu.VMEM(block.shape, BF16), pltpu.VMEM(weight.shape, BF16)]
    return comm_call(body, [block, weight], outs, scratch,
                     6 + 2 * GATHER_COPIES, 5, number, 0, name)


def layer_norm(row_data, gain_vector):
    row_data = row_data.astype(F32)
    centered = row_data - jnp.mean(row_data, axis=-1, keepdims=True)
    spread = jnp.mean(centered * centered, axis=-1, keepdims=True)
    return centered * lax.rsqrt(spread + 1e-06) * gain_vector


def gelu(v):
    return v * (0.5 + 0.5 * lax.erf(v * 0.5**0.5))


def dot(a, b):
    return jnp.dot(a, b, preferred_element_type=F32)


def dot_nt(a, b):
    return lax.dot_general(a, b, (((1,), (1,)), ((), ())), preferred_element_type=F32)


def tail_kernel(table, normed, hidden, placed, in_all, down_all, expert_in, expert_out, number):
    width = normed.shape[1]
    chunk, chunks = 512, width // 512

    def body(tab, nor, hid, pla, win, wdown, ein, eout, out,
             nor_v, hid_v, pla_v, win_v, wdown_v, ein_v, eout_v,
             units, dense, xx, aside, passing, away, mine, hop, near, ahead, sib,
             terms, got, across, ss, rs, ls):
        at = Spot()
        cross = {"zh": 1 - at.zh, "zl": 1 - at.zl}
        own_load = pltpu.make_async_copy(tab.at[:, 0, 0], xx.at[pl.ds(0, 2), 0, 0], ls.at[0])
        pairs = [(nor, nor_v), (win, win_v), (wdown, wdown_v), (ein, ein_v), (eout, eout_v), (pla, pla_v), (hid, hid_v)]
        loads = [pltpu.make_async_copy(src, dst, ls.at[1 + n]) for n, (src, dst) in enumerate(pairs)]
        own_load.start()
        for load in loads:
            load.start()
        greet([at.up["x"], at.down["x"], at.up["y"], at.down["y"], at.sibling, at.pair, cross])
        wire = Wire(ss, rs)
        both = pl.ds(0, 2)
        core0 = wire.send(tab.at[:, 0, 1], xx.at[both, 0, 1], at.sibling)
        core1 = wire.send(tab.at[:, pl.ds(1, 3), 1], aside, at.sibling)
        pair_in, far_in = [], []

        def z_part(src, where, t):
            pair_in.append(wire.send(src(1), xx.at[(2, *where)], at.pair))
            x = wire.send(src(0), xx.at[(3, *where)], cross)
            yield t, x
            far_in.append(wire.send(xx.at[(3, *where)], xx.at[(4, *where)], at.pair))

        def held(where):
            return lambda n: xx.at[(n, *where)]

        def own_y():
            yield from z_part(lambda n: tab.at[n, 0, 0], (0, 0), 2.5)

        def sib_y():
            yield 1.5, core0
            yield from z_part(held((0, 1)), (0, 1), 5)

        y1 = wire.send(tab.at[:, 1, 0], xx.at[both, 1, 0], at.up["y"])
        y3 = wire.send(tab.at[:, 3, 0], xx.at[both, 3, 0], at.down["y"])
        y2 = wire.send(tab.at[:, 2, 0], passing.at[0], at.up["y"])
        second = {}

        def middle():
            yield 1.6, core1
            second[2] = wire.send(aside.at[:, 1], passing.at[1], at.down["y"])
            second[1] = wire.send(aside.at[:, 0], xx.at[both, 1, 1], at.up["y"])
            second[3] = wire.send(aside.at[:, 2], xx.at[both, 3, 1], at.down["y"])
            yield 6, y2
            e = wire.send(passing.at[0], xx.at[both, 2, 0], at.up["y"])
            yield 6.2, second[2]
            f = wire.send(passing.at[1], xx.at[both, 2, 1], at.down["y"])
            yield 8, y1
            yield 9, second[1]
            later.append(z_part(held((1,)), (1,), 15))
            yield from start_later()
            yield 9, y3
            yield 9.5, second[3]
            later.append(z_part(held((3,)), (3,), 18))
            yield from start_later()
            yield 12, e
            yield 12, f
            later.append(z_part(held((2,)), (2,), 21))
            yield from start_later()

        later = []
        running = []

        def start_later():
            stream = later.pop()
            step = next(stream)
            running.append((step, stream))
            return
            yield

        tile = 256

        def ffn():
            t = 3.0
            yield t, None
            loads[0].wait()
            loads[1].wait()
            for part in range(4):
                yield t, None
                t += 1.6

                def step(n, carry, part=part):
                    columns = pl.ds(pl.multiple_of(part * 512 + n * tile, tile), tile)
                    source = pl.ds(pl.multiple_of((part % 2) * 512 + n * tile, tile), tile)
                    inner = dot(nor_v[...], win_v[part // 2, :, source])
                    units[:, columns] = gelu(inner).astype(BF16)
                    return carry

                lax.fori_loop(0, 2, step, 0)
            loads[2].wait()
            for part in range(4):
                yield t, None
                t += 1.6

                def step(n, carry, part=part):
                    columns = pl.ds(pl.multiple_of(part * 512 + n * tile, tile), tile)
                    dense[:, columns] = dot_nt(units[:, pl.ds(0, 1024)], wdown_v[0, columns, :]) + dot_nt(
                        units[:, pl.ds(1024, 1024)], wdown_v[1, columns, :]
                    )
                    return carry

                lax.fori_loop(0, 2, step, 0)

        queue = [own_y(), sib_y(), middle(), ffn()]
        run_streams(queue, running)
        own_load.wait()
        for copy in pair_in:
            copy.wait_recv()
        loads[3].wait()

        def expert_up(first):
            def step(n, carry):
                columns = pl.ds(pl.multiple_of(n * tile, tile), tile)
                rows = xx[pl.ds(1 + first, 2)].reshape(256, width)
                inner = dot(rows, ein_v[:, columns])
                units[pl.ds(first * 128, 256), columns] = gelu(inner).astype(BF16)
                return carry

            lax.fori_loop(0, width // tile, step, 0)

        expert_up(0)
        for copy in far_in:
            copy.wait_recv()
        expert_up(2)
        loads[4].wait()
        loads[5].wait()
        loads[6].wait()

        def one_chunk(j):
            yield 1.5 * j, None
            for n in range(chunk // tile):
                inside = pl.ds(n * tile, tile)
                part = dot(units[...], eout_v[:, pl.ds(j * chunk + n * tile, tile)]).astype(BF16)
                part = part.reshape(4, 4, 2, 16, tile)
                mine[j, 0, :, :, :, inside] = part[0]
                away[j, :, :, :, :, inside] = part[1:]
            z1 = wire.send(away.at[j, 0], mine.at[j, 1], at.pair)
            z3 = wire.send(away.at[j, 2], hop.at[j], at.pair)
            z2 = wire.send(away.at[j, 1], mine.at[j, 2], cross)
            t = 5.6 * j
            yield t + 7, z3
            f = wire.send(hop.at[j], mine.at[j, 3], cross)
            yield t + 7, z1
            yield t + 7, z2
            yield t + 10, f
            c = wire.send(mine.at[j, :, 2, 0], near.at[j, 0], at.down["y"])
            d = wire.send(mine.at[j, :, 2, 1], near.at[j, 1], at.up["y"])
            a = wire.send(mine.at[j, :, 1], ahead.at[j, :, 1], at.down["y"])
            b = wire.send(mine.at[j, :, 3], ahead.at[j, :, 3], at.up["y"])
            k0 = wire.send(mine.at[j, :, 0, 1], sib.at[j, :, 0], at.sibling)
            yield t + 13, c
            c2 = wire.send(near.at[j, 0], ahead.at[j, :, 2, 0], at.down["y"])
            yield t + 13, d
            d2 = wire.send(near.at[j, 1], ahead.at[j, :, 2, 1], at.up["y"])
            yield t + 16, a
            yield t + 16, b
            yield t + 17, c2
            yield t + 17, d2
            k1 = wire.send(ahead.at[j, :, pl.ds(1, 3), 1], sib.at[j, :, pl.ds(1, 3)], at.sibling)
            yield t + 18.5, k0
            yield t + 18.5, k1
            columns = pl.ds(j * chunk, chunk)
            first = jnp.concatenate(
                [mine[j, :, pl.ds(0, 1), 0], ahead[j, :, pl.ds(1, 3), 0]], axis=1
            ).reshape(256, chunk)
            total = dense[:, columns] + dot(pla_v[:, pl.ds(0, 256)], first)
            total = total + dot(pla_v[:, pl.ds(256, 256)], sib[j].reshape(256, chunk))
            terms[j] = total.astype(BF16).reshape(4, 128, chunk)
            yield from scatter_x(wire, at, terms.at[j], got.at[j], across.at[j], t + 19, 1.6)
            total = hid_v[:, columns].astype(F32) + terms[j, 0].astype(F32)
            for n in range(3):
                total = total + got[j, n].astype(F32)
            out[:, columns] = total.astype(BF16)

        run_streams([one_chunk(j) for j in range(chunks)])
        for copy in wire.sent:
            copy.wait_send()

    inputs = [table, normed, hidden, placed, in_all, down_all, expert_in, expert_out]
    copies = 25 + chunks * 18
    return pl.pallas_call(
        body,
        out_shape=like((128, width)),
        in_specs=[pl.BlockSpec(memory_space=pl.ANY)] * len(inputs),
        out_specs=pl.BlockSpec(memory_space=pltpu.VMEM),
        scratch_shapes=[
            *[pltpu.VMEM(a.shape, BF16) for a in (normed, hidden, placed, in_all, down_all, expert_in, expert_out)],
            pltpu.VMEM((512, width), BF16),
            pltpu.VMEM((512, width), F32),
            pltpu.VMEM((5, 4, 2, 16, width), BF16),
            pltpu.VMEM((2, 3, 16, width), BF16),
            pltpu.VMEM((2, 2, 16, width), BF16),
            pltpu.VMEM((chunks, 3, 4, 2, 16, chunk), BF16),
            pltpu.VMEM((chunks, 4, 4, 2, 16, chunk), BF16),
            pltpu.VMEM((chunks, 4, 2, 16, chunk), BF16),
            pltpu.VMEM((chunks, 2, 4, 16, chunk), BF16),
            pltpu.VMEM((chunks, 4, 4, 2, 16, chunk), BF16),
            pltpu.VMEM((chunks, 4, 4, 16, chunk), BF16),
            pltpu.VMEM((chunks, 4, 128, chunk), BF16),
            pltpu.VMEM((chunks, 3, 128, chunk), BF16),
            pltpu.VMEM((chunks, 2, 64, chunk), BF16),
            pltpu.SemaphoreType.DMA((copies,)),
            pltpu.SemaphoreType.DMA((copies,)),
            pltpu.SemaphoreType.DMA((8,)),
        ],
        compiler_params=pltpu.CompilerParams(
            collective_id=number, has_side_effects=True, vmem_limit_bytes=67_000_000
        ),
        name="experts_and_dense",
    )(*inputs)


def shards(
    tokens, ln1_gain, qkv_weight, out_weight, ln2_gain, ffn_in, ffn_out,
    expert_ids, expert_in, expert_out,
):
    count, width = tokens.shape
    experts, slots = 64, 4
    chosen = expert_ids[:, 0]
    one_hot = (chosen[:, None] == jnp.arange(experts, dtype=jnp.int32)[None, :]).astype(BF16)
    order = jnp.arange(count, dtype=jnp.int32)
    before = (order[None, :] < order[:, None]).astype(BF16)
    earlier = jnp.sum(dot(before, one_hot) * one_hot.astype(F32), axis=1)
    pos = (chosen * slots + earlier.astype(jnp.int32))[None, :]

    heads, head_dim = qkv_weight.shape[1], qkv_weight.shape[3]
    qkv_width = heads * 3 * head_dim
    tiles, spots, qkv_all, out_all = first_gather(
        tokens, pos, qkv_weight.reshape(2, -1, qkv_width), out_weight.T.reshape(2, -1, out_weight.shape[0])
    )
    normed = layer_norm(tiles.reshape(4 * count, width), ln1_gain).astype(BF16)
    qkv_all = qkv_all.reshape(2, width, qkv_width)
    projected = jnp.stack([dot(normed, qkv_all[n]).astype(BF16) for n in range(2)])
    other = pair_swap(projected, 2, "swap_heads")
    image = jnp.concatenate([projected[0], other]).reshape(-1, heads, 3, head_dim)
    scores = jnp.einsum(
        "qhd,khd->hqk", image[:, :, 0], image[:, :, 1], preferred_element_type=F32
    ) * head_dim ** (-0.5)
    weights = jnp.exp(scores - jnp.max(scores, axis=-1, keepdims=True))
    probabilities = (weights / jnp.sum(weights, axis=-1, keepdims=True)).astype(BF16)
    attended = jnp.einsum("hqk,khd->qhd", probabilities, image[:, :, 2], preferred_element_type=F32)
    attended = attended.astype(BF16).reshape(2, 4 * count, heads * head_dim)
    other = pair_swap(attended, 3, "swap_attended")
    out_all = out_all.reshape(2, width, -1)
    mixed = dot_nt(attended[0], out_all[0]) + dot_nt(other, out_all[1])
    mixed = mixed.astype(BF16).reshape(4, count, width)
    got, in_all = scatter_and_weight(mixed, ffn_in.reshape(2, -1, ffn_in.shape[1]), 4, "scatter_heads")
    hidden = (
        tokens.astype(F32) + mixed[0].astype(F32) + got[0].astype(F32) + got[1].astype(F32) + got[2].astype(F32)
    ).astype(BF16)
    normed_mine = layer_norm(hidden, ln2_gain).astype(BF16)
    down = ffn_out.T
    tiles, down_all = gather_and_weight(normed_mine, down.reshape(2, -1, down.shape[1]), 5, "gather_normed")
    normed = tiles.reshape(4 * count, width)

    zh, y, core, x = (lax.axis_index(name) for name in ("zh", "y", "core", "x"))

    def named(pair, dy, dc):
        expert = (((jnp.where(pair, zh, 1 - zh) * 4 + (y + dy) % 4) * 2 + (core + dc) % 2) * 4) + x
        wanted = expert[..., None] * slots + jnp.arange(slots, dtype=jnp.int32)
        hit = wanted[..., None, :, None, None] == spots.reshape(4, count)
        same = jnp.arange(4)[:, None, None, None] == jnp.arange(4)[None, None, :, None]
        return (hit & same).astype(BF16).reshape(-1, 4 * count)

    def steps(size, dim, dims):
        return lax.broadcasted_iota(jnp.int32, dims, dim)

    dims = (2, 4, 2)
    sending = named(steps(2, 0, dims) == 1, steps(4, 1, dims), steps(2, 2, dims))
    table = dot(sending, normed).astype(BF16).reshape(2, 4, 2, 16, width)
    dims = (2, 4, 4)
    placed = named(steps(4, 1, dims) < 2, steps(4, 2, dims), steps(2, 0, dims)).T
    return tail_kernel(
        table, normed, hidden, placed, in_all.reshape(2, width, -1), down_all.reshape(2, width, -1),
        expert_in[0], expert_out[0], 6,
    )


def solution(mesh):
    split = Mesh(mesh.devices.reshape(2, 4, 2, 4, 2), ROW_COL)
    in_specs = (
        P(ROW_COL, None),
        P(),
        P(ROW, COL, None, None),
        P(COL, ROW),
        P(),
        P(ROW, COL),
        P(COL, ROW),
        P(ROW_COL, None),
        P(ROW_COL, None, None),
        P(ROW_COL, None, None),
    )
    out_specs = P(ROW_COL, None)
    return jax.shard_map(shards, mesh=split, in_specs=in_specs, out_specs=out_specs, check_vma=False)
```

```python
import heapq

import jax
import jax.numpy as jnp
from jax import lax
from jax.experimental import pallas as pl
from jax.experimental.pallas import tpu as pltpu
from jax.sharding import Mesh
from jax.sharding import PartitionSpec as P

ROW = ("zh", "y", "core")
COL = ("x", "zl")
ROW_COL = ("zh", "y", "core", "x", "zl")
BF16 = jnp.bfloat16
F32 = jnp.float32


class Spot:
    def __init__(self):
        self.x = lax.axis_index("x")
        self.y = lax.axis_index("y")
        self.zh = lax.axis_index("zh")
        self.zl = lax.axis_index("zl")
        self.core = lax.axis_index("core")
        self.row = (self.zh * 4 + self.y) * 2 + self.core
        z = self.zh * 2 + self.zl
        zp, zm = lax.rem(z + 1, 4), lax.rem(z + 3, 4)
        self.zhp, self.zhm = lax.div(zp, 2), lax.div(zm, 2)
        self.yp, self.ym = lax.rem(self.y + 1, 4), lax.rem(self.y + 3, 4)
        self.up = {
            "x": {"x": lax.rem(self.x + 1, 4)},
            "y": {"y": self.yp},
            "z": {"zh": self.zhp, "zl": lax.rem(zp, 2)},
        }
        self.down = {
            "x": {"x": lax.rem(self.x + 3, 4)},
            "y": {"y": self.ym},
            "z": {"zh": self.zhm, "zl": lax.rem(zm, 2)},
        }
        self.sibling = {"core": 1 - self.core}
        self.pair = {"zl": 1 - self.zl}


class Wire:
    def __init__(self, send_sems, recv_sems):
        self.send_sems, self.recv_sems = send_sems, recv_sems
        self.sent = []

    def send(self, src, dst, where):
        k = len(self.sent)
        copy = pltpu.make_async_remote_copy(
            src_ref=src,
            dst_ref=dst,
            send_sem=self.send_sems.at[k],
            recv_sem=self.recv_sems.at[k],
            device_id=where,
            device_id_type=pl.DeviceIdType.MESH,
        )
        copy.start()
        self.sent.append(copy)
        return copy


def greet(places):
    barrier = pltpu.get_barrier_semaphore()
    for place in places:
        pl.semaphore_signal(
            barrier, inc=1, device_id=place, device_id_type=pl.DeviceIdType.MESH
        )
    pl.semaphore_wait(barrier, len(places))


def run_streams(streams, late=()):
    queue, count = [], 0
    for stream in streams:
        step = next(stream, None)
        if step is not None:
            heapq.heappush(queue, (step[0], count, step[1], stream))
        count += 1
    while queue:
        _, n, copy, stream = heapq.heappop(queue)
        if copy is not None:
            copy.wait_recv()
        step = next(stream, None)
        if step is not None:
            heapq.heappush(queue, (step[0], n, step[1], stream))
        while late:
            step, stream = late.pop()
            heapq.heappush(queue, (step[0], count, step[1], stream))
            count += 1


def gather_weight(wire, at, own, local, whole, half, first, start, block, hold=None):
    c, zh, y = at.core, at.zh, at.y
    rows = own.shape[0] // 2
    low, high = pl.ds(0, rows), pl.ds(rows, rows)
    if first == "y":
        a = wire.send(own, whole.at[0, zh, y, c, half], at.up["y"])
        b = wire.send(own, whole.at[0, zh, y, c, half], at.down["y"])
        yield start + 2 * block, a
        slot = whole.at[0, zh, at.ym, c, half, low]
        e = wire.send(slot, slot, at.up["y"])
        yield start + 2 * block, b
        slot = whole.at[0, zh, at.yp, c, half, high]
        f = wire.send(slot, slot, at.down["y"])
        yield start + 3 * block, e
        yield start + 3 * block, f
        if local is not None:
            local.wait()
        if hold is not None:
            yield hold, None
            start = hold
        group = whole.at[0, zh, :, c, half]
        far = whole.at[1, zh, :, c, half]
        g = wire.send(group, far, at.up["z"])
        h = wire.send(group, far, at.down["z"])
        s = [wire.send(group, group, at.sibling)]
        yield start + 11 * block, g
        lower = pl.ds(0, 2)
        i = wire.send(
            whole.at[1, at.zhm, lower, c, half], whole.at[0, at.zhm, lower, c, half], at.up["z"]
        )
        s.append(wire.send(whole.at[1, at.zhm, :, c, half], whole.at[1, at.zhm, :, c, half], at.sibling))
        yield start + 11 * block, h
        upper = pl.ds(2, 2)
        j = wire.send(
            whole.at[1, at.zhp, upper, c, half], whole.at[0, at.zhp, upper, c, half], at.down["z"]
        )
        s.append(wire.send(whole.at[1, at.zhp, :, c, half], whole.at[1, at.zhp, :, c, half], at.sibling))
        yield start + 15 * block, i
        slot = whole.at[0, 1 - zh, lower, c, half]
        s.append(wire.send(slot, slot, at.sibling))
        yield start + 15 * block, j
        slot = whole.at[0, 1 - zh, upper, c, half]
        s.append(wire.send(slot, slot, at.sibling))
    else:
        a = wire.send(own, whole.at[1, zh, y, c, half], at.up["z"])
        b = wire.send(own, whole.at[1, zh, y, c, half], at.down["z"])
        yield start + 2 * block, a
        e = wire.send(
            whole.at[1, at.zhm, y, c, half, low], whole.at[0, at.zhm, y, c, half, low], at.up["z"]
        )
        yield start + 2 * block, b
        f = wire.send(
            whole.at[1, at.zhp, y, c, half, high], whole.at[0, at.zhp, y, c, half, high], at.down["z"]
        )
        yield start + 3 * block, e
        yield start + 3 * block, f
        if local is not None:
            local.wait()
        if hold is not None:
            yield hold, None
            start = hold
        group = whole.at[:, :, y, c, half]
        g = wire.send(group, group, at.up["y"])
        h = wire.send(group, group, at.down["y"])
        s = [wire.send(group, group, at.sibling)]
        yield start + 11 * block, g
        slot = whole.at[0, :, at.ym, c, half]
        i = wire.send(slot, slot, at.up["y"])
        slot = whole.at[:, :, at.ym, c, half]
        s.append(wire.send(slot, slot, at.sibling))
        yield start + 11 * block, h
        slot = whole.at[1, :, at.yp, c, half]
        j = wire.send(slot, slot, at.down["y"])
        slot = whole.at[:, :, at.yp, c, half]
        s.append(wire.send(slot, slot, at.sibling))
        across = lax.rem(y + 2, 4)
        yield start + 15 * block, i
        slot = whole.at[0, :, across, c, half]
        s.append(wire.send(slot, slot, at.sibling))
        yield start + 15 * block, j
        slot = whole.at[1, :, across, c, half]
        s.append(wire.send(slot, slot, at.sibling))
    for n, copy in enumerate(s):
        yield start + 15 * block + 2 + n / 8, copy


def gather_x(wire, at, own, tiles, parts, start, block, ready=lambda s: None):
    half = own.shape[0] // 2 if parts == 2 else own.shape[0]
    low, high = pl.ds(0, half), pl.ds(half, half)
    if parts == 2:
        a1 = wire.send(own.at[low], tiles.at[3, low], at.up["x"])
        b1 = wire.send(own.at[high], tiles.at[1, high], at.down["x"])
        a2 = wire.send(own.at[high], tiles.at[3, high], at.up["x"])
        b2 = wire.send(own.at[low], tiles.at[1, low], at.down["x"])
        yield start + block, a1
        e = wire.send(tiles.at[3, low], tiles.at[2, low], at.up["x"])
        yield start + block, b1
        f = wire.send(tiles.at[1, high], tiles.at[2, high], at.down["x"])
        yield start + 2 * block, a2
        ready(3)
        yield start + 2 * block, b2
        ready(1)
        yield start + 3 * block, e
        yield start + 3 * block, f
        ready(2)
    else:
        a = wire.send(own, tiles.at[3], at.up["x"])
        b = wire.send(own, tiles.at[1], at.down["x"])
        yield start + block, a
        e = wire.send(tiles.at[3], tiles.at[2], at.up["x"])
        yield start + block, b
        yield start + 2 * block, e


def scatter_x(wire, at, terms, got, passing, start, block):
    half = terms.shape[1] // 2
    low, high = pl.ds(0, half), pl.ds(half, half)
    c1 = wire.send(terms.at[2, low], passing.at[0], at.up["x"])
    c2 = wire.send(terms.at[2, high], passing.at[1], at.down["x"])
    a = wire.send(terms.at[1], got.at[0], at.up["x"])
    b = wire.send(terms.at[3], got.at[1], at.down["x"])
    yield start + block, c1
    d1 = wire.send(passing.at[0], got.at[2, low], at.up["x"])
    yield start + block, c2
    d2 = wire.send(passing.at[1], got.at[2, high], at.down["x"])
    yield start + 3 * block, a
    yield start + 3 * block, b
    yield start + 4 * block, d1
    yield start + 4 * block, d2


def like(shape, dtype=BF16):
    return jax.ShapeDtypeStruct(shape, dtype)


GATHER_COPIES = 13


def layer_norm(row_data, gain_vector):
    row_data = row_data.astype(F32)
    centered = row_data - jnp.mean(row_data, axis=-1, keepdims=True)
    spread = jnp.mean(centered * centered, axis=-1, keepdims=True)
    return centered * lax.rsqrt(spread + 1e-06) * gain_vector


def gelu(v):
    return v * (0.5 + 0.5 * lax.erf(v * 0.5**0.5))


def dot(a, b):
    return jnp.dot(a, b, preferred_element_type=F32)


def dot_nt(a, b):
    return lax.dot_general(a, b, (((1,), (1,)), ((), ())), preferred_element_type=F32)


def ring(wire, own, arrive, to_next, to_far, up, down, t, dt, ready):
    before, after, far = arrive
    rows = own.shape[0] // 2
    low, high = pl.ds(0, rows), pl.ds(rows, rows)
    a = wire.send(own, to_next, up)
    b = wire.send(own, to_next, down)
    yield t + dt, a
    e = wire.send(before.at[low], to_far[0].at[low], up)
    ready(0)
    yield t + dt, b
    f = wire.send(after.at[high], to_far[1].at[high], down)
    ready(1)
    yield t + 2 * dt, e
    yield t + 2 * dt, f
    ready(2)


def gather_fine(wire, at, whole, half, first, times, late, siblings):
    c, zh, y, yf = at.core, at.zh, at.y, lax.rem(at.y + 2, 4)
    t, dt = times

    def cell(zr, zhi, yi):
        return whole.at[zr, zhi, yi, c, half]

    def share(ref):
        siblings.append(wire.send(ref, ref, at.sibling))

    def over_z(yi, t, ready):
        return ring(
            wire, cell(0, zh, yi), (cell(1, at.zhm, yi), cell(1, at.zhp, yi), cell(0, 1 - zh, yi)),
            cell(1, zh, yi), (cell(0, at.zhm, yi), cell(0, at.zhp, yi)), at.up["z"], at.down["z"], t, dt, ready,
        )

    def over_y(zr, zhi, t, ready):
        return ring(
            wire, cell(zr, zhi, y), (cell(zr, zhi, at.ym), cell(zr, zhi, at.yp), cell(zr, zhi, yf)),
            cell(zr, zhi, y), (cell(zr, zhi, at.ym), cell(zr, zhi, at.yp)), at.up["y"], at.down["y"], t, dt, ready,
        )

    order = [at.ym, at.yp, yf] if first == "y" else [(1, at.zhm), (1, at.zhp), (0, 1 - zh)]

    def second(n, t):
        if first == "y":
            yi = y if n < 0 else order[n]
            share(cell(0, zh, yi))
            got = [cell(1, at.zhm, yi), cell(1, at.zhp, yi), cell(0, 1 - zh, yi)]
            stream = over_z(yi, t, lambda m: share(got[m]))
        else:
            place = (0, zh) if n < 0 else order[n]
            share(cell(*place, y))
            got = [cell(*place, at.ym), cell(*place, at.yp), cell(*place, yf)]
            stream = over_y(*place, t, lambda m: share(got[m]))
        late.append((next(stream), stream))

    ready = lambda n: second(n, t + dt * (1.5 + 1.5 * n))
    stream = over_z(y, t, ready) if first == "z" else over_y(0, zh, t, ready)
    step = next(stream)
    second(-1, t)
    while step is not None:
        yield step
        step = next(stream, None)


def front_kernel(tokens, pos, qkv, out, ffn_in, down, gain_one, gain_two, number):
    width = tokens.shape[1]
    chunk, chunks = 512, width // 512
    scale = 128.0**-0.5

    def norm(rows, gain):
        return layer_norm(rows, gain[...]).astype(BF16)

    def body(tok, pos_in, qkv_in, out_in, in_in, down_in, gain1, gain2,
             hidden, tiles_out, spots, in_all, down_all,
             tiles, normed, qkv_all, out_all, in_v, down_v, pos_v, keys, theirs, queries,
             tops, sums, parts, att, terms, got, across, mine, ss, rs, ls):
        at = Spot()
        zh, y, c = at.zh, at.y, at.core
        copies = [
            (tok, tiles.at[0]),
            (qkv_in.at[0], qkv_all.at[0, zh, y, c, 0]),
            (qkv_in.at[1], qkv_all.at[0, zh, y, c, 1]),
            (pos_in, pos_v),
            (out_in.at[0], out_all.at[0, zh, y, c, 0]),
            (out_in.at[1], out_all.at[0, zh, y, c, 1]),
            (in_in, in_v),
            (down_in, down_v),
        ]
        loads = [pltpu.make_async_copy(src, dst, ls.at[n]) for n, (src, dst) in enumerate(copies)]
        for load in loads:
            load.start()
        greet([at.up["x"], at.down["x"], at.up["y"], at.down["y"], at.up["z"], at.down["z"], at.sibling])
        for load in loads:
            load.wait()
        copies = [
            (pos_v, spots.at[0]),
            (in_v.at[0], in_all.at[0, zh, y, c, 0]),
            (in_v.at[1], in_all.at[0, zh, y, c, 1]),
            (down_v.at[0], down_all.at[0, zh, y, c, 0]),
            (down_v.at[1], down_all.at[0, zh, y, c, 1]),
        ]
        stores = [pltpu.make_async_copy(src, dst, ls.at[n]) for n, (src, dst) in enumerate(copies)]
        for store in stores:
            store.start()
        wire = Wire(ss, rs)
        late, siblings = [], []

        def norm_tile(s):
            normed[pl.ds(s * 128, 128), :] = norm(tiles[s], gain1)

        def main():
            yield 1, None
            norm_tile(0)
            yield 21, None
            assert len(siblings) == 32
            for copy in siblings:
                yield 21, copy
            columns = [pl.ds(h * 384 + 128, 256) for h in range(2)]
            swaps = []
            for r in range(2):
                for h in range(2):
                    weight = qkv_all[r, :, :, :, :, :, columns[h]].reshape(width, 256)
                    keys[r, h] = dot(normed[...], weight).astype(BF16)
                    swaps.append(wire.send(keys.at[r, h], theirs.at[1 - r, h], at.pair))
            yield 26, None

            def queries_of(n, carry):
                column = pl.ds(pl.multiple_of(lax.rem(n, 2) * 384, 128), 128)
                weight = qkv_all[lax.div(n, 2), :, :, :, :, :, column].reshape(width, 128)
                queries[n] = dot(normed[...], weight).astype(BF16)
                return carry

            lax.fori_loop(0, 4, queries_of, 0)
            yield 27, None

            def scored(n, rows, pair):
                scores = dot_nt(queries[n, rows, :], pair[:, pl.ds(0, 128)]) * scale
                top = jnp.max(scores, axis=-1, keepdims=True)
                weights = jnp.exp(scores - top)
                part = dot(weights.astype(BF16), pair[:, pl.ds(128, 128)])
                return top, jnp.sum(weights, axis=-1, keepdims=True), part

            for n in range(4):
                def own_keys(m, carry, n=n):
                    rows = pl.ds(pl.multiple_of(m * 128, 128), 128)
                    top, total, part = scored(n, rows, keys.at[n // 2, n % 2])
                    tops[n, rows, :] = top
                    sums[n, rows, :] = total
                    parts[n, rows, :] = part
                    return carry

                lax.fori_loop(0, 4, own_keys, 0)
                yield 28 + n, None

            for k, n in enumerate((2, 3, 0, 1)):
                yield 27 + 5.6 * (k + 1), swaps[k]

                def their_keys(m, carry, n=n):
                    rows = pl.ds(pl.multiple_of(m * 128, 128), 128)
                    top, total, part = scored(n, rows, theirs.at[n // 2, n % 2])
                    best = jnp.maximum(top, tops[n, rows, :])
                    ours, new = jnp.exp(tops[n, rows, :] - best), jnp.exp(top - best)
                    total = total * new + sums[n, rows, :] * ours
                    value = (part * new + parts[n, rows, :] * ours) / total
                    att[rows, pl.ds(n * 128, 128)] = value.astype(BF16)
                    return carry

                lax.fori_loop(0, 4, their_keys, 0)
            for j in range(chunks):
                late.append(((50 + 0.6 * j, None), mix(j)))

        left = [chunks]

        def mix(j):
            zhi, yi = j // 2, (j % 2) * 2
            first = out_all[0, zhi, pl.ds(yi, 2)].reshape(chunk, 256)
            second = out_all[1, zhi, pl.ds(yi, 2)].reshape(chunk, 256)
            mixed = dot_nt(att[:, pl.ds(0, 256)], first) + dot_nt(att[:, pl.ds(256, 256)], second)
            terms[j] = mixed.astype(BF16).reshape(4, 128, chunk)
            yield from scatter_x(wire, at, terms.at[j], got.at[j], across.at[j], 52 + 5.6 * j, 1.4)
            columns = pl.ds(j * chunk, chunk)
            total = tiles[0, :, columns].astype(F32) + terms[j, 0].astype(F32)
            for n in range(3):
                total = total + got[j, n].astype(F32)
            hidden[:, columns] = total.astype(BF16)
            left[0] -= 1
            if left[0] == 0:
                mine[...] = norm(hidden[...], gain2)
                last = pltpu.make_async_copy(mine, tiles_out.at[0], ls.at[5])
                last.start()
                stores.append(last)
                stream = gather_x(wire, at, mine, tiles_out, 2, 77, 5.7)
                late.append((next(stream), stream))

        def after(t, stream):
            yield t, None
            yield from stream

        run_streams([
            gather_x(wire, at, pos_v, spots, 1, 0, 2),
            gather_x(wire, at, tiles.at[0], tiles, 2, 0, 5.7, norm_tile),
            gather_fine(wire, at, qkv_all, 0, "y", (0, 3.2), late, siblings),
            gather_fine(wire, at, qkv_all, 1, "z", (0, 3.2), late, siblings),
            main(),
            after(10, gather_weight(wire, at, out_all.at[0, zh, y, c, 0], None, out_all, 0, "y", 10, 0.8)),
            after(10, gather_weight(wire, at, out_all.at[0, zh, y, c, 1], None, out_all, 1, "z", 10, 0.8)),
            after(13, gather_weight(wire, at, in_v.at[0], stores[1], in_all, 0, "y", 16, 2.8, 27)),
            after(13.5, gather_weight(wire, at, in_v.at[1], stores[2], in_all, 1, "y", 18, 2.8, 38)),
            after(26.5, gather_weight(wire, at, down_v.at[0], stores[3], down_all, 0, "z", 43, 2.8, 52)),
            after(26.6, gather_weight(wire, at, down_v.at[1], stores[4], down_all, 1, "z", 46, 2.8, 58)),
        ], late)
        for store in [stores[0], *stores[5:]]:
            store.wait()
        for copy in wire.sent:
            copy.wait_send()

    hbm, vmem = pl.BlockSpec(memory_space=pl.ANY), pl.BlockSpec(memory_space=pltpu.VMEM)
    inputs = [tokens, pos, qkv, out, ffn_in, down, gain_one, gain_two]
    copies = 4 + 3 + 6 + 2 * 36 + 6 * GATHER_COPIES + 6 * chunks + 6
    return pl.pallas_call(
        body,
        out_shape=[
            like(tokens.shape),
            like((4, *tokens.shape)),
            like((4, *pos.shape), jnp.int32),
            like((2, 2, 4, 2, *ffn_in.shape)),
            like((2, 2, 4, 2, *down.shape)),
        ],
        in_specs=[hbm] * 6 + [vmem] * 2,
        out_specs=[vmem] + [hbm] * 4,
        scratch_shapes=[
            pltpu.VMEM((4, *tokens.shape), BF16),
            pltpu.VMEM((512, width), BF16),
            pltpu.VMEM((2, 2, 4, 2, *qkv.shape), BF16),
            pltpu.VMEM((2, 2, 4, 2, *out.shape), BF16),
            pltpu.VMEM(ffn_in.shape, BF16),
            pltpu.VMEM(down.shape, BF16),
            pltpu.VMEM(pos.shape, jnp.int32),
            pltpu.VMEM((2, 2, 512, 256), BF16),
            pltpu.VMEM((2, 2, 512, 256), BF16),
            pltpu.VMEM((4, 512, 128), BF16),
            pltpu.VMEM((4, 512, 1), F32),
            pltpu.VMEM((4, 512, 1), F32),
            pltpu.VMEM((4, 512, 128), F32),
            pltpu.VMEM((512, 512), BF16),
            pltpu.VMEM((chunks, 4, 128, chunk), BF16),
            pltpu.VMEM((chunks, 3, 128, chunk), BF16),
            pltpu.VMEM((chunks, 2, 64, chunk), BF16),
            pltpu.VMEM(tokens.shape, BF16),
            pltpu.SemaphoreType.DMA((copies,)),
            pltpu.SemaphoreType.DMA((copies,)),
            pltpu.SemaphoreType.DMA((8,)),
        ],
        compiler_params=pltpu.CompilerParams(
            collective_id=number, has_side_effects=True, vmem_limit_bytes=66_000_000
        ),
        name="attention_front",
    )(*inputs)


def tail_kernel(table, normed, hidden, placed, in_all, down_all, expert_in, expert_out, number):
    width = normed.shape[1]
    chunk, chunks = 512, width // 512

    def body(tab, nor, hid, pla, win, wdown, ein, eout, out,
             nor_v, hid_v, pla_v, win_v, wdown_v, ein_v, eout_v,
             units, dense, xx, aside, passing, away, mine, hop, near, ahead, sib,
             terms, got, across, ss, rs, ls):
        at = Spot()
        cross = {"zh": 1 - at.zh, "zl": 1 - at.zl}
        own_load = pltpu.make_async_copy(tab.at[:, 0, 0], xx.at[pl.ds(0, 2), 0, 0], ls.at[0])
        pairs = [(nor, nor_v), (win, win_v), (wdown, wdown_v), (ein, ein_v), (eout, eout_v), (pla, pla_v), (hid, hid_v)]
        loads = [pltpu.make_async_copy(src, dst, ls.at[1 + n]) for n, (src, dst) in enumerate(pairs)]
        own_load.start()
        for load in loads:
            load.start()
        greet([at.up["x"], at.down["x"], at.up["y"], at.down["y"], at.sibling, at.pair, cross])
        wire = Wire(ss, rs)
        both = pl.ds(0, 2)
        core0 = wire.send(tab.at[:, 0, 1], xx.at[both, 0, 1], at.sibling)
        core1 = wire.send(tab.at[:, pl.ds(1, 3), 1], aside, at.sibling)
        pair_in, far_in = [], []

        def z_part(src, where, t):
            pair_in.append(wire.send(src(1), xx.at[(2, *where)], at.pair))
            x = wire.send(src(0), xx.at[(3, *where)], cross)
            yield t, x
            far_in.append(wire.send(xx.at[(3, *where)], xx.at[(4, *where)], at.pair))

        def held(where):
            return lambda n: xx.at[(n, *where)]

        def own_y():
            yield from z_part(lambda n: tab.at[n, 0, 0], (0, 0), 2.5)

        def sib_y():
            yield 1.5, core0
            yield from z_part(held((0, 1)), (0, 1), 5)

        y1 = wire.send(tab.at[:, 1, 0], xx.at[both, 1, 0], at.up["y"])
        y3 = wire.send(tab.at[:, 3, 0], xx.at[both, 3, 0], at.down["y"])
        y2 = wire.send(tab.at[:, 2, 0], passing.at[0], at.up["y"])
        second = {}

        def middle():
            yield 1.6, core1
            second[2] = wire.send(aside.at[:, 1], passing.at[1], at.down["y"])
            second[1] = wire.send(aside.at[:, 0], xx.at[both, 1, 1], at.up["y"])
            second[3] = wire.send(aside.at[:, 2], xx.at[both, 3, 1], at.down["y"])
            yield 6, y2
            e = wire.send(passing.at[0], xx.at[both, 2, 0], at.up["y"])
            yield 6.2, second[2]
            f = wire.send(passing.at[1], xx.at[both, 2, 1], at.down["y"])
            yield 8, y1
            yield 9, second[1]
            later.append(z_part(held((1,)), (1,), 15))
            yield from start_later()
            yield 9, y3
            yield 9.5, second[3]
            later.append(z_part(held((3,)), (3,), 18))
            yield from start_later()
            yield 12, e
            yield 12, f
            later.append(z_part(held((2,)), (2,), 21))
            yield from start_later()

        later = []
        running = []

        def start_later():
            stream = later.pop()
            step = next(stream)
            running.append((step, stream))
            return
            yield

        tile = 256

        def ffn():
            t = 3.0
            yield t, None
            loads[0].wait()
            loads[1].wait()
            for part in range(4):
                yield t, None
                t += 1.6

                def step(n, carry, part=part):
                    columns = pl.ds(pl.multiple_of(part * 512 + n * tile, tile), tile)
                    source = pl.ds(pl.multiple_of((part % 2) * 512 + n * tile, tile), tile)
                    inner = dot(nor_v[...], win_v[part // 2, :, source])
                    units[:, columns] = gelu(inner).astype(BF16)
                    return carry

                lax.fori_loop(0, 2, step, 0)
            loads[2].wait()
            for part in range(4):
                yield t, None
                t += 1.6

                def step(n, carry, part=part):
                    columns = pl.ds(pl.multiple_of(part * 512 + n * tile, tile), tile)
                    dense[:, columns] = dot_nt(units[:, pl.ds(0, 1024)], wdown_v[0, columns, :]) + dot_nt(
                        units[:, pl.ds(1024, 1024)], wdown_v[1, columns, :]
                    )
                    return carry

                lax.fori_loop(0, 2, step, 0)

        queue = [own_y(), sib_y(), middle(), ffn()]
        run_streams(queue, running)
        own_load.wait()
        for copy in pair_in:
            copy.wait_recv()
        loads[3].wait()

        def expert_up(first):
            def step(n, carry):
                columns = pl.ds(pl.multiple_of(n * tile, tile), tile)
                rows = xx[pl.ds(1 + first, 2)].reshape(256, width)
                inner = dot(rows, ein_v[:, columns])
                units[pl.ds(first * 128, 256), columns] = gelu(inner).astype(BF16)
                return carry

            lax.fori_loop(0, width // tile, step, 0)

        expert_up(0)
        for copy in far_in:
            copy.wait_recv()
        expert_up(2)
        loads[4].wait()
        loads[5].wait()
        loads[6].wait()

        def one_chunk(j):
            yield 1.5 * j, None
            for n in range(chunk // tile):
                inside = pl.ds(n * tile, tile)
                part = dot(units[...], eout_v[:, pl.ds(j * chunk + n * tile, tile)]).astype(BF16)
                part = part.reshape(4, 4, 2, 16, tile)
                mine[j, 0, :, :, :, inside] = part[0]
                away[j, :, :, :, :, inside] = part[1:]
            z1 = wire.send(away.at[j, 0], mine.at[j, 1], at.pair)
            z3 = wire.send(away.at[j, 2], hop.at[j], at.pair)
            z2 = wire.send(away.at[j, 1], mine.at[j, 2], cross)
            t = 5.6 * j
            yield t + 7, z3
            f = wire.send(hop.at[j], mine.at[j, 3], cross)
            yield t + 7, z1
            yield t + 7, z2
            yield t + 10, f
            c = wire.send(mine.at[j, :, 2, 0], near.at[j, 0], at.down["y"])
            d = wire.send(mine.at[j, :, 2, 1], near.at[j, 1], at.up["y"])
            a = wire.send(mine.at[j, :, 1], ahead.at[j, :, 1], at.down["y"])
            b = wire.send(mine.at[j, :, 3], ahead.at[j, :, 3], at.up["y"])
            k0 = wire.send(mine.at[j, :, 0, 1], sib.at[j, :, 0], at.sibling)
            yield t + 13, c
            c2 = wire.send(near.at[j, 0], ahead.at[j, :, 2, 0], at.down["y"])
            yield t + 13, d
            d2 = wire.send(near.at[j, 1], ahead.at[j, :, 2, 1], at.up["y"])
            yield t + 16, a
            yield t + 16, b
            yield t + 17, c2
            yield t + 17, d2
            k1 = wire.send(ahead.at[j, :, pl.ds(1, 3), 1], sib.at[j, :, pl.ds(1, 3)], at.sibling)
            yield t + 18.5, k0
            yield t + 18.5, k1
            columns = pl.ds(j * chunk, chunk)
            first = jnp.concatenate(
                [mine[j, :, pl.ds(0, 1), 0], ahead[j, :, pl.ds(1, 3), 0]], axis=1
            ).reshape(256, chunk)
            total = dense[:, columns] + dot(pla_v[:, pl.ds(0, 256)], first)
            total = total + dot(pla_v[:, pl.ds(256, 256)], sib[j].reshape(256, chunk))
            terms[j] = total.astype(BF16).reshape(4, 128, chunk)
            yield from scatter_x(wire, at, terms.at[j], got.at[j], across.at[j], t + 19, 1.6)
            total = hid_v[:, columns].astype(F32) + terms[j, 0].astype(F32)
            for n in range(3):
                total = total + got[j, n].astype(F32)
            out[:, columns] = total.astype(BF16)

        run_streams([one_chunk(j) for j in range(chunks)])
        for copy in wire.sent:
            copy.wait_send()

    inputs = [table, normed, hidden, placed, in_all, down_all, expert_in, expert_out]
    copies = 25 + chunks * 18
    return pl.pallas_call(
        body,
        out_shape=like((128, width)),
        in_specs=[pl.BlockSpec(memory_space=pl.ANY)] * len(inputs),
        out_specs=pl.BlockSpec(memory_space=pltpu.VMEM),
        scratch_shapes=[
            *[pltpu.VMEM(a.shape, BF16) for a in (normed, hidden, placed, in_all, down_all, expert_in, expert_out)],
            pltpu.VMEM((512, width), BF16),
            pltpu.VMEM((512, width), F32),
            pltpu.VMEM((5, 4, 2, 16, width), BF16),
            pltpu.VMEM((2, 3, 16, width), BF16),
            pltpu.VMEM((2, 2, 16, width), BF16),
            pltpu.VMEM((chunks, 3, 4, 2, 16, chunk), BF16),
            pltpu.VMEM((chunks, 4, 4, 2, 16, chunk), BF16),
            pltpu.VMEM((chunks, 4, 2, 16, chunk), BF16),
            pltpu.VMEM((chunks, 2, 4, 16, chunk), BF16),
            pltpu.VMEM((chunks, 4, 4, 2, 16, chunk), BF16),
            pltpu.VMEM((chunks, 4, 4, 16, chunk), BF16),
            pltpu.VMEM((chunks, 4, 128, chunk), BF16),
            pltpu.VMEM((chunks, 3, 128, chunk), BF16),
            pltpu.VMEM((chunks, 2, 64, chunk), BF16),
            pltpu.SemaphoreType.DMA((copies,)),
            pltpu.SemaphoreType.DMA((copies,)),
            pltpu.SemaphoreType.DMA((8,)),
        ],
        compiler_params=pltpu.CompilerParams(
            collective_id=number, has_side_effects=True, vmem_limit_bytes=67_000_000
        ),
        name="experts_and_dense",
    )(*inputs)


def shards(
    tokens, ln1_gain, qkv_weight, out_weight, ln2_gain, ffn_in, ffn_out,
    expert_ids, expert_in, expert_out,
):
    count, width = tokens.shape
    experts, slots = 64, 4
    chosen = expert_ids[:, 0]
    one_hot = (chosen[:, None] == jnp.arange(experts, dtype=jnp.int32)[None, :]).astype(BF16)
    order = jnp.arange(count, dtype=jnp.int32)
    before = (order[None, :] < order[:, None]).astype(BF16)
    earlier = jnp.sum(dot(before, one_hot) * one_hot.astype(F32), axis=1)
    pos = (chosen * slots + earlier.astype(jnp.int32))[None, :]

    qkv_width = qkv_weight.shape[1] * 3 * qkv_weight.shape[3]
    hidden, tiles, spots, in_all, down_all = front_kernel(
        tokens, pos, qkv_weight.reshape(2, -1, qkv_width), out_weight.T.reshape(2, -1, out_weight.shape[0]),
        ffn_in.reshape(2, -1, ffn_in.shape[1]), ffn_out.T.reshape(2, -1, ffn_out.shape[0]),
        ln1_gain[None, :], ln2_gain[None, :], 1,
    )
    normed = tiles.reshape(4 * count, width)

    zh, y, core, x = (lax.axis_index(name) for name in ("zh", "y", "core", "x"))

    def named(pair, dy, dc):
        expert = (((jnp.where(pair, zh, 1 - zh) * 4 + (y + dy) % 4) * 2 + (core + dc) % 2) * 4) + x
        wanted = expert[..., None] * slots + jnp.arange(slots, dtype=jnp.int32)
        hit = wanted[..., None, :, None, None] == spots.reshape(4, count)
        same = jnp.arange(4)[:, None, None, None] == jnp.arange(4)[None, None, :, None]
        return (hit & same).astype(BF16).reshape(-1, 4 * count)

    def steps(size, dim, dims):
        return lax.broadcasted_iota(jnp.int32, dims, dim)

    dims = (2, 4, 2)
    sending = named(steps(2, 0, dims) == 1, steps(4, 1, dims), steps(2, 2, dims))
    table = dot(sending, normed).astype(BF16).reshape(2, 4, 2, 16, width)
    dims = (2, 4, 4)
    placed = named(steps(4, 1, dims) < 2, steps(4, 2, dims), steps(2, 0, dims)).T
    return tail_kernel(
        table, normed, hidden, placed, in_all.reshape(2, width, -1), down_all.reshape(2, width, -1),
        expert_in[0], expert_out[0], 6,
    )


def solution(mesh):
    split = Mesh(mesh.devices.reshape(2, 4, 2, 4, 2), ROW_COL)
    in_specs = (
        P(ROW_COL, None),
        P(),
        P(ROW, COL, None, None),
        P(COL, ROW),
        P(),
        P(ROW, COL),
        P(COL, ROW),
        P(ROW_COL, None),
        P(ROW_COL, None, None),
        P(ROW_COL, None, None),
    )
    out_specs = P(ROW_COL, None)
    return jax.shard_map(shards, mesh=split, in_specs=in_specs, out_specs=out_specs, check_vma=False)
```

```python
import heapq

import jax
import jax.numpy as jnp
from jax import lax
from jax.experimental import pallas as pl
from jax.experimental.pallas import tpu as pltpu
from jax.sharding import Mesh
from jax.sharding import PartitionSpec as P

ROW = ("zh", "y", "core")
COL = ("x", "zl")
ROW_COL = ("zh", "y", "core", "x", "zl")
BF16 = jnp.bfloat16
F32 = jnp.float32


class Spot:
    def __init__(self):
        self.x = lax.axis_index("x")
        self.y = lax.axis_index("y")
        self.zh = lax.axis_index("zh")
        self.zl = lax.axis_index("zl")
        self.core = lax.axis_index("core")
        self.row = (self.zh * 4 + self.y) * 2 + self.core
        z = self.zh * 2 + self.zl
        zp, zm = lax.rem(z + 1, 4), lax.rem(z + 3, 4)
        self.zhp, self.zhm = lax.div(zp, 2), lax.div(zm, 2)
        self.yp, self.ym = lax.rem(self.y + 1, 4), lax.rem(self.y + 3, 4)
        self.up = {
            "x": {"x": lax.rem(self.x + 1, 4)},
            "y": {"y": self.yp},
            "z": {"zh": self.zhp, "zl": lax.rem(zp, 2)},
        }
        self.down = {
            "x": {"x": lax.rem(self.x + 3, 4)},
            "y": {"y": self.ym},
            "z": {"zh": self.zhm, "zl": lax.rem(zm, 2)},
        }
        self.sibling = {"core": 1 - self.core}
        self.pair = {"zl": 1 - self.zl}


class Wire:
    def __init__(self, send_sems, recv_sems):
        self.send_sems, self.recv_sems = send_sems, recv_sems
        self.sent = []

    def send(self, src, dst, where):
        k = len(self.sent)
        copy = pltpu.make_async_remote_copy(
            src_ref=src,
            dst_ref=dst,
            send_sem=self.send_sems.at[k],
            recv_sem=self.recv_sems.at[k],
            device_id=where,
            device_id_type=pl.DeviceIdType.MESH,
        )
        copy.start()
        self.sent.append(copy)
        return copy


def greet(places):
    barrier = pltpu.get_barrier_semaphore()
    for place in places:
        pl.semaphore_signal(
            barrier, inc=1, device_id=place, device_id_type=pl.DeviceIdType.MESH
        )
    pl.semaphore_wait(barrier, len(places))


def run_streams(streams, late=()):
    queue, count = [], 0
    for stream in streams:
        step = next(stream, None)
        if step is not None:
            heapq.heappush(queue, (step[0], count, step[1], stream))
        count += 1
    while queue:
        _, n, copy, stream = heapq.heappop(queue)
        if copy is not None:
            copy.wait_recv()
        step = next(stream, None)
        if step is not None:
            heapq.heappush(queue, (step[0], n, step[1], stream))
        while late:
            step, stream = late.pop()
            heapq.heappush(queue, (step[0], count, step[1], stream))
            count += 1


def gather_weight(wire, at, own, local, whole, half, first, times):
    c, zh, y = at.core, at.zh, at.y
    near, relayed, hold, grouped, last = times
    rows = own.shape[0] // 2
    low, high = pl.ds(0, rows), pl.ds(rows, rows)
    if first == "y":
        a = wire.send(own, whole.at[0, zh, y, c, half], at.up["y"])
        b = wire.send(own, whole.at[0, zh, y, c, half], at.down["y"])
        yield near, a
        slot = whole.at[0, zh, at.ym, c, half, low]
        e = wire.send(slot, slot, at.up["y"])
        yield near, b
        slot = whole.at[0, zh, at.yp, c, half, high]
        f = wire.send(slot, slot, at.down["y"])
        yield relayed, e
        yield relayed, f
        if local is not None:
            local.wait()
        yield hold, None
        group = whole.at[0, zh, :, c, half]
        far = whole.at[1, zh, :, c, half]
        g = wire.send(group, far, at.up["z"])
        h = wire.send(group, far, at.down["z"])
        s = [wire.send(group, group, at.sibling)]
        yield grouped, g
        lower = pl.ds(0, 2)
        i = wire.send(
            whole.at[1, at.zhm, lower, c, half], whole.at[0, at.zhm, lower, c, half], at.up["z"]
        )
        s.append(wire.send(whole.at[1, at.zhm, :, c, half], whole.at[1, at.zhm, :, c, half], at.sibling))
        yield grouped, h
        upper = pl.ds(2, 2)
        j = wire.send(
            whole.at[1, at.zhp, upper, c, half], whole.at[0, at.zhp, upper, c, half], at.down["z"]
        )
        s.append(wire.send(whole.at[1, at.zhp, :, c, half], whole.at[1, at.zhp, :, c, half], at.sibling))
        yield last, i
        slot = whole.at[0, 1 - zh, lower, c, half]
        s.append(wire.send(slot, slot, at.sibling))
        yield last, j
        slot = whole.at[0, 1 - zh, upper, c, half]
        s.append(wire.send(slot, slot, at.sibling))
    else:
        a = wire.send(own, whole.at[1, zh, y, c, half], at.up["z"])
        b = wire.send(own, whole.at[1, zh, y, c, half], at.down["z"])
        yield near, a
        e = wire.send(
            whole.at[1, at.zhm, y, c, half, low], whole.at[0, at.zhm, y, c, half, low], at.up["z"]
        )
        yield near, b
        f = wire.send(
            whole.at[1, at.zhp, y, c, half, high], whole.at[0, at.zhp, y, c, half, high], at.down["z"]
        )
        yield relayed, e
        yield relayed, f
        if local is not None:
            local.wait()
        yield hold, None
        group = whole.at[:, :, y, c, half]
        g = wire.send(group, group, at.up["y"])
        h = wire.send(group, group, at.down["y"])
        s = [wire.send(group, group, at.sibling)]
        yield grouped, g
        slot = whole.at[0, :, at.ym, c, half]
        i = wire.send(slot, slot, at.up["y"])
        slot = whole.at[:, :, at.ym, c, half]
        s.append(wire.send(slot, slot, at.sibling))
        yield grouped, h
        slot = whole.at[1, :, at.yp, c, half]
        j = wire.send(slot, slot, at.down["y"])
        slot = whole.at[:, :, at.yp, c, half]
        s.append(wire.send(slot, slot, at.sibling))
        across = lax.rem(y + 2, 4)
        yield last, i
        slot = whole.at[0, :, across, c, half]
        s.append(wire.send(slot, slot, at.sibling))
        yield last, j
        slot = whole.at[1, :, across, c, half]
        s.append(wire.send(slot, slot, at.sibling))
    for n, copy in enumerate(s):
        yield last + 2 + n / 8, copy


def gather_x(wire, at, own, tiles, parts, start, block, ready=lambda s: None):
    half = own.shape[0] // 2 if parts == 2 else own.shape[0]
    low, high = pl.ds(0, half), pl.ds(half, half)
    if parts == 2:
        a1 = wire.send(own.at[low], tiles.at[3, low], at.up["x"])
        b1 = wire.send(own.at[high], tiles.at[1, high], at.down["x"])
        a2 = wire.send(own.at[high], tiles.at[3, high], at.up["x"])
        b2 = wire.send(own.at[low], tiles.at[1, low], at.down["x"])
        yield start + block, a1
        e = wire.send(tiles.at[3, low], tiles.at[2, low], at.up["x"])
        yield start + block, b1
        f = wire.send(tiles.at[1, high], tiles.at[2, high], at.down["x"])
        yield start + 2 * block, a2
        ready(3)
        yield start + 2 * block, b2
        ready(1)
        yield start + 3 * block, e
        yield start + 3 * block, f
        ready(2)
    else:
        a = wire.send(own, tiles.at[3], at.up["x"])
        b = wire.send(own, tiles.at[1], at.down["x"])
        yield start + block, a
        e = wire.send(tiles.at[3], tiles.at[2], at.up["x"])
        yield start + block, b
        yield start + 2 * block, e


def scatter_x(wire, at, terms, got, passing, times):
    first, near, last = times
    half = terms.shape[1] // 2
    low, high = pl.ds(0, half), pl.ds(half, half)
    c1 = wire.send(terms.at[2, low], passing.at[0], at.up["x"])
    c2 = wire.send(terms.at[2, high], passing.at[1], at.down["x"])
    a = wire.send(terms.at[1], got.at[0], at.up["x"])
    b = wire.send(terms.at[3], got.at[1], at.down["x"])
    yield first, c1
    d1 = wire.send(passing.at[0], got.at[2, low], at.up["x"])
    yield first, c2
    d2 = wire.send(passing.at[1], got.at[2, high], at.down["x"])
    yield near, a
    yield near, b
    yield last, d1
    yield last, d2


def like(shape, dtype=BF16):
    return jax.ShapeDtypeStruct(shape, dtype)


GATHER_COPIES = 13


def layer_norm(row_data, gain_vector):
    row_data = row_data.astype(F32)
    centered = row_data - jnp.mean(row_data, axis=-1, keepdims=True)
    spread = jnp.mean(centered * centered, axis=-1, keepdims=True)
    return centered * lax.rsqrt(spread + 1e-06) * gain_vector


def gelu(v):
    return v * (0.5 + 0.5 * lax.erf(v * 0.5**0.5))


def dot(a, b):
    return jnp.dot(a, b, preferred_element_type=F32)


def dot_nt(a, b):
    return lax.dot_general(a, b, (((1,), (1,)), ((), ())), preferred_element_type=F32)


def ring(wire, own, arrive, to_next, to_far, up, down, t, dt, ready):
    before, after, far = arrive
    rows = own.shape[0] // 2
    low, high = pl.ds(0, rows), pl.ds(rows, rows)
    a = wire.send(own, to_next, up)
    b = wire.send(own, to_next, down)
    yield t + dt, a
    e = wire.send(before.at[low], to_far[0].at[low], up)
    ready(0)
    yield t + dt, b
    f = wire.send(after.at[high], to_far[1].at[high], down)
    ready(1)
    yield t + 2 * dt, e
    yield t + 2 * dt, f
    ready(2)


def gather_fine(wire, at, whole, half, first, times, late, siblings):
    c, zh, y, yf = at.core, at.zh, at.y, lax.rem(at.y + 2, 4)
    t, dt = times

    def cell(zr, zhi, yi):
        return whole.at[zr, zhi, yi, c, half]

    def share(ref):
        siblings.append(wire.send(ref, ref, at.sibling))

    def over_z(yi, t, ready):
        return ring(
            wire, cell(0, zh, yi), (cell(1, at.zhm, yi), cell(1, at.zhp, yi), cell(0, 1 - zh, yi)),
            cell(1, zh, yi), (cell(0, at.zhm, yi), cell(0, at.zhp, yi)), at.up["z"], at.down["z"], t, dt, ready,
        )

    def over_y(zr, zhi, t, ready):
        return ring(
            wire, cell(zr, zhi, y), (cell(zr, zhi, at.ym), cell(zr, zhi, at.yp), cell(zr, zhi, yf)),
            cell(zr, zhi, y), (cell(zr, zhi, at.ym), cell(zr, zhi, at.yp)), at.up["y"], at.down["y"], t, dt, ready,
        )

    order = [at.ym, at.yp, yf] if first == "y" else [(1, at.zhm), (1, at.zhp), (0, 1 - zh)]

    def second(n, t):
        if first == "y":
            yi = y if n < 0 else order[n]
            share(cell(0, zh, yi))
            got = [cell(1, at.zhm, yi), cell(1, at.zhp, yi), cell(0, 1 - zh, yi)]
            stream = over_z(yi, t, lambda m: share(got[m]))
        else:
            place = (0, zh) if n < 0 else order[n]
            share(cell(*place, y))
            got = [cell(*place, at.ym), cell(*place, at.yp), cell(*place, yf)]
            stream = over_y(*place, t, lambda m: share(got[m]))
        late.append((next(stream), stream))

    ready = lambda n: second(n, t + dt * (1.5 + 1.5 * n))
    stream = over_z(y, t, ready) if first == "z" else over_y(0, zh, t, ready)
    step = next(stream)
    second(-1, t)
    while step is not None:
        yield step
        step = next(stream, None)


def front_kernel(tokens, pos, qkv, out, ffn_in, down, gain_one, gain_two, number):
    width = tokens.shape[1]
    chunk, chunks = 512, width // 512
    scale = 128.0**-0.5

    def norm(rows, gain):
        return layer_norm(rows, gain[...]).astype(BF16)

    def body(tok, pos_in, qkv_in, out_in, in_in, down_in, gain1, gain2,
             hidden, tiles_out, spots, in_all, down_all,
             tiles, normed, qkv_all, out_all, in_v, down_v, pos_v, keys, theirs, queries,
             tops, sums, parts, att, terms, got, across, mine, ss, rs, ls):
        at = Spot()
        zh, y, c = at.zh, at.y, at.core
        copies = [
            (tok, tiles.at[0]),
            (qkv_in.at[0], qkv_all.at[0, zh, y, c, 0]),
            (qkv_in.at[1], qkv_all.at[0, zh, y, c, 1]),
            (pos_in, pos_v),
            (out_in.at[0], out_all.at[0, zh, y, c, 0]),
            (out_in.at[1], out_all.at[0, zh, y, c, 1]),
            (in_in, in_v),
            (down_in, down_v),
        ]
        loads = [pltpu.make_async_copy(src, dst, ls.at[n]) for n, (src, dst) in enumerate(copies)]
        for load in loads:
            load.start()
        greet([at.up["x"], at.down["x"], at.up["y"], at.down["y"], at.up["z"], at.down["z"], at.sibling])
        for n in (0, 1, 2, 3, 6, 7):
            loads[n].wait()
        copies = [
            (pos_v, spots.at[0]),
            (in_v.at[0], in_all.at[0, zh, y, c, 0]),
            (in_v.at[1], in_all.at[0, zh, y, c, 1]),
            (down_v.at[0], down_all.at[0, zh, y, c, 0]),
            (down_v.at[1], down_all.at[0, zh, y, c, 1]),
        ]
        stores = [pltpu.make_async_copy(src, dst, ls.at[8 + n]) for n, (src, dst) in enumerate(copies)]
        for store in stores:
            store.start()
        wire = Wire(ss, rs)
        late, siblings = [], []

        def norm_tile(s):
            normed[pl.ds(s * 128, 128), :] = norm(tiles[s], gain1)

        def main():
            yield 1, None
            norm_tile(0)
            yield 11.2, None
            loads[4].wait()
            loads[5].wait()
            yield 21, None
            assert len(siblings) == 32
            for copy in siblings:
                yield 21, copy
            columns = [pl.ds(h * 384 + 128, 256) for h in range(2)]
            swaps = []
            for r in range(2):
                for h in range(2):
                    weight = qkv_all[r, :, :, :, :, :, columns[h]].reshape(width, 256)
                    keys[r, h] = dot(normed[...], weight).astype(BF16)
                    swaps.append(wire.send(keys.at[r, h], theirs.at[1 - r, h], at.pair))
            yield 26, None

            def queries_of(n, carry):
                column = pl.ds(pl.multiple_of(lax.rem(n, 2) * 384, 128), 128)
                weight = qkv_all[lax.div(n, 2), :, :, :, :, :, column].reshape(width, 128)
                queries[n] = dot(normed[...], weight).astype(BF16)
                return carry

            lax.fori_loop(0, 4, queries_of, 0)
            yield 27, None

            def scored(n, rows, pair):
                scores = dot_nt(queries[n, rows, :], pair[:, pl.ds(0, 128)]) * scale
                top = jnp.max(scores, axis=-1, keepdims=True)
                weights = jnp.exp(scores - top)
                part = dot(weights.astype(BF16), pair[:, pl.ds(128, 128)])
                return top, jnp.sum(weights, axis=-1, keepdims=True), part

            for n in range(4):
                def own_keys(m, carry, n=n):
                    rows = pl.ds(pl.multiple_of(m * 128, 128), 128)
                    top, total, part = scored(n, rows, keys.at[n // 2, n % 2])
                    tops[n, rows, :] = top
                    sums[n, rows, :] = total
                    parts[n, rows, :] = part
                    return carry

                lax.fori_loop(0, 4, own_keys, 0)
                yield 28 + n, None

            for k, n in enumerate((2, 3, 0, 1)):
                yield 27 + 5.6 * (k + 1), swaps[k]

                def their_keys(m, carry, n=n):
                    rows = pl.ds(pl.multiple_of(m * 128, 128), 128)
                    top, total, part = scored(n, rows, theirs.at[n // 2, n % 2])
                    best = jnp.maximum(top, tops[n, rows, :])
                    ours, new = jnp.exp(tops[n, rows, :] - best), jnp.exp(top - best)
                    total = total * new + sums[n, rows, :] * ours
                    value = (part * new + parts[n, rows, :] * ours) / total
                    att[rows, pl.ds(n * 128, 128)] = value.astype(BF16)
                    return carry

                lax.fori_loop(0, 4, their_keys, 0)
            for j in range(chunks):
                late.append(((50 + 0.6 * j, None), mix(j)))

        left = [chunks]

        def mix(j):
            zhi, yi = j // 2, (j % 2) * 2
            first = out_all[0, zhi, pl.ds(yi, 2)].reshape(chunk, 256)
            second = out_all[1, zhi, pl.ds(yi, 2)].reshape(chunk, 256)
            mixed = dot_nt(att[:, pl.ds(0, 256)], first) + dot_nt(att[:, pl.ds(256, 256)], second)
            terms[j] = mixed.astype(BF16).reshape(4, 128, chunk)
            yield from scatter_x(wire, at, terms.at[j], got.at[j], across.at[j], (53.4 + 4.2 * j, 56.2 + 4.2 * j, 69.5 + 1.4 * j))
            columns = pl.ds(j * chunk, chunk)
            total = tiles[0, :, columns].astype(F32) + terms[j, 0].astype(F32)
            for n in range(3):
                total = total + got[j, n].astype(F32)
            hidden[:, columns] = total.astype(BF16)
            left[0] -= 1
            if left[0] == 0:
                mine[...] = norm(hidden[...], gain2)
                last = pltpu.make_async_copy(mine, tiles_out.at[0], ls.at[13])
                last.start()
                stores.append(last)
                stream = gather_x(wire, at, mine, tiles_out, 2, 77, 5.7)
                late.append((next(stream), stream))

        def after(t, stream):
            yield t, None
            yield from stream

        run_streams([
            gather_x(wire, at, pos_v, spots, 1, 30, 20),
            gather_x(wire, at, tiles.at[0], tiles, 2, 0, 5.7, norm_tile),
            gather_fine(wire, at, qkv_all, 0, "y", (0, 3.2), late, siblings),
            gather_fine(wire, at, qkv_all, 1, "z", (0, 3.2), late, siblings),
            main(),
            after(11.3, gather_weight(wire, at, out_all.at[0, zh, y, c, 0], None, out_all, 0, "z", (16.5, 20.9, 21.1, 38, 45))),
            after(11.3, gather_weight(wire, at, out_all.at[0, zh, y, c, 1], None, out_all, 1, "z", (16.6, 20.9, 21.1, 38, 45))),
            after(20.95, gather_weight(wire, at, in_v.at[0], stores[1], in_all, 0, "y", (29.5, 31.5, 55.3, 76, 85))),
            after(20.95, gather_weight(wire, at, in_v.at[1], stores[2], in_all, 1, "y", (29.6, 31.6, 55.4, 80, 90))),
            after(26.5, gather_weight(wire, at, down_v.at[0], stores[3], down_all, 0, "z", (55.2, 60, 60, 76.5, 85.5))),
            after(26.6, gather_weight(wire, at, down_v.at[1], stores[4], down_all, 1, "z", (55.2, 60, 60, 80.5, 90.5))),
        ], late)
        for store in [stores[0], *stores[5:]]:
            store.wait()
        for copy in wire.sent:
            copy.wait_send()

    hbm, vmem = pl.BlockSpec(memory_space=pl.ANY), pl.BlockSpec(memory_space=pltpu.VMEM)
    inputs = [tokens, pos, qkv, out, ffn_in, down, gain_one, gain_two]
    copies = 4 + 3 + 6 + 2 * 36 + 6 * GATHER_COPIES + 6 * chunks + 6
    return pl.pallas_call(
        body,
        out_shape=[
            like(tokens.shape),
            like((4, *tokens.shape)),
            like((4, *pos.shape), jnp.int32),
            like((2, 2, 4, 2, *ffn_in.shape)),
            like((2, 2, 4, 2, *down.shape)),
        ],
        in_specs=[hbm] * 6 + [vmem] * 2,
        out_specs=[vmem] + [hbm] * 4,
        scratch_shapes=[
            pltpu.VMEM((4, *tokens.shape), BF16),
            pltpu.VMEM((512, width), BF16),
            pltpu.VMEM((2, 2, 4, 2, *qkv.shape), BF16),
            pltpu.VMEM((2, 2, 4, 2, *out.shape), BF16),
            pltpu.VMEM(ffn_in.shape, BF16),
            pltpu.VMEM(down.shape, BF16),
            pltpu.VMEM(pos.shape, jnp.int32),
            pltpu.VMEM((2, 2, 512, 256), BF16),
            pltpu.VMEM((2, 2, 512, 256), BF16),
            pltpu.VMEM((4, 512, 128), BF16),
            pltpu.VMEM((4, 512, 1), F32),
            pltpu.VMEM((4, 512, 1), F32),
            pltpu.VMEM((4, 512, 128), F32),
            pltpu.VMEM((512, 512), BF16),
            pltpu.VMEM((chunks, 4, 128, chunk), BF16),
            pltpu.VMEM((chunks, 3, 128, chunk), BF16),
            pltpu.VMEM((chunks, 2, 64, chunk), BF16),
            pltpu.VMEM(tokens.shape, BF16),
            pltpu.SemaphoreType.DMA((copies,)),
            pltpu.SemaphoreType.DMA((copies,)),
            pltpu.SemaphoreType.DMA((14,)),
        ],
        compiler_params=pltpu.CompilerParams(
            collective_id=number, has_side_effects=True, vmem_limit_bytes=66_000_000
        ),
        name="attention_front",
    )(*inputs)


def tail_kernel(table, normed, hidden, placed, in_all, down_all, expert_in, expert_out, number):
    width = normed.shape[1]
    chunk, chunks = 512, width // 512

    def body(tab, nor, hid, pla, win, wdown, ein, eout, out,
             nor_v, hid_v, pla_v, win_v, wdown_v, ein_v, eout_v,
             units, dense, xx, aside, passing, away, mine, hop, other, summed, both_sums, near, ahead, sib,
             terms, got, across, ss, rs, ls):
        at = Spot()
        cross = {"zh": 1 - at.zh, "zl": 1 - at.zl}
        own_load = pltpu.make_async_copy(tab.at[:, 0, 0], xx.at[pl.ds(0, 2), 0, 0], ls.at[0])
        pairs = [(nor, nor_v), (win, win_v), (wdown, wdown_v), (ein, ein_v), (eout, eout_v), (pla, pla_v), (hid, hid_v)]
        loads = [pltpu.make_async_copy(src, dst, ls.at[1 + n]) for n, (src, dst) in enumerate(pairs)]
        own_load.start()
        for load in loads:
            load.start()
        greet([at.up["x"], at.down["x"], at.up["y"], at.down["y"], at.sibling, at.pair, cross])
        wire = Wire(ss, rs)
        both = pl.ds(0, 2)
        core0 = wire.send(tab.at[:, 0, 1], xx.at[both, 0, 1], at.sibling)
        core1 = wire.send(tab.at[:, pl.ds(1, 3), 1], aside, at.sibling)
        pair_in, far_in = [], []

        def z_part(src, where, t):
            pair_in.append(wire.send(src(1), xx.at[(2, *where)], at.pair))
            x = wire.send(src(0), xx.at[(3, *where)], cross)
            yield t, x
            far_in.append(wire.send(xx.at[(3, *where)], xx.at[(4, *where)], at.pair))

        def held(where):
            return lambda n: xx.at[(n, *where)]

        def own_y():
            yield from z_part(lambda n: tab.at[n, 0, 0], (0, 0), 2.5)

        def sib_y():
            yield 1.5, core0
            yield from z_part(held((0, 1)), (0, 1), 5)

        y1 = wire.send(tab.at[:, 1, 0], xx.at[both, 1, 0], at.up["y"])
        y3 = wire.send(tab.at[:, 3, 0], xx.at[both, 3, 0], at.down["y"])
        y2 = wire.send(tab.at[:, 2, 0], passing.at[0], at.up["y"])
        second = {}

        def middle():
            yield 1.6, core1
            second[2] = wire.send(aside.at[:, 1], passing.at[1], at.down["y"])
            second[1] = wire.send(aside.at[:, 0], xx.at[both, 1, 1], at.up["y"])
            second[3] = wire.send(aside.at[:, 2], xx.at[both, 3, 1], at.down["y"])
            yield 6, y2
            e = wire.send(passing.at[0], xx.at[both, 2, 0], at.up["y"])
            yield 6.2, second[2]
            f = wire.send(passing.at[1], xx.at[both, 2, 1], at.down["y"])
            yield 8, y1
            yield 9, second[1]
            later.append(z_part(held((1,)), (1,), 15))
            yield from start_later()
            yield 9, y3
            yield 9.5, second[3]
            later.append(z_part(held((3,)), (3,), 18))
            yield from start_later()
            yield 12, e
            yield 12, f
            later.append(z_part(held((2,)), (2,), 21))
            yield from start_later()

        later = []
        running = []

        def start_later():
            stream = later.pop()
            step = next(stream)
            running.append((step, stream))
            return
            yield

        tile = 256

        def ffn():
            t = 3.0
            yield t, None
            loads[0].wait()
            loads[1].wait()
            for part in range(4):
                yield t, None
                t += 1.6

                def step(n, carry, part=part):
                    columns = pl.ds(pl.multiple_of(part * 512 + n * tile, tile), tile)
                    source = pl.ds(pl.multiple_of((part % 2) * 512 + n * tile, tile), tile)
                    inner = dot(nor_v[...], win_v[part // 2, :, source])
                    units[:, columns] = gelu(inner).astype(BF16)
                    return carry

                lax.fori_loop(0, 2, step, 0)
            loads[2].wait()
            for part in range(4):
                yield t, None
                t += 1.6

                def step(n, carry, part=part):
                    columns = pl.ds(pl.multiple_of(part * 512 + n * tile, tile), tile)
                    dense[:, columns] = dot_nt(units[:, pl.ds(0, 1024)], wdown_v[0, columns, :]) + dot_nt(
                        units[:, pl.ds(1024, 1024)], wdown_v[1, columns, :]
                    )
                    return carry

                lax.fori_loop(0, 2, step, 0)

        queue = [own_y(), sib_y(), middle(), ffn()]
        run_streams(queue, running)
        own_load.wait()
        for copy in pair_in:
            copy.wait_recv()
        loads[3].wait()

        def expert_up(first):
            def step(n, carry):
                columns = pl.ds(pl.multiple_of(n * tile, tile), tile)
                rows = xx[pl.ds(1 + first, 2)].reshape(256, width)
                inner = dot(rows, ein_v[:, columns])
                units[pl.ds(first * 128, 256), columns] = gelu(inner).astype(BF16)
                return carry

            lax.fori_loop(0, width // tile, step, 0)

        expert_up(0)
        for copy in far_in:
            copy.wait_recv()
        expert_up(2)
        loads[4].wait()
        loads[5].wait()
        loads[6].wait()

        def one_chunk(j):
            yield 1.5 * j, None
            for n in range(chunk // tile):
                inside = pl.ds(n * tile, tile)
                part = dot(units[...], eout_v[:, pl.ds(j * chunk + n * tile, tile)]).astype(BF16)
                part = part.reshape(4, 4, 2, 16, tile)
                mine[j, :, :, :, inside] = part[0]
                away[j, :, :, :, :, inside] = part[1:]
            z3 = wire.send(away.at[j, 2], hop.at[j], at.pair)
            z1 = wire.send(away.at[j, 0], other.at[j], at.pair)
            t = 5.6 * j
            yield t + 5, z3
            summed[j] = (away[j, 1].astype(F32) + hop[j].astype(F32)).astype(BF16)
            f = wire.send(summed.at[j], both_sums.at[j, 1], cross)
            yield t + 8, z1
            both_sums[j, 0] = (mine[j].astype(F32) + other[j].astype(F32)).astype(BF16)
            yield t + 9.5, f
            c = wire.send(both_sums.at[j, :, 2, 0], near.at[j, 0], at.down["y"])
            d = wire.send(both_sums.at[j, :, 2, 1], near.at[j, 1], at.up["y"])
            a = wire.send(both_sums.at[j, :, 1], ahead.at[j, :, 1], at.down["y"])
            b = wire.send(both_sums.at[j, :, 3], ahead.at[j, :, 3], at.up["y"])
            k0 = wire.send(both_sums.at[j, :, 0, 1], sib.at[j, :, 0], at.sibling)
            yield t + 12, c
            c2 = wire.send(near.at[j, 0], ahead.at[j, :, 2, 0], at.down["y"])
            yield t + 12, d
            d2 = wire.send(near.at[j, 1], ahead.at[j, :, 2, 1], at.up["y"])
            yield t + 13.6, a
            yield t + 13.6, b
            yield t + 14.8, c2
            yield t + 14.8, d2
            k1 = wire.send(ahead.at[j, :, pl.ds(1, 3), 1], sib.at[j, :, pl.ds(1, 3)], at.sibling)
            yield t + 16.5, k0
            yield t + 16.5, k1
            columns = pl.ds(j * chunk, chunk)
            first = jnp.concatenate(
                [both_sums[j, :, pl.ds(0, 1), 0], ahead[j, :, pl.ds(1, 3), 0]], axis=1
            ).reshape(128, chunk)
            total = dense[:, columns] + dot(pla_v[:, pl.ds(0, 128)], first)
            total = total + dot(pla_v[:, pl.ds(128, 128)], sib[j].reshape(128, chunk))
            terms[j] = total.astype(BF16).reshape(4, 128, chunk)
            yield from scatter_x(wire, at, terms.at[j], got.at[j], across.at[j], (t + 18.6, t + 21.8, t + 23.4))
            total = hid_v[:, columns].astype(F32) + terms[j, 0].astype(F32)
            for n in range(3):
                total = total + got[j, n].astype(F32)
            out[:, columns] = total.astype(BF16)

        run_streams([one_chunk(j) for j in range(chunks)])
        for copy in wire.sent:
            copy.wait_send()

    inputs = [table, normed, hidden, placed, in_all, down_all, expert_in, expert_out]
    copies = 25 + chunks * 17
    return pl.pallas_call(
        body,
        out_shape=like((128, width)),
        in_specs=[pl.BlockSpec(memory_space=pl.ANY)] * len(inputs),
        out_specs=pl.BlockSpec(memory_space=pltpu.VMEM),
        scratch_shapes=[
            *[pltpu.VMEM(a.shape, BF16) for a in (normed, hidden, placed, in_all, down_all, expert_in, expert_out)],
            pltpu.VMEM((512, width), BF16),
            pltpu.VMEM((512, width), F32),
            pltpu.VMEM((5, 4, 2, 16, width), BF16),
            pltpu.VMEM((2, 3, 16, width), BF16),
            pltpu.VMEM((2, 2, 16, width), BF16),
            pltpu.VMEM((chunks, 3, 4, 2, 16, chunk), BF16),
            *[pltpu.VMEM((chunks, 4, 2, 16, chunk), BF16)] * 4,
            pltpu.VMEM((chunks, 2, 4, 2, 16, chunk), BF16),
            pltpu.VMEM((chunks, 2, 2, 16, chunk), BF16),
            pltpu.VMEM((chunks, 2, 4, 2, 16, chunk), BF16),
            pltpu.VMEM((chunks, 2, 4, 16, chunk), BF16),
            pltpu.VMEM((chunks, 4, 128, chunk), BF16),
            pltpu.VMEM((chunks, 3, 128, chunk), BF16),
            pltpu.VMEM((chunks, 2, 64, chunk), BF16),
            pltpu.SemaphoreType.DMA((copies,)),
            pltpu.SemaphoreType.DMA((copies,)),
            pltpu.SemaphoreType.DMA((8,)),
        ],
        compiler_params=pltpu.CompilerParams(
            collective_id=number, has_side_effects=True, vmem_limit_bytes=67_000_000
        ),
        name="experts_and_dense",
    )(*inputs)


def shards(
    tokens, ln1_gain, qkv_weight, out_weight, ln2_gain, ffn_in, ffn_out,
    expert_ids, expert_in, expert_out,
):
    count, width = tokens.shape
    experts, slots = 64, 4
    chosen = expert_ids[:, 0]
    one_hot = (chosen[:, None] == jnp.arange(experts, dtype=jnp.int32)[None, :]).astype(BF16)
    order = jnp.arange(count, dtype=jnp.int32)
    before = (order[None, :] < order[:, None]).astype(BF16)
    earlier = jnp.sum(dot(before, one_hot) * one_hot.astype(F32), axis=1)
    pos = (chosen * slots + earlier.astype(jnp.int32))[None, :]

    qkv_width = qkv_weight.shape[1] * 3 * qkv_weight.shape[3]
    hidden, tiles, spots, in_all, down_all = front_kernel(
        tokens, pos, qkv_weight.reshape(2, -1, qkv_width), out_weight.T.reshape(2, -1, out_weight.shape[0]),
        ffn_in.reshape(2, -1, ffn_in.shape[1]), ffn_out.T.reshape(2, -1, ffn_out.shape[0]),
        ln1_gain[None, :], ln2_gain[None, :], 1,
    )
    normed = tiles.reshape(4 * count, width)

    zh, y, core, x = (lax.axis_index(name) for name in ("zh", "y", "core", "x"))

    def named(pair, dy, dc):
        expert = (((jnp.where(pair, zh, 1 - zh) * 4 + (y + dy) % 4) * 2 + (core + dc) % 2) * 4) + x
        wanted = expert[..., None] * slots + jnp.arange(slots, dtype=jnp.int32)
        hit = wanted[..., None, :, None, None] == spots.reshape(4, count)
        same = jnp.arange(4)[:, None, None, None] == jnp.arange(4)[None, None, :, None]
        return (hit & same).astype(BF16).reshape(-1, 4 * count)

    def steps(size, dim, dims):
        return lax.broadcasted_iota(jnp.int32, dims, dim)

    dims = (2, 4, 2)
    sending = named(steps(2, 0, dims) == 1, steps(4, 1, dims), steps(2, 2, dims))
    table = dot(sending, normed).astype(BF16).reshape(2, 4, 2, 16, width)
    dims = (2, 2, 4)
    placed = named(steps(2, 1, dims) == 0, steps(4, 2, dims), steps(2, 0, dims)).T
    return tail_kernel(
        table, normed, hidden, placed, in_all.reshape(2, width, -1), down_all.reshape(2, width, -1),
        expert_in[0], expert_out[0], 6,
    )


def solution(mesh):
    split = Mesh(mesh.devices.reshape(2, 4, 2, 4, 2), ROW_COL)
    in_specs = (
        P(ROW_COL, None),
        P(),
        P(ROW, COL, None, None),
        P(COL, ROW),
        P(),
        P(ROW, COL),
        P(COL, ROW),
        P(ROW_COL, None),
        P(ROW_COL, None, None),
        P(ROW_COL, None, None),
    )
    out_specs = P(ROW_COL, None)
    return jax.shard_map(shards, mesh=split, in_specs=in_specs, out_specs=out_specs, check_vma=False)
```

```python
import heapq

import jax
import jax.numpy as jnp
from jax import lax
from jax.experimental import pallas as pl
from jax.experimental.pallas import tpu as pltpu
from jax.sharding import Mesh
from jax.sharding import PartitionSpec as P

ROW = ("zh", "y", "core")
COL = ("x", "zl")
ROW_COL = ("zh", "y", "core", "x", "zl")
BF16 = jnp.bfloat16
F32 = jnp.float32


class Spot:
    def __init__(self):
        self.x = lax.axis_index("x")
        self.y = lax.axis_index("y")
        self.zh = lax.axis_index("zh")
        self.zl = lax.axis_index("zl")
        self.core = lax.axis_index("core")
        self.row = (self.zh * 4 + self.y) * 2 + self.core
        z = self.zh * 2 + self.zl
        zp, zm = lax.rem(z + 1, 4), lax.rem(z + 3, 4)
        self.zhp, self.zhm = lax.div(zp, 2), lax.div(zm, 2)
        self.yp, self.ym = lax.rem(self.y + 1, 4), lax.rem(self.y + 3, 4)
        self.up = {
            "x": {"x": lax.rem(self.x + 1, 4)},
            "y": {"y": self.yp},
            "z": {"zh": self.zhp, "zl": lax.rem(zp, 2)},
        }
        self.down = {
            "x": {"x": lax.rem(self.x + 3, 4)},
            "y": {"y": self.ym},
            "z": {"zh": self.zhm, "zl": lax.rem(zm, 2)},
        }
        self.sibling = {"core": 1 - self.core}
        self.pair = {"zl": 1 - self.zl}


class Wire:
    def __init__(self, send_sems, recv_sems):
        self.send_sems, self.recv_sems = send_sems, recv_sems
        self.sent = []

    def send(self, src, dst, where):
        k = len(self.sent)
        copy = pltpu.make_async_remote_copy(
            src_ref=src,
            dst_ref=dst,
            send_sem=self.send_sems.at[k],
            recv_sem=self.recv_sems.at[k],
            device_id=where,
            device_id_type=pl.DeviceIdType.MESH,
        )
        copy.start()
        self.sent.append(copy)
        return copy


def greet(places):
    barrier = pltpu.get_barrier_semaphore()
    for place in places:
        pl.semaphore_signal(
            barrier, inc=1, device_id=place, device_id_type=pl.DeviceIdType.MESH
        )
    pl.semaphore_wait(barrier, len(places))


def run_streams(streams, late=()):
    queue, count = [], 0
    for stream in streams:
        step = next(stream, None)
        if step is not None:
            heapq.heappush(queue, (step[0], count, step[1], stream))
        count += 1
    while queue:
        _, n, copy, stream = heapq.heappop(queue)
        if copy is not None:
            copy.wait_recv()
        step = next(stream, None)
        if step is not None:
            heapq.heappush(queue, (step[0], n, step[1], stream))
        while late:
            step, stream = late.pop()
            heapq.heappush(queue, (step[0], count, step[1], stream))
            count += 1


def gather_weight(wire, at, own, local, whole, half, first, times):
    c, zh, y = at.core, at.zh, at.y
    near, relayed, hold, grouped, last = times
    rows = own.shape[0] // 2
    low, high = pl.ds(0, rows), pl.ds(rows, rows)
    if first == "y":
        a = wire.send(own, whole.at[0, zh, y, c, half], at.up["y"])
        b = wire.send(own, whole.at[0, zh, y, c, half], at.down["y"])
        yield near, a
        slot = whole.at[0, zh, at.ym, c, half, low]
        e = wire.send(slot, slot, at.up["y"])
        yield near, b
        slot = whole.at[0, zh, at.yp, c, half, high]
        f = wire.send(slot, slot, at.down["y"])
        yield relayed, e
        yield relayed, f
        if local is not None:
            local.wait()
        yield hold, None
        group = whole.at[0, zh, :, c, half]
        far = whole.at[1, zh, :, c, half]
        g = wire.send(group, far, at.up["z"])
        h = wire.send(group, far, at.down["z"])
        s = [wire.send(group, group, at.sibling)]
        yield grouped, g
        lower = pl.ds(0, 2)
        i = wire.send(
            whole.at[1, at.zhm, lower, c, half], whole.at[0, at.zhm, lower, c, half], at.up["z"]
        )
        s.append(wire.send(whole.at[1, at.zhm, :, c, half], whole.at[1, at.zhm, :, c, half], at.sibling))
        yield grouped, h
        upper = pl.ds(2, 2)
        j = wire.send(
            whole.at[1, at.zhp, upper, c, half], whole.at[0, at.zhp, upper, c, half], at.down["z"]
        )
        s.append(wire.send(whole.at[1, at.zhp, :, c, half], whole.at[1, at.zhp, :, c, half], at.sibling))
        yield last, i
        slot = whole.at[0, 1 - zh, lower, c, half]
        s.append(wire.send(slot, slot, at.sibling))
        yield last, j
        slot = whole.at[0, 1 - zh, upper, c, half]
        s.append(wire.send(slot, slot, at.sibling))
    else:
        a = wire.send(own, whole.at[1, zh, y, c, half], at.up["z"])
        b = wire.send(own, whole.at[1, zh, y, c, half], at.down["z"])
        yield near, a
        e = wire.send(
            whole.at[1, at.zhm, y, c, half, low], whole.at[0, at.zhm, y, c, half, low], at.up["z"]
        )
        yield near, b
        f = wire.send(
            whole.at[1, at.zhp, y, c, half, high], whole.at[0, at.zhp, y, c, half, high], at.down["z"]
        )
        yield relayed, e
        yield relayed, f
        if local is not None:
            local.wait()
        yield hold, None
        group = whole.at[:, :, y, c, half]
        g = wire.send(group, group, at.up["y"])
        h = wire.send(group, group, at.down["y"])
        s = [wire.send(group, group, at.sibling)]
        yield grouped, g
        slot = whole.at[0, :, at.ym, c, half]
        i = wire.send(slot, slot, at.up["y"])
        slot = whole.at[:, :, at.ym, c, half]
        s.append(wire.send(slot, slot, at.sibling))
        yield grouped, h
        slot = whole.at[1, :, at.yp, c, half]
        j = wire.send(slot, slot, at.down["y"])
        slot = whole.at[:, :, at.yp, c, half]
        s.append(wire.send(slot, slot, at.sibling))
        across = lax.rem(y + 2, 4)
        yield last, i
        slot = whole.at[0, :, across, c, half]
        s.append(wire.send(slot, slot, at.sibling))
        yield last, j
        slot = whole.at[1, :, across, c, half]
        s.append(wire.send(slot, slot, at.sibling))
    for n, copy in enumerate(s):
        yield last + 2 + n / 8, copy


def gather_x(wire, at, own, tiles, parts, start, block, ready=lambda s: None):
    half = own.shape[0] // 2 if parts == 2 else own.shape[0]
    low, high = pl.ds(0, half), pl.ds(half, half)
    if parts == 2:
        a1 = wire.send(own.at[low], tiles.at[3, low], at.up["x"])
        b1 = wire.send(own.at[high], tiles.at[1, high], at.down["x"])
        a2 = wire.send(own.at[high], tiles.at[3, high], at.up["x"])
        b2 = wire.send(own.at[low], tiles.at[1, low], at.down["x"])
        yield start + 1.6 * block, a1
        e = wire.send(tiles.at[3, low], tiles.at[2, low], at.up["x"])
        yield start + 1.6 * block, b1
        f = wire.send(tiles.at[1, high], tiles.at[2, high], at.down["x"])
        yield start + 2.4 * block, a2
        ready(3)
        yield start + 2.4 * block, b2
        ready(1)
        yield start + 3.3 * block, e
        yield start + 3.3 * block, f
        ready(2)
    else:
        a = wire.send(own, tiles.at[3], at.up["x"])
        b = wire.send(own, tiles.at[1], at.down["x"])
        yield start + block, a
        e = wire.send(tiles.at[3], tiles.at[2], at.up["x"])
        yield start + block, b
        yield start + 2 * block, e


def scatter_x(wire, at, terms, got, passing, times):
    first, near, last = times
    half = terms.shape[1] // 2
    low, high = pl.ds(0, half), pl.ds(half, half)
    c1 = wire.send(terms.at[2, low], passing.at[0], at.up["x"])
    c2 = wire.send(terms.at[2, high], passing.at[1], at.down["x"])
    a2 = wire.send(terms.at[1, high], got.at[0, high], at.up["x"])
    b2 = wire.send(terms.at[3, low], got.at[1, low], at.down["x"])
    yield first, c1
    terms[1, low, :] = (terms[1, low, :].astype(F32) + passing[0].astype(F32)).astype(BF16)
    a1 = wire.send(terms.at[1, low], got.at[0, low], at.up["x"])
    yield first, c2
    terms[3, high, :] = (terms[3, high, :].astype(F32) + passing[1].astype(F32)).astype(BF16)
    b1 = wire.send(terms.at[3, high], got.at[1, high], at.down["x"])
    yield near, a2
    yield near, b2
    yield last, a1
    yield last, b1


def like(shape, dtype=BF16):
    return jax.ShapeDtypeStruct(shape, dtype)


GATHER_COPIES = 13


def layer_norm(row_data, gain_vector):
    row_data = row_data.astype(F32)
    centered = row_data - jnp.mean(row_data, axis=-1, keepdims=True)
    spread = jnp.mean(centered * centered, axis=-1, keepdims=True)
    return centered * lax.rsqrt(spread + 1e-06) * gain_vector


def gelu(v):
    return v * (0.5 + 0.5 * lax.erf(v * 0.5**0.5))


def dot(a, b):
    return jnp.dot(a, b, preferred_element_type=F32)


def dot_nt(a, b):
    return lax.dot_general(a, b, (((1,), (1,)), ((), ())), preferred_element_type=F32)


def ring(wire, own, arrive, to_next, to_far, up, down, t, dt, ready):
    before, after, far = arrive
    rows = own.shape[0] // 2
    low, high = pl.ds(0, rows), pl.ds(rows, rows)
    a = wire.send(own, to_next, up)
    b = wire.send(own, to_next, down)
    yield t + dt, a
    e = wire.send(before.at[low], to_far[0].at[low], up)
    ready(0)
    yield t + dt, b
    f = wire.send(after.at[high], to_far[1].at[high], down)
    ready(1)
    yield t + 2 * dt, e
    yield t + 2 * dt, f
    ready(2)


def gather_fine(wire, at, whole, half, first, times, late, siblings):
    c, zh, y, yf = at.core, at.zh, at.y, lax.rem(at.y + 2, 4)
    t, dt = times

    def cell(zr, zhi, yi):
        return whole.at[zr, zhi, yi, c, half]

    def share(ref):
        siblings.append(wire.send(ref, ref, at.sibling))

    def over_z(yi, t, ready):
        return ring(
            wire, cell(0, zh, yi), (cell(1, at.zhm, yi), cell(1, at.zhp, yi), cell(0, 1 - zh, yi)),
            cell(1, zh, yi), (cell(0, at.zhm, yi), cell(0, at.zhp, yi)), at.up["z"], at.down["z"], t, dt, ready,
        )

    def over_y(zr, zhi, t, ready):
        return ring(
            wire, cell(zr, zhi, y), (cell(zr, zhi, at.ym), cell(zr, zhi, at.yp), cell(zr, zhi, yf)),
            cell(zr, zhi, y), (cell(zr, zhi, at.ym), cell(zr, zhi, at.yp)), at.up["y"], at.down["y"], t, dt, ready,
        )

    order = [at.ym, at.yp, yf] if first == "y" else [(1, at.zhm), (1, at.zhp), (0, 1 - zh)]

    def second(n, t):
        if first == "y":
            yi = y if n < 0 else order[n]
            share(cell(0, zh, yi))
            got = [cell(1, at.zhm, yi), cell(1, at.zhp, yi), cell(0, 1 - zh, yi)]
            stream = over_z(yi, t, lambda m: share(got[m]))
        else:
            place = (0, zh) if n < 0 else order[n]
            share(cell(*place, y))
            got = [cell(*place, at.ym), cell(*place, at.yp), cell(*place, yf)]
            stream = over_y(*place, t, lambda m: share(got[m]))
        late.append((next(stream), stream))

    ready = lambda n: second(n, t + dt * (1.5 + 1.5 * n))
    stream = over_z(y, t, ready) if first == "z" else over_y(0, zh, t, ready)
    step = next(stream)
    second(-1, t)
    while step is not None:
        yield step
        step = next(stream, None)


def front_kernel(tokens, pos, qkv, out, ffn_in, down, gain_one, gain_two, number):
    width = tokens.shape[1]
    chunk, chunks = 512, width // 512
    scale = 128.0**-0.5

    def norm(rows, gain):
        return layer_norm(rows, gain[...]).astype(BF16)

    def body(tok, ids, qkv_in, out_in, in_in, down_in, gain1, gain2,
             hidden, tiles_out, spots, in_all, down_all,
             tiles, normed, qkv_all, out_all, in_v, down_v, out_raw, down_raw, ids_v, pos_v, keys, theirs, queries,
             tops, sums, parts, att, terms, got, across, mine, ss, rs, ls):
        at = Spot()
        zh, y, c = at.zh, at.y, at.core
        copies = [
            (tok, tiles.at[0]),
            (qkv_in.at[0], qkv_all.at[0, zh, y, c, 0]),
            (qkv_in.at[1], qkv_all.at[0, zh, y, c, 1]),
            (ids, ids_v),
            (out_in, out_raw),
            (down_in, down_raw),
            (in_in, in_v),
        ]
        loads = [pltpu.make_async_copy(src, dst, ls.at[n]) for n, (src, dst) in enumerate(copies)]
        for load in loads:
            load.start()
        greet([at.up["x"], at.down["x"], at.up["y"], at.down["y"], at.up["z"], at.down["z"], at.sibling])
        for n in (0, 1, 2):
            loads[n].wait()
        for n in range(3, 7):
            loads[n].wait()
        copies = [
            (pos_v, spots.at[0]),
            (in_v.at[0], in_all.at[0, zh, y, c, 0]),
            (in_v.at[1], in_all.at[0, zh, y, c, 1]),
            (down_v.at[0], down_all.at[0, zh, y, c, 0]),
            (down_v.at[1], down_all.at[0, zh, y, c, 1]),
        ]
        stores = [pltpu.make_async_copy(src, dst, ls.at[10 + n]) for n, (src, dst) in enumerate(copies)]
        for store in stores[1:3]:
            store.start()
        wire = Wire(ss, rs)
        late, siblings = [], []

        def slots_of_tokens():
            wanted = jnp.broadcast_to(ids_v[...].astype(F32), (128, 128))
            order = [lax.broadcasted_iota(jnp.int32, (128, 128), n) for n in range(2)]
            again = (wanted == wanted.T) & (order[0] < order[1])
            earlier = jnp.sum(jnp.where(again, 1.0, 0.0), axis=0, keepdims=True)
            pos_v[...] = ids_v[...] * 4 + earlier.astype(jnp.int32)
            stores[0].start()

        def norm_tile(s):
            normed[pl.ds(s * 128, 128), :] = norm(tiles[s], gain1)

        def main():
            yield 1, None
            out_all[0, zh, y, c] = out_raw[...].T.reshape(2, 64, 256)
            yield 1.1, None
            norm_tile(0)
            yield 3.21, None
            slots_of_tokens()
            down_v[...] = down_raw[...].T.reshape(2, 64, 1024)
            for store in stores[3:5]:
                store.start()
            yield 21, None
            assert len(siblings) == 32
            for copy in siblings:
                yield 21, copy
            swaps = []
            for r in range(2):
                part = dot(normed[...], qkv_all[r, :, :, :, :, :, pl.ds(0, 512)].reshape(width, 512)).astype(BF16)
                for h in range(2):
                    keys[r, h] = part[:, h * 256 : (h + 1) * 256]
                    swaps.append(wire.send(keys.at[r, h], theirs.at[1 - r, h], at.pair))
            yield 26, None
            both = [
                dot(normed[...], qkv_all[r, :, :, :, :, :, pl.ds(512, 256)].reshape(width, 256)).astype(BF16)
                for r in range(2)
            ]
            for n in range(4):
                queries[n] = both[n // 2][:, (n % 2) * 128 : (n % 2 + 1) * 128]
            yield 27, None

            def scored(n, rows, pair):
                scores = dot_nt(queries[n, rows, :], pair[:, pl.ds(0, 128)]) * scale
                top = jnp.max(scores, axis=-1, keepdims=True)
                weights = jnp.exp(scores - top)
                part = dot(weights.astype(BF16), pair[:, pl.ds(128, 128)])
                return top, jnp.sum(weights, axis=-1, keepdims=True), part

            for n in range(4):
                def own_keys(m, carry, n=n):
                    rows = pl.ds(pl.multiple_of(m * 128, 128), 128)
                    top, total, part = scored(n, rows, keys.at[n // 2, n % 2])
                    tops[n, rows, :] = top
                    sums[n, rows, :] = total
                    parts[n, rows, :] = part
                    return carry

                lax.fori_loop(0, 4, own_keys, 0)
                yield 30.7 + n, None

            for k, n in enumerate((2, 3, 0, 1)):
                yield 35 + 5 * k, swaps[k]

                def their_keys(m, carry, n=n):
                    rows = pl.ds(pl.multiple_of(m * 128, 128), 128)
                    top, total, part = scored(n, rows, theirs.at[n // 2, n % 2])
                    best = jnp.maximum(top, tops[n, rows, :])
                    ours, new = jnp.exp(tops[n, rows, :] - best), jnp.exp(top - best)
                    total = total * new + sums[n, rows, :] * ours
                    value = (part * new + parts[n, rows, :] * ours) / total
                    att[rows, pl.ds(n * 128, 128)] = value.astype(BF16)
                    return carry

                lax.fori_loop(0, 4, their_keys, 0)
            for j in range(chunks):
                late.append(((50.5 + 0.6 * j, None), mix(j)))

        left = [chunks]

        def mix(j):
            zhi, yi = j // 2, (j % 2) * 2
            first = out_all[0, zhi, pl.ds(yi, 2)].reshape(chunk, 256)
            second = out_all[1, zhi, pl.ds(yi, 2)].reshape(chunk, 256)
            mixed = dot_nt(att[:, pl.ds(0, 256)], first) + dot_nt(att[:, pl.ds(256, 256)], second)
            terms[j] = mixed.astype(BF16).reshape(4, 128, chunk)
            yield from scatter_x(wire, at, terms.at[j], got.at[j], across.at[j], (54 + 2.8 * j, 55.4 + 2.8 * j, 66.5 + 1.4 * j))
            columns = pl.ds(j * chunk, chunk)
            total = tiles[0, :, columns].astype(F32) + terms[j, 0].astype(F32)
            for n in range(2):
                total = total + got[j, n].astype(F32)
            hidden[:, columns] = total.astype(BF16)
            left[0] -= 1
            if left[0] == 0:
                mine[...] = norm(hidden[...], gain2)
                last = pltpu.make_async_copy(mine, tiles_out.at[0], ls.at[15])
                last.start()
                stores.append(last)
                stream = gather_x(wire, at, mine, tiles_out, 2, 71, 5.2)
                late.append((next(stream), stream))

        def after(t, stream):
            yield t, None
            yield from stream

        run_streams([
            after(12, gather_x(wire, at, pos_v, spots, 1, 30, 20)),
            gather_x(wire, at, tiles.at[0], tiles, 2, 0, 5.7, norm_tile),
            gather_fine(wire, at, qkv_all, 0, "y", (0, 3.2), late, siblings),
            gather_fine(wire, at, qkv_all, 1, "z", (0, 3.2), late, siblings),
            main(),
            after(11.3, gather_weight(wire, at, out_all.at[0, zh, y, c, 0], None, out_all, 0, "z", (16.5, 20.85, 20.86, 30.8, 40))),
            after(11.3, gather_weight(wire, at, out_all.at[0, zh, y, c, 1], None, out_all, 1, "z", (16.6, 20.85, 20.86, 30.8, 40))),
            after(11.4, gather_weight(wire, at, in_v.at[0], stores[1], in_all, 0, "z", (18, 20.92, 31.6, 52.35, 71.5))),
            after(20.95, gather_weight(wire, at, in_v.at[1], stores[2], in_all, 1, "z", (29.5, 52, 52.1, 64, 79.5))),
            after(26.5, gather_weight(wire, at, down_v.at[1], stores[4], down_all, 1, "y", (33, 52.4, 52.5, 61.5, 84))),
            after(26.6, gather_weight(wire, at, down_v.at[0], stores[3], down_all, 0, "y", (33, 52.4, 52.6, 80, 89))),
        ], late)
        for store in [stores[0], *stores[5:]]:
            store.wait()
        for copy in wire.sent:
            copy.wait_send()

    hbm, vmem = pl.BlockSpec(memory_space=pl.ANY), pl.BlockSpec(memory_space=pltpu.VMEM)
    inputs = [tokens, pos, qkv, out, ffn_in, down, gain_one, gain_two]
    copies = 4 + 3 + 6 + 2 * 36 + 6 * GATHER_COPIES + 6 * chunks + 6
    return pl.pallas_call(
        body,
        out_shape=[
            like(tokens.shape),
            like((4, *tokens.shape)),
            like((4, *pos.shape), jnp.int32),
            like((2, 2, 4, 2, *ffn_in.shape)),
            like((2, 2, 4, 2, 2, 64, down.shape[0])),
        ],
        in_specs=[hbm] * 6 + [vmem] * 2,
        out_specs=[vmem] + [hbm] * 4,
        scratch_shapes=[
            pltpu.VMEM((4, *tokens.shape), BF16),
            pltpu.VMEM((512, width), BF16),
            pltpu.VMEM((2, 2, 4, 2, *qkv.shape), BF16),
            pltpu.VMEM((2, 2, 4, 2, 2, 64, out.shape[0]), BF16),
            pltpu.VMEM(ffn_in.shape, BF16),
            pltpu.VMEM((2, 64, down.shape[0]), BF16),
            pltpu.VMEM(out.shape, BF16),
            pltpu.VMEM(down.shape, BF16),
            pltpu.VMEM(pos.shape, jnp.int32),
            pltpu.VMEM(pos.shape, jnp.int32),
            pltpu.VMEM((2, 2, 512, 256), BF16),
            pltpu.VMEM((2, 2, 512, 256), BF16),
            pltpu.VMEM((4, 512, 128), BF16),
            pltpu.VMEM((4, 512, 1), F32),
            pltpu.VMEM((4, 512, 1), F32),
            pltpu.VMEM((4, 512, 128), F32),
            pltpu.VMEM((512, 512), BF16),
            pltpu.VMEM((chunks, 4, 128, chunk), BF16),
            pltpu.VMEM((chunks, 2, 128, chunk), BF16),
            pltpu.VMEM((chunks, 2, 64, chunk), BF16),
            pltpu.VMEM(tokens.shape, BF16),
            pltpu.SemaphoreType.DMA((copies,)),
            pltpu.SemaphoreType.DMA((copies,)),
            pltpu.SemaphoreType.DMA((16,)),
        ],
        compiler_params=pltpu.CompilerParams(
            collective_id=number, has_side_effects=True, vmem_limit_bytes=66_000_000
        ),
        name="attention_front",
    )(*inputs)


def tail_kernel(table, normed, hidden, placed, in_all, down_all, expert_in, expert_out, number):
    width = normed.shape[1]
    chunk, chunks = 512, width // 512

    def body(tab, nor, hid, pla, win, wdown, ein, eout, out,
             nor_v, hid_v, pla_v, win_v, wdown_v, ein_v, eout_v,
             units, dense, xx, aside, passing, away, mine, hop, other, summed, both_sums, near, ahead, sib,
             terms, got, across, ss, rs, ls):
        at = Spot()
        cross = {"zh": 1 - at.zh, "zl": 1 - at.zl}
        own_load = pltpu.make_async_copy(tab.at[:, 0, 0], xx.at[pl.ds(0, 2), 0, 0], ls.at[0])
        pairs = [(nor, nor_v), (win, win_v), (wdown, wdown_v), (ein, ein_v), (eout, eout_v), (pla, pla_v), (hid, hid_v)]
        loads = [pltpu.make_async_copy(src, dst, ls.at[1 + n]) for n, (src, dst) in enumerate(pairs)]
        own_load.start()
        for load in loads:
            load.start()
        greet([at.up["x"], at.down["x"], at.up["y"], at.down["y"], at.sibling, at.pair, cross])
        wire = Wire(ss, rs)
        both = pl.ds(0, 2)
        core0 = wire.send(tab.at[:, 0, 1], xx.at[both, 0, 1], at.sibling)
        core1 = wire.send(tab.at[:, pl.ds(1, 3), 1], aside, at.sibling)
        pair_in, far_in = [], []

        def z_part(src, where, t):
            pair_in.append(wire.send(src(1), xx.at[(2, *where)], at.pair))
            x = wire.send(src(0), xx.at[(3, *where)], cross)
            yield t, x
            far_in.append(wire.send(xx.at[(3, *where)], xx.at[(4, *where)], at.pair))

        def held(where):
            return lambda n: xx.at[(n, *where)]

        def own_y():
            yield from z_part(lambda n: tab.at[n, 0, 0], (0, 0), 2.5)

        def sib_y():
            yield 1.5, core0
            yield from z_part(held((0, 1)), (0, 1), 5)

        y1 = wire.send(tab.at[:, 1, 0], xx.at[both, 1, 0], at.up["y"])
        y3 = wire.send(tab.at[:, 3, 0], xx.at[both, 3, 0], at.down["y"])
        y2 = wire.send(tab.at[:, 2, 0], passing.at[0], at.up["y"])
        second = {}

        def middle():
            yield 1.6, core1
            second[2] = wire.send(aside.at[:, 1], passing.at[1], at.down["y"])
            second[1] = wire.send(aside.at[:, 0], xx.at[both, 1, 1], at.up["y"])
            second[3] = wire.send(aside.at[:, 2], xx.at[both, 3, 1], at.down["y"])
            yield 6, y2
            e = wire.send(passing.at[0], xx.at[both, 2, 0], at.up["y"])
            yield 6.2, second[2]
            f = wire.send(passing.at[1], xx.at[both, 2, 1], at.down["y"])
            yield 8, y1
            yield 9, second[1]
            later.append(z_part(held((1,)), (1,), 15))
            yield from start_later()
            yield 9, y3
            yield 9.5, second[3]
            later.append(z_part(held((3,)), (3,), 18))
            yield from start_later()
            yield 12, e
            yield 12, f
            later.append(z_part(held((2,)), (2,), 21))
            yield from start_later()

        later = []
        running = []

        def start_later():
            stream = later.pop()
            step = next(stream)
            running.append((step, stream))
            return
            yield

        tile = 512

        def ffn():
            t = 3.0
            yield t, None
            loads[0].wait()
            loads[1].wait()
            for part in range(4):
                yield t, None
                t += 1.6

                def step(n, carry, part=part):
                    columns = pl.ds(part * 512, 512)
                    source = pl.ds((part % 2) * 512, 512)
                    inner = dot(nor_v[...], win_v[part // 2, :, source])
                    units[:, columns] = gelu(inner).astype(BF16)
                    return carry

                step(0, 0)
            loads[2].wait()
            for part in range(4):
                yield t, None
                t += 1.6

                def step(n, carry, part=part):
                    columns = pl.ds(part * 512, 512)
                    dense[:, columns] = dot_nt(units[:, pl.ds(0, 1024)], wdown_v[0, columns, :]) + dot_nt(
                        units[:, pl.ds(1024, 1024)], wdown_v[1, columns, :]
                    )
                    return carry

                step(0, 0)

        queue = [own_y(), sib_y(), middle(), ffn()]
        run_streams(queue, running)
        own_load.wait()
        loads[3].wait()

        def expert_up(first):
            def step(n, carry):
                columns = pl.ds(pl.multiple_of(n * tile, tile), tile)
                rows = jnp.concatenate([xx[first].reshape(128, width), xx[first + 2].reshape(128, width)])
                inner = gelu(dot(rows, ein_v[:, columns])).astype(BF16)
                units[pl.ds((first - 1) * 128, 128), columns] = inner[:128]
                units[pl.ds((first + 1) * 128, 128), columns] = inner[128:]
                return carry

            lax.fori_loop(0, width // tile, step, 0)

        expert_up(1)
        for copy in pair_in + far_in:
            copy.wait_recv()
        expert_up(2)
        loads[4].wait()
        loads[5].wait()
        loads[6].wait()

        def one_chunk(j):
            yield 1.5 * j, None
            for n in range(1):
                inside = pl.ds(0, tile)
                part = dot(units[...], eout_v[:, pl.ds(j * chunk + n * tile, tile)]).astype(BF16)
                part = part.reshape(4, 4, 2, 16, tile)
                mine[j, :, :, :, inside] = part[0]
                away[j, :, :, :, :, inside] = part[1:]
            z3 = wire.send(away.at[j, 2], hop.at[j], at.pair)
            z1 = wire.send(away.at[j, 0], other.at[j], at.pair)
            t = 5.6 * j
            yield t + 5, z3
            summed[j] = (away[j, 1].astype(F32) + hop[j].astype(F32)).astype(BF16)
            f = wire.send(summed.at[j], both_sums.at[j, 1], cross)
            yield t + 8, z1
            both_sums[j, 0] = (mine[j].astype(F32) + other[j].astype(F32)).astype(BF16)
            yield t + 9.5, f
            c = wire.send(both_sums.at[j, :, 2, 0], near.at[j, 0], at.down["y"])
            d = wire.send(both_sums.at[j, :, 2, 1], near.at[j, 1], at.up["y"])
            a = wire.send(both_sums.at[j, :, 1], ahead.at[j, :, 1], at.down["y"])
            b = wire.send(both_sums.at[j, :, 3], ahead.at[j, :, 3], at.up["y"])
            k0 = wire.send(both_sums.at[j, :, 0, 1], sib.at[j, :, 0], at.sibling)
            yield t + 12, c
            c2 = wire.send(near.at[j, 0], ahead.at[j, :, 2, 0], at.down["y"])
            yield t + 12, d
            d2 = wire.send(near.at[j, 1], ahead.at[j, :, 2, 1], at.up["y"])
            yield t + 13.6, a
            yield t + 13.6, b
            yield t + 14.8, c2
            yield t + 14.8, d2
            k1 = wire.send(ahead.at[j, :, pl.ds(1, 3), 1], sib.at[j, :, pl.ds(1, 3)], at.sibling)
            yield t + 16.5, k0
            yield t + 16.5, k1
            columns = pl.ds(j * chunk, chunk)
            first = jnp.concatenate(
                [both_sums[j, :, pl.ds(0, 1), 0], ahead[j, :, pl.ds(1, 3), 0]], axis=1
            ).reshape(128, chunk)
            total = dense[:, columns] + dot(pla_v[:, pl.ds(0, 128)], first)
            total = total + dot(pla_v[:, pl.ds(128, 128)], sib[j].reshape(128, chunk))
            terms[j] = total.astype(BF16).reshape(4, 128, chunk)
            yield from scatter_x(wire, at, terms.at[j], got.at[j], across.at[j], (t + 19, t + 21, t + 23))
            total = hid_v[:, columns].astype(F32) + terms[j, 0].astype(F32)
            for n in range(2):
                total = total + got[j, n].astype(F32)
            out[:, columns] = total.astype(BF16)

        run_streams([one_chunk(j) for j in range(chunks)])
        for copy in wire.sent:
            copy.wait_send()

    inputs = [table, normed, hidden, placed, in_all, down_all, expert_in, expert_out]
    copies = 25 + chunks * 17
    return pl.pallas_call(
        body,
        out_shape=like((128, width)),
        in_specs=[pl.BlockSpec(memory_space=pl.ANY)] * len(inputs),
        out_specs=pl.BlockSpec(memory_space=pltpu.VMEM),
        scratch_shapes=[
            *[pltpu.VMEM(a.shape, BF16) for a in (normed, hidden, placed, in_all, down_all, expert_in, expert_out)],
            pltpu.VMEM((512, width), BF16),
            pltpu.VMEM((512, width), F32),
            pltpu.VMEM((5, 4, 2, 16, width), BF16),
            pltpu.VMEM((2, 3, 16, width), BF16),
            pltpu.VMEM((2, 2, 16, width), BF16),
            pltpu.VMEM((chunks, 3, 4, 2, 16, chunk), BF16),
            *[pltpu.VMEM((chunks, 4, 2, 16, chunk), BF16)] * 4,
            pltpu.VMEM((chunks, 2, 4, 2, 16, chunk), BF16),
            pltpu.VMEM((chunks, 2, 2, 16, chunk), BF16),
            pltpu.VMEM((chunks, 2, 4, 2, 16, chunk), BF16),
            pltpu.VMEM((chunks, 2, 4, 16, chunk), BF16),
            pltpu.VMEM((chunks, 4, 128, chunk), BF16),
            pltpu.VMEM((chunks, 2, 128, chunk), BF16),
            pltpu.VMEM((chunks, 2, 64, chunk), BF16),
            pltpu.SemaphoreType.DMA((copies,)),
            pltpu.SemaphoreType.DMA((copies,)),
            pltpu.SemaphoreType.DMA((8,)),
        ],
        compiler_params=pltpu.CompilerParams(
            collective_id=number, has_side_effects=True, vmem_limit_bytes=67_000_000
        ),
        name="experts_and_dense",
    )(*inputs)


def shards(
    tokens, ln1_gain, qkv_weight, out_weight, ln2_gain, ffn_in, ffn_out,
    expert_ids, expert_in, expert_out,
):
    count, width = tokens.shape
    slots = 4
    query, pairs = qkv_weight[:, :, 0], qkv_weight[:, :, 1:]
    qkv = jnp.concatenate([pairs.reshape(128, 512), query.reshape(128, 256)], axis=1).reshape(2, 64, 768)
    hidden, tiles, spots, in_all, down_all = front_kernel(
        tokens, expert_ids.reshape(1, count), qkv, out_weight,
        ffn_in.reshape(2, -1, ffn_in.shape[1]), ffn_out,
        ln1_gain[None, :], ln2_gain[None, :], 1,
    )
    normed = tiles.reshape(4 * count, width)

    zh, y, core, x = (lax.axis_index(name) for name in ("zh", "y", "core", "x"))

    def named(pair, dy, dc):
        expert = (((jnp.where(pair, zh, 1 - zh) * 4 + (y + dy) % 4) * 2 + (core + dc) % 2) * 4) + x
        wanted = expert[..., None] * slots + jnp.arange(slots, dtype=jnp.int32)
        hit = wanted[..., None, :, None, None] == spots.reshape(4, count)
        same = jnp.arange(4)[:, None, None, None] == jnp.arange(4)[None, None, :, None]
        return (hit & same).astype(BF16).reshape(-1, 4 * count)

    def steps(size, dim, dims):
        return lax.broadcasted_iota(jnp.int32, dims, dim)

    dims = (2, 4, 2)
    sending = named(steps(2, 0, dims) == 1, steps(4, 1, dims), steps(2, 2, dims))
    table = dot(sending, normed).astype(BF16).reshape(2, 4, 2, 16, width)
    dims = (2, 2, 4)
    placed = named(steps(2, 1, dims) == 0, steps(4, 2, dims), steps(2, 0, dims)).T
    return tail_kernel(
        table, normed, hidden, placed, in_all.reshape(2, width, -1), down_all.reshape(2, width, -1),
        expert_in[0], expert_out[0], 6,
    )


def solution(mesh):
    split = Mesh(mesh.devices.reshape(2, 4, 2, 4, 2), ROW_COL)
    in_specs = (
        P(ROW_COL, None),
        P(),
        P(ROW, COL, None, None),
        P(COL, ROW),
        P(),
        P(ROW, COL),
        P(COL, ROW),
        P(ROW_COL, None),
        P(ROW_COL, None, None),
        P(ROW_COL, None, None),
    )
    out_specs = P(ROW_COL, None)
    return jax.shard_map(shards, mesh=split, in_specs=in_specs, out_specs=out_specs, check_vma=False)
```

```python
import heapq

import jax
import jax.numpy as jnp
from jax import lax
from jax.experimental import pallas as pl
from jax.experimental.pallas import tpu as pltpu
from jax.sharding import Mesh
from jax.sharding import PartitionSpec as P

ROW = ("zh", "y", "core")
COL = ("x", "zl")
ROW_COL = ("zh", "y", "core", "x", "zl")
BF16 = jnp.bfloat16
F32 = jnp.float32


class Spot:
    def __init__(self):
        self.x = lax.axis_index("x")
        self.y = lax.axis_index("y")
        self.zh = lax.axis_index("zh")
        self.zl = lax.axis_index("zl")
        self.core = lax.axis_index("core")
        self.row = (self.zh * 4 + self.y) * 2 + self.core
        z = self.zh * 2 + self.zl
        zp, zm = lax.rem(z + 1, 4), lax.rem(z + 3, 4)
        self.zhp, self.zhm = lax.div(zp, 2), lax.div(zm, 2)
        self.yp, self.ym = lax.rem(self.y + 1, 4), lax.rem(self.y + 3, 4)
        self.up = {
            "x": {"x": lax.rem(self.x + 1, 4)},
            "y": {"y": self.yp},
            "z": {"zh": self.zhp, "zl": lax.rem(zp, 2)},
        }
        self.down = {
            "x": {"x": lax.rem(self.x + 3, 4)},
            "y": {"y": self.ym},
            "z": {"zh": self.zhm, "zl": lax.rem(zm, 2)},
        }
        self.sibling = {"core": 1 - self.core}
        self.pair = {"zl": 1 - self.zl}


class Wire:
    def __init__(self, send_sems, recv_sems):
        self.send_sems, self.recv_sems = send_sems, recv_sems
        self.sent = []

    def send(self, src, dst, where):
        k = len(self.sent)
        copy = pltpu.make_async_remote_copy(
            src_ref=src,
            dst_ref=dst,
            send_sem=self.send_sems.at[k],
            recv_sem=self.recv_sems.at[k],
            device_id=where,
            device_id_type=pl.DeviceIdType.MESH,
        )
        copy.start()
        self.sent.append(copy)
        return copy


def greet(places):
    barrier = pltpu.get_barrier_semaphore()
    for place in places:
        pl.semaphore_signal(
            barrier, inc=1, device_id=place, device_id_type=pl.DeviceIdType.MESH
        )
    pl.semaphore_wait(barrier, len(places))


def run_streams(streams, late=()):
    queue, count = [], 0
    for stream in streams:
        step = next(stream, None)
        if step is not None:
            heapq.heappush(queue, (step[0], count, step[1], stream))
        count += 1
    while queue:
        _, n, copy, stream = heapq.heappop(queue)
        if copy is not None:
            copy.wait_recv()
        step = next(stream, None)
        if step is not None:
            heapq.heappush(queue, (step[0], n, step[1], stream))
        while late:
            step, stream = late.pop()
            heapq.heappush(queue, (step[0], count, step[1], stream))
            count += 1


def gather_weight(wire, at, own, local, whole, half, first, times):
    c, zh, y = at.core, at.zh, at.y
    near, relayed, hold, grouped, last = times
    rows = own.shape[0] // 2
    low, high = pl.ds(0, rows), pl.ds(rows, rows)
    if first == "y":
        a = wire.send(own, whole.at[0, zh, y, c, half], at.up["y"])
        b = wire.send(own, whole.at[0, zh, y, c, half], at.down["y"])
        yield near, a
        slot = whole.at[0, zh, at.ym, c, half, low]
        e = wire.send(slot, slot, at.up["y"])
        yield near, b
        slot = whole.at[0, zh, at.yp, c, half, high]
        f = wire.send(slot, slot, at.down["y"])
        yield relayed, e
        yield relayed, f
        if local is not None:
            local.wait()
        yield hold, None
        group = whole.at[0, zh, :, c, half]
        far = whole.at[1, zh, :, c, half]
        g = wire.send(group, far, at.up["z"])
        h = wire.send(group, far, at.down["z"])
        s = [wire.send(group, group, at.sibling)]
        yield grouped, g
        lower = pl.ds(0, 2)
        i = wire.send(
            whole.at[1, at.zhm, lower, c, half], whole.at[0, at.zhm, lower, c, half], at.up["z"]
        )
        s.append(wire.send(whole.at[1, at.zhm, :, c, half], whole.at[1, at.zhm, :, c, half], at.sibling))
        yield grouped, h
        upper = pl.ds(2, 2)
        j = wire.send(
            whole.at[1, at.zhp, upper, c, half], whole.at[0, at.zhp, upper, c, half], at.down["z"]
        )
        s.append(wire.send(whole.at[1, at.zhp, :, c, half], whole.at[1, at.zhp, :, c, half], at.sibling))
        yield last, i
        slot = whole.at[0, 1 - zh, lower, c, half]
        s.append(wire.send(slot, slot, at.sibling))
        yield last, j
        slot = whole.at[0, 1 - zh, upper, c, half]
        s.append(wire.send(slot, slot, at.sibling))
    else:
        a = wire.send(own, whole.at[1, zh, y, c, half], at.up["z"])
        b = wire.send(own, whole.at[1, zh, y, c, half], at.down["z"])
        yield near, a
        e = wire.send(
            whole.at[1, at.zhm, y, c, half, low], whole.at[0, at.zhm, y, c, half, low], at.up["z"]
        )
        yield near, b
        f = wire.send(
            whole.at[1, at.zhp, y, c, half, high], whole.at[0, at.zhp, y, c, half, high], at.down["z"]
        )
        yield relayed, e
        yield relayed, f
        if local is not None:
            local.wait()
        yield hold, None
        group = whole.at[:, :, y, c, half]
        g = wire.send(group, group, at.up["y"])
        h = wire.send(group, group, at.down["y"])
        s = [wire.send(group, group, at.sibling)]
        yield grouped, g
        slot = whole.at[0, :, at.ym, c, half]
        i = wire.send(slot, slot, at.up["y"])
        slot = whole.at[:, :, at.ym, c, half]
        s.append(wire.send(slot, slot, at.sibling))
        yield grouped, h
        slot = whole.at[1, :, at.yp, c, half]
        j = wire.send(slot, slot, at.down["y"])
        slot = whole.at[:, :, at.yp, c, half]
        s.append(wire.send(slot, slot, at.sibling))
        across = lax.rem(y + 2, 4)
        yield last, i
        slot = whole.at[0, :, across, c, half]
        s.append(wire.send(slot, slot, at.sibling))
        yield last, j
        slot = whole.at[1, :, across, c, half]
        s.append(wire.send(slot, slot, at.sibling))
    for n, copy in enumerate(s):
        yield last + 2 + n / 8, copy


def gather_x(wire, at, own, tiles, parts, start, block, ready=lambda s: None):
    half = own.shape[0] // 2 if parts == 2 else own.shape[0]
    low, high = pl.ds(0, half), pl.ds(half, half)
    if parts == 2:
        a1 = wire.send(own.at[low], tiles.at[3, low], at.up["x"])
        b1 = wire.send(own.at[high], tiles.at[1, high], at.down["x"])
        a2 = wire.send(own.at[high], tiles.at[3, high], at.up["x"])
        b2 = wire.send(own.at[low], tiles.at[1, low], at.down["x"])
        yield start + 1.6 * block, a1
        e = wire.send(tiles.at[3, low], tiles.at[2, low], at.up["x"])
        yield start + 1.6 * block, b1
        f = wire.send(tiles.at[1, high], tiles.at[2, high], at.down["x"])
        yield start + 2.4 * block, a2
        ready(3)
        yield start + 2.4 * block, b2
        ready(1)
        yield start + 3.3 * block, e
        yield start + 3.3 * block, f
        ready(2)
    else:
        a = wire.send(own, tiles.at[3], at.up["x"])
        b = wire.send(own, tiles.at[1], at.down["x"])
        yield start + block, a
        e = wire.send(tiles.at[3], tiles.at[2], at.up["x"])
        yield start + block, b
        yield start + 2 * block, e


def scatter_x(wire, at, terms, got, passing, times):
    first, near, last = times
    half = terms.shape[1] // 2
    low, high = pl.ds(0, half), pl.ds(half, half)
    c1 = wire.send(terms.at[2, low], passing.at[0], at.up["x"])
    c2 = wire.send(terms.at[2, high], passing.at[1], at.down["x"])
    a2 = wire.send(terms.at[1, high], got.at[0, high], at.up["x"])
    b2 = wire.send(terms.at[3, low], got.at[1, low], at.down["x"])
    yield first, c1
    terms[1, low, :] = (terms[1, low, :].astype(F32) + passing[0].astype(F32)).astype(BF16)
    a1 = wire.send(terms.at[1, low], got.at[0, low], at.up["x"])
    yield first, c2
    terms[3, high, :] = (terms[3, high, :].astype(F32) + passing[1].astype(F32)).astype(BF16)
    b1 = wire.send(terms.at[3, high], got.at[1, high], at.down["x"])
    yield near, a2
    yield near, b2
    yield last, a1
    yield last, b1


def like(shape, dtype=BF16):
    return jax.ShapeDtypeStruct(shape, dtype)


GATHER_COPIES = 13


def layer_norm(row_data, gain_vector):
    row_data = row_data.astype(F32)
    centered = row_data - jnp.mean(row_data, axis=-1, keepdims=True)
    spread = jnp.mean(centered * centered, axis=-1, keepdims=True)
    return centered * lax.rsqrt(spread + 1e-06) * gain_vector


def gelu(v):
    return v * (0.5 + 0.5 * lax.erf(v * 0.5**0.5))


def dot(a, b):
    return jnp.dot(a, b, preferred_element_type=F32)


def dot_nt(a, b):
    return lax.dot_general(a, b, (((1,), (1,)), ((), ())), preferred_element_type=F32)


def ring(wire, own, arrive, to_next, to_far, up, down, t, dt, ready):
    before, after, far = arrive
    rows = own.shape[0] // 2
    low, high = pl.ds(0, rows), pl.ds(rows, rows)
    a = wire.send(own, to_next, up)
    b = wire.send(own, to_next, down)
    yield t + dt, a
    e = wire.send(before.at[low], to_far[0].at[low], up)
    ready(0)
    yield t + dt, b
    f = wire.send(after.at[high], to_far[1].at[high], down)
    ready(1)
    yield t + 2 * dt, e
    yield t + 2 * dt, f
    ready(2)


def gather_fine(wire, at, whole, half, first, times, late, siblings):
    c, zh, y, yf = at.core, at.zh, at.y, lax.rem(at.y + 2, 4)
    t, dt = times

    def cell(zr, zhi, yi):
        return whole.at[zr, zhi, yi, c, half]

    def share(ref):
        siblings.append(wire.send(ref, ref, at.sibling))

    def over_z(yi, t, ready):
        return ring(
            wire, cell(0, zh, yi), (cell(1, at.zhm, yi), cell(1, at.zhp, yi), cell(0, 1 - zh, yi)),
            cell(1, zh, yi), (cell(0, at.zhm, yi), cell(0, at.zhp, yi)), at.up["z"], at.down["z"], t, dt, ready,
        )

    def over_y(zr, zhi, t, ready):
        return ring(
            wire, cell(zr, zhi, y), (cell(zr, zhi, at.ym), cell(zr, zhi, at.yp), cell(zr, zhi, yf)),
            cell(zr, zhi, y), (cell(zr, zhi, at.ym), cell(zr, zhi, at.yp)), at.up["y"], at.down["y"], t, dt, ready,
        )

    order = [at.ym, at.yp, yf] if first == "y" else [(1, at.zhm), (1, at.zhp), (0, 1 - zh)]

    def second(n, t):
        if first == "y":
            yi = y if n < 0 else order[n]
            share(cell(0, zh, yi))
            got = [cell(1, at.zhm, yi), cell(1, at.zhp, yi), cell(0, 1 - zh, yi)]
            stream = over_z(yi, t, lambda m: share(got[m]))
        else:
            place = (0, zh) if n < 0 else order[n]
            share(cell(*place, y))
            got = [cell(*place, at.ym), cell(*place, at.yp), cell(*place, yf)]
            stream = over_y(*place, t, lambda m: share(got[m]))
        late.append((next(stream), stream))

    ready = lambda n: second(n, t + dt * (1.5 + 1.5 * n))
    stream = over_z(y, t, ready) if first == "z" else over_y(0, zh, t, ready)
    step = next(stream)
    second(-1, t)
    while step is not None:
        yield step
        step = next(stream, None)


def front_kernel(tokens, pos, qkv, out, ffn_in, down, gain_one, gain_two, number):
    width = tokens.shape[1]
    chunk, chunks = 512, width // 512
    scale = 128.0**-0.5

    def norm(rows, gain):
        return layer_norm(rows, gain[...]).astype(BF16)

    def body(tok, ids, qkv_in, out_in, in_in, down_in, gain1, gain2,
             hidden, tiles_out, spots, in_all, down_all,
             tiles, normed, qkv_all, out_all, in_v, down_v, out_raw, down_raw, ids_v, pos_v, keys, theirs, queries,
             tops, sums, parts, att, terms, got, across, mine, ss, rs, ls):
        at = Spot()
        zh, y, c = at.zh, at.y, at.core
        copies = [
            (tok, tiles.at[0]),
            (qkv_in.at[0], qkv_all.at[0, zh, y, c, 0]),
            (qkv_in.at[1], qkv_all.at[0, zh, y, c, 1]),
            (ids, ids_v),
            (out_in, out_raw),
            (down_in, down_raw),
            (in_in, in_v),
        ]
        loads = [pltpu.make_async_copy(src, dst, ls.at[n]) for n, (src, dst) in enumerate(copies)]
        for load in loads:
            load.start()
        greet([at.up["x"], at.down["x"], at.up["y"], at.down["y"], at.up["z"], at.down["z"], at.sibling])
        for n in (0, 1, 2):
            loads[n].wait()
        for n in range(3, 7):
            loads[n].wait()
        copies = [
            (pos_v, spots.at[0]),
            (in_v.at[0], in_all.at[0, zh, y, c, 0]),
            (in_v.at[1], in_all.at[0, zh, y, c, 1]),
            (down_v.at[0], down_all.at[0, zh, y, c, 0]),
            (down_v.at[1], down_all.at[0, zh, y, c, 1]),
        ]
        stores = [pltpu.make_async_copy(src, dst, ls.at[10 + n]) for n, (src, dst) in enumerate(copies)]
        for store in stores[1:3]:
            store.start()
        wire = Wire(ss, rs)
        late, siblings = [], []

        def slots_of_tokens():
            wanted = jnp.broadcast_to(ids_v[...].astype(F32), (128, 128))
            order = [lax.broadcasted_iota(jnp.int32, (128, 128), n) for n in range(2)]
            again = (wanted == wanted.T) & (order[0] < order[1])
            earlier = jnp.sum(jnp.where(again, 1.0, 0.0), axis=0, keepdims=True)
            pos_v[...] = ids_v[...] * 4 + earlier.astype(jnp.int32)
            stores[0].start()

        def norm_tile(s):
            normed[pl.ds(s * 128, 128), :] = norm(tiles[s], gain1)

        def main():
            yield 1, None
            out_all[0, zh, y, c] = out_raw[...].T.reshape(2, 64, 256)
            yield 1.1, None
            norm_tile(0)
            yield 3.21, None
            slots_of_tokens()
            down_v[...] = down_raw[...].T.reshape(2, 64, 1024)
            for store in stores[3:5]:
                store.start()
            yield 21, None
            assert len(siblings) == 32
            for copy in siblings:
                yield 21, copy
            swaps = []
            for r in range(2):
                part = dot(normed[...], qkv_all[r, :, :, :, :, :, pl.ds(0, 512)].reshape(width, 512)).astype(BF16)
                for h in range(2):
                    keys[r, h] = part[:, h * 256 : (h + 1) * 256]
                    swaps.append(wire.send(keys.at[r, h], theirs.at[1 - r, h], at.pair))
            yield 26, None
            both = [
                dot(normed[...], qkv_all[r, :, :, :, :, :, pl.ds(512, 256)].reshape(width, 256)).astype(BF16)
                for r in range(2)
            ]
            for n in range(4):
                queries[n] = both[n // 2][:, (n % 2) * 128 : (n % 2 + 1) * 128]
            yield 27, None

            def scored(n, rows, pair):
                scores = dot_nt(queries[n, rows, :], pair[:, pl.ds(0, 128)]) * scale
                top = jnp.max(scores, axis=-1, keepdims=True)
                weights = jnp.exp(scores - top)
                part = dot(weights.astype(BF16), pair[:, pl.ds(128, 128)])
                return top, jnp.sum(weights, axis=-1, keepdims=True), part

            for n in range(4):
                def own_keys(m, carry, n=n):
                    rows = pl.ds(pl.multiple_of(m * 128, 128), 128)
                    top, total, part = scored(n, rows, keys.at[n // 2, n % 2])
                    tops[n, rows, :] = top
                    sums[n, rows, :] = total
                    parts[n, rows, :] = part
                    return carry

                lax.fori_loop(0, 4, own_keys, 0)
                yield 30.7 + n, None

            for k, n in enumerate((2, 3, 0, 1)):
                yield 35 + 5 * k, swaps[k]

                def their_keys(m, carry, n=n):
                    rows = pl.ds(pl.multiple_of(m * 128, 128), 128)
                    top, total, part = scored(n, rows, theirs.at[n // 2, n % 2])
                    best = jnp.maximum(top, tops[n, rows, :])
                    ours, new = jnp.exp(tops[n, rows, :] - best), jnp.exp(top - best)
                    total = total * new + sums[n, rows, :] * ours
                    value = (part * new + parts[n, rows, :] * ours) / total
                    att[rows, pl.ds(n * 128, 128)] = value.astype(BF16)
                    return carry

                lax.fori_loop(0, 4, their_keys, 0)
            for j in range(chunks):
                late.append(((50.5 + 0.6 * j, None), mix(j)))

        left = [chunks]

        def mix(j):
            zhi, yi = j // 2, (j % 2) * 2
            first = out_all[0, zhi, pl.ds(yi, 2)].reshape(chunk, 256)
            second = out_all[1, zhi, pl.ds(yi, 2)].reshape(chunk, 256)
            mixed = dot_nt(att[:, pl.ds(0, 256)], first) + dot_nt(att[:, pl.ds(256, 256)], second)
            terms[j] = mixed.astype(BF16).reshape(4, 128, chunk)
            yield from scatter_x(wire, at, terms.at[j], got.at[j], across.at[j], (54 + 2.8 * j, 55.4 + 2.8 * j, 66.5 + 1.4 * j))
            columns = pl.ds(j * chunk, chunk)
            total = tiles[0, :, columns].astype(F32) + terms[j, 0].astype(F32)
            for n in range(2):
                total = total + got[j, n].astype(F32)
            hidden[:, columns] = total.astype(BF16)
            left[0] -= 1
            if left[0] == 0:
                mine[...] = norm(hidden[...], gain2)
                last = pltpu.make_async_copy(mine, tiles_out.at[0], ls.at[15])
                last.start()
                stores.append(last)
                stream = gather_x(wire, at, mine, tiles_out, 2, 71, 5.2)
                late.append((next(stream), stream))

        def after(t, stream):
            yield t, None
            yield from stream

        run_streams([
            after(12, gather_x(wire, at, pos_v, spots, 1, 30, 20)),
            gather_x(wire, at, tiles.at[0], tiles, 2, 0, 5.7, norm_tile),
            gather_fine(wire, at, qkv_all, 0, "y", (0, 3.2), late, siblings),
            gather_fine(wire, at, qkv_all, 1, "z", (0, 3.2), late, siblings),
            main(),
            after(11.3, gather_weight(wire, at, out_all.at[0, zh, y, c, 0], None, out_all, 0, "z", (16.5, 20.85, 20.86, 30.8, 40))),
            after(11.3, gather_weight(wire, at, out_all.at[0, zh, y, c, 1], None, out_all, 1, "z", (16.6, 20.85, 20.86, 30.8, 40))),
            after(11.4, gather_weight(wire, at, in_v.at[0], stores[1], in_all, 0, "z", (18, 20.92, 31.6, 52.35, 71.5))),
            after(20.95, gather_weight(wire, at, in_v.at[1], stores[2], in_all, 1, "z", (29.5, 52, 52.1, 64, 79.5))),
            after(26.5, gather_weight(wire, at, down_v.at[1], stores[4], down_all, 1, "y", (33, 52.4, 52.5, 61.5, 84))),
            after(26.6, gather_weight(wire, at, down_v.at[0], stores[3], down_all, 0, "y", (33, 52.4, 52.6, 80, 89))),
        ], late)
        for store in [stores[0], *stores[5:]]:
            store.wait()
        for copy in wire.sent:
            copy.wait_send()

    hbm, vmem = pl.BlockSpec(memory_space=pl.ANY), pl.BlockSpec(memory_space=pltpu.VMEM)
    inputs = [tokens, pos, qkv, out, ffn_in, down, gain_one, gain_two]
    copies = 4 + 3 + 6 + 2 * 36 + 6 * GATHER_COPIES + 6 * chunks + 6
    return pl.pallas_call(
        body,
        out_shape=[
            like(tokens.shape),
            like((4, *tokens.shape)),
            like((4, *pos.shape), jnp.int32),
            like((2, 2, 4, 2, *ffn_in.shape)),
            like((2, 2, 4, 2, 2, 64, down.shape[0])),
        ],
        in_specs=[hbm] * 6 + [vmem] * 2,
        out_specs=[vmem] + [hbm] * 4,
        scratch_shapes=[
            pltpu.VMEM((4, *tokens.shape), BF16),
            pltpu.VMEM((512, width), BF16),
            pltpu.VMEM((2, 2, 4, 2, *qkv.shape), BF16),
            pltpu.VMEM((2, 2, 4, 2, 2, 64, out.shape[0]), BF16),
            pltpu.VMEM(ffn_in.shape, BF16),
            pltpu.VMEM((2, 64, down.shape[0]), BF16),
            pltpu.VMEM(out.shape, BF16),
            pltpu.VMEM(down.shape, BF16),
            pltpu.VMEM(pos.shape, jnp.int32),
            pltpu.VMEM(pos.shape, jnp.int32),
            pltpu.VMEM((2, 2, 512, 256), BF16),
            pltpu.VMEM((2, 2, 512, 256), BF16),
            pltpu.VMEM((4, 512, 128), BF16),
            pltpu.VMEM((4, 512, 1), F32),
            pltpu.VMEM((4, 512, 1), F32),
            pltpu.VMEM((4, 512, 128), F32),
            pltpu.VMEM((512, 512), BF16),
            pltpu.VMEM((chunks, 4, 128, chunk), BF16),
            pltpu.VMEM((chunks, 2, 128, chunk), BF16),
            pltpu.VMEM((chunks, 2, 64, chunk), BF16),
            pltpu.VMEM(tokens.shape, BF16),
            pltpu.SemaphoreType.DMA((copies,)),
            pltpu.SemaphoreType.DMA((copies,)),
            pltpu.SemaphoreType.DMA((16,)),
        ],
        compiler_params=pltpu.CompilerParams(
            collective_id=number, has_side_effects=True, vmem_limit_bytes=66_000_000
        ),
        name="attention_front",
    )(*inputs)


def tail_kernel(spots, normed, hidden, in_all, down_all, expert_in, expert_out, number):
    width = normed.shape[1]
    chunk, chunks = 512, width // 512

    def body(spo, nor, hid, win, wdown, ein, eout, out,
             spo_v, tab, pla_v, nor_v, hid_v, win_v, wdown_v, ein_v, eout_v,
             units, dense, xx, aside, passing, away, mine, hop, other, summed, both_sums, near, ahead, sib,
             terms, got, across, ss, rs, ls):
        at = Spot()
        cross = {"zh": 1 - at.zh, "zl": 1 - at.zl}
        own_load = pltpu.make_async_copy(spo, spo_v, ls.at[0])
        pairs = [(nor, nor_v), (win, win_v), (wdown, wdown_v), (ein, ein_v), (eout, eout_v), (hid, hid_v)]
        loads = [pltpu.make_async_copy(src, dst, ls.at[1 + n]) for n, (src, dst) in enumerate(pairs)]
        own_load.start()
        for load in loads:
            load.start()
        greet([at.up["x"], at.down["x"], at.up["y"], at.down["y"], at.sibling, at.pair, cross])
        own_load.wait()
        tokens_at = jnp.concatenate([spo_v[n] for n in range(4)], axis=1)
        dims = (256, 512)
        line = lax.broadcasted_iota(jnp.int32, dims, 0)
        source = lax.broadcasted_iota(jnp.int32, dims, 1) >> 7

        def named(pair, dy, dc):
            zh = jnp.where(pair, at.zh, 1 - at.zh)
            expert = ((zh * 4 + ((at.y + dy) & 3)) * 2 + ((at.core + dc) & 1)) * 4 + at.x
            hit = (expert * 4 + (line & 3) == tokens_at) & (((line >> 2) & 3) == source)
            return jnp.where(hit, 1.0, 0.0)

        sending = named((line >> 7) == 1, (line >> 5) & 3, (line >> 4) & 1).astype(BF16)
        loads[0].wait()
        for n in range(width // 512):
            columns = pl.ds(n * 512, 512)
            rows = dot(sending, nor_v[:, columns]).astype(BF16).reshape(2, 4, 2, 16, 512)
            tab[:, :, :, :, columns] = rows
            xx[pl.ds(0, 2), 0, 0, :, columns] = rows[:, 0, 0]
        wire = Wire(ss, rs)
        both = pl.ds(0, 2)
        core0 = wire.send(tab.at[:, 0, 1], xx.at[both, 0, 1], at.sibling)
        core1 = wire.send(tab.at[:, pl.ds(1, 3), 1], aside, at.sibling)
        pair_in, far_in = [], []

        def z_part(src, where, t):
            pair_in.append(wire.send(src(1), xx.at[(2, *where)], at.pair))
            x = wire.send(src(0), xx.at[(3, *where)], cross)
            yield t, x
            far_in.append(wire.send(xx.at[(3, *where)], xx.at[(4, *where)], at.pair))

        def held(where):
            return lambda n: xx.at[(n, *where)]

        def own_y():
            yield from z_part(lambda n: tab.at[n, 0, 0], (0, 0), 2.5)

        def sib_y():
            yield 1.5, core0
            yield from z_part(held((0, 1)), (0, 1), 5)

        y1 = wire.send(tab.at[:, 1, 0], xx.at[both, 1, 0], at.up["y"])
        y3 = wire.send(tab.at[:, 3, 0], xx.at[both, 3, 0], at.down["y"])
        y2 = wire.send(tab.at[:, 2, 0], passing.at[0], at.up["y"])
        second = {}

        def middle():
            yield 1.6, core1
            second[2] = wire.send(aside.at[:, 1], passing.at[1], at.down["y"])
            second[1] = wire.send(aside.at[:, 0], xx.at[both, 1, 1], at.up["y"])
            second[3] = wire.send(aside.at[:, 2], xx.at[both, 3, 1], at.down["y"])
            yield 6, y2
            e = wire.send(passing.at[0], xx.at[both, 2, 0], at.up["y"])
            yield 6.2, second[2]
            f = wire.send(passing.at[1], xx.at[both, 2, 1], at.down["y"])
            yield 8, y1
            yield 9, second[1]
            later.append(z_part(held((1,)), (1,), 15))
            yield from start_later()
            yield 9, y3
            yield 9.5, second[3]
            later.append(z_part(held((3,)), (3,), 18))
            yield from start_later()
            yield 12, e
            yield 12, f
            later.append(z_part(held((2,)), (2,), 21))
            yield from start_later()

        later = []
        running = []

        def start_later():
            stream = later.pop()
            step = next(stream)
            running.append((step, stream))
            return
            yield

        tile = 512

        def ffn():
            t = 3.0
            yield t, None
            placed = named(((line >> 6) & 1) == 0, (line >> 4) & 3, line >> 7)
            pla_v[...] = placed.T.astype(BF16)
            loads[1].wait()
            for part in range(4):
                yield t, None
                t += 1.6

                def step(n, carry, part=part):
                    columns = pl.ds(part * 512, 512)
                    source = pl.ds((part % 2) * 512, 512)
                    inner = dot(nor_v[...], win_v[part // 2, :, source])
                    units[:, columns] = gelu(inner).astype(BF16)
                    return carry

                step(0, 0)
            loads[2].wait()
            for part in range(4):
                yield t, None
                t += 1.6

                def step(n, carry, part=part):
                    columns = pl.ds(part * 512, 512)
                    dense[:, columns] = dot_nt(units[:, pl.ds(0, 1024)], wdown_v[0, columns, :]) + dot_nt(
                        units[:, pl.ds(1024, 1024)], wdown_v[1, columns, :]
                    )
                    return carry

                step(0, 0)

        queue = [own_y(), sib_y(), middle(), ffn()]
        run_streams(queue, running)
        loads[3].wait()

        def expert_up(first):
            def step(n, carry):
                columns = pl.ds(pl.multiple_of(n * tile, tile), tile)
                rows = jnp.concatenate([xx[first].reshape(128, width), xx[first + 2].reshape(128, width)])
                inner = gelu(dot(rows, ein_v[:, columns])).astype(BF16)
                units[pl.ds((first - 1) * 128, 128), columns] = inner[:128]
                units[pl.ds((first + 1) * 128, 128), columns] = inner[128:]
                return carry

            lax.fori_loop(0, width // tile, step, 0)

        expert_up(1)
        for copy in pair_in + far_in:
            copy.wait_recv()
        expert_up(2)
        loads[4].wait()
        loads[5].wait()

        def one_chunk(j):
            yield 1.5 * j, None
            for n in range(1):
                inside = pl.ds(0, tile)
                part = dot(units[...], eout_v[:, pl.ds(j * chunk + n * tile, tile)]).astype(BF16)
                part = part.reshape(4, 4, 2, 16, tile)
                mine[j, :, :, :, inside] = part[0]
                away[j, :, :, :, :, inside] = part[1:]
            z3 = wire.send(away.at[j, 2], hop.at[j], at.pair)
            z1 = wire.send(away.at[j, 0], other.at[j], at.pair)
            t = 5.6 * j
            yield t + 5, z3
            summed[j] = (away[j, 1].astype(F32) + hop[j].astype(F32)).astype(BF16)
            f = wire.send(summed.at[j], both_sums.at[j, 1], cross)
            yield t + 8, z1
            both_sums[j, 0] = (mine[j].astype(F32) + other[j].astype(F32)).astype(BF16)
            yield t + 9.5, f
            c = wire.send(both_sums.at[j, :, 2, 0], near.at[j, 0], at.down["y"])
            d = wire.send(both_sums.at[j, :, 2, 1], near.at[j, 1], at.up["y"])
            a = wire.send(both_sums.at[j, :, 1], ahead.at[j, :, 1], at.down["y"])
            b = wire.send(both_sums.at[j, :, 3], ahead.at[j, :, 3], at.up["y"])
            k0 = wire.send(both_sums.at[j, :, 0, 1], sib.at[j, :, 0], at.sibling)
            yield t + 12, c
            c2 = wire.send(near.at[j, 0], ahead.at[j, :, 2, 0], at.down["y"])
            yield t + 12, d
            d2 = wire.send(near.at[j, 1], ahead.at[j, :, 2, 1], at.up["y"])
            yield t + 13.6, a
            yield t + 13.6, b
            yield t + 14.8, c2
            yield t + 14.8, d2
            k1 = wire.send(ahead.at[j, :, pl.ds(1, 3), 1], sib.at[j, :, pl.ds(1, 3)], at.sibling)
            yield t + 16.5, k0
            yield t + 16.5, k1
            columns = pl.ds(j * chunk, chunk)
            first = jnp.concatenate(
                [both_sums[j, :, pl.ds(0, 1), 0], ahead[j, :, pl.ds(1, 3), 0]], axis=1
            ).reshape(128, chunk)
            total = dense[:, columns] + dot(pla_v[:, pl.ds(0, 128)], first)
            total = total + dot(pla_v[:, pl.ds(128, 128)], sib[j].reshape(128, chunk))
            terms[j] = total.astype(BF16).reshape(4, 128, chunk)
            yield from scatter_x(wire, at, terms.at[j], got.at[j], across.at[j], (t + 19, t + 21, t + 23))
            total = hid_v[:, columns].astype(F32) + terms[j, 0].astype(F32)
            for n in range(2):
                total = total + got[j, n].astype(F32)
            out[:, columns] = total.astype(BF16)

        run_streams([one_chunk(j) for j in range(chunks)])
        for copy in wire.sent:
            copy.wait_send()

    inputs = [spots, normed, hidden, in_all, down_all, expert_in, expert_out]
    copies = 25 + chunks * 17
    return pl.pallas_call(
        body,
        out_shape=like((128, width)),
        in_specs=[pl.BlockSpec(memory_space=pl.ANY)] * len(inputs),
        out_specs=pl.BlockSpec(memory_space=pltpu.VMEM),
        scratch_shapes=[
            pltpu.VMEM(spots.shape, jnp.int32),
            pltpu.VMEM((2, 4, 2, 16, width), BF16),
            pltpu.VMEM((512, 256), BF16),
            *[pltpu.VMEM(a.shape, BF16) for a in (normed, hidden, in_all, down_all, expert_in, expert_out)],
            pltpu.VMEM((512, width), BF16),
            pltpu.VMEM((512, width), F32),
            pltpu.VMEM((5, 4, 2, 16, width), BF16),
            pltpu.VMEM((2, 3, 16, width), BF16),
            pltpu.VMEM((2, 2, 16, width), BF16),
            pltpu.VMEM((chunks, 3, 4, 2, 16, chunk), BF16),
            *[pltpu.VMEM((chunks, 4, 2, 16, chunk), BF16)] * 4,
            pltpu.VMEM((chunks, 2, 4, 2, 16, chunk), BF16),
            pltpu.VMEM((chunks, 2, 2, 16, chunk), BF16),
            pltpu.VMEM((chunks, 2, 4, 2, 16, chunk), BF16),
            pltpu.VMEM((chunks, 2, 4, 16, chunk), BF16),
            pltpu.VMEM((chunks, 4, 128, chunk), BF16),
            pltpu.VMEM((chunks, 2, 128, chunk), BF16),
            pltpu.VMEM((chunks, 2, 64, chunk), BF16),
            pltpu.SemaphoreType.DMA((copies,)),
            pltpu.SemaphoreType.DMA((copies,)),
            pltpu.SemaphoreType.DMA((8,)),
        ],
        compiler_params=pltpu.CompilerParams(
            collective_id=number, has_side_effects=True, vmem_limit_bytes=67_000_000
        ),
        name="experts_and_dense",
    )(*inputs)


def shards(
    tokens, ln1_gain, qkv_weight, out_weight, ln2_gain, ffn_in, ffn_out,
    expert_ids, expert_in, expert_out,
):
    count, width = tokens.shape
    query, pairs = qkv_weight[:, :, 0], qkv_weight[:, :, 1:]
    qkv = jnp.concatenate([pairs.reshape(128, 512), query.reshape(128, 256)], axis=1).reshape(2, 64, 768)
    hidden, tiles, spots, in_all, down_all = front_kernel(
        tokens, expert_ids.reshape(1, count), qkv, out_weight,
        ffn_in.reshape(2, -1, ffn_in.shape[1]), ffn_out,
        ln1_gain[None, :], ln2_gain[None, :], 1,
    )
    normed = tiles.reshape(4 * count, width)

    return tail_kernel(
        spots, normed, hidden, in_all.reshape(2, width, -1), down_all.reshape(2, width, -1),
        expert_in[0], expert_out[0], 6,
    )


def solution(mesh):
    split = Mesh(mesh.devices.reshape(2, 4, 2, 4, 2), ROW_COL)
    in_specs = (
        P(ROW_COL, None),
        P(),
        P(ROW, COL, None, None),
        P(COL, ROW),
        P(),
        P(ROW, COL),
        P(COL, ROW),
        P(ROW_COL, None),
        P(ROW_COL, None, None),
        P(ROW_COL, None, None),
    )
    out_specs = P(ROW_COL, None)
    return jax.shard_map(shards, mesh=split, in_specs=in_specs, out_specs=out_specs, check_vma=False)
```
